8 devices in a mesh: dp: 1 (over z), embed: 2 (over y), heads: 4 (over x, core).
Axes of the slice: x: 2, y: 2, z: 1, core: 2. Of those that a mesh axis runs over, the one named last changes fastest.
Arguments:
- x_in: bfloat16 [256, 3072], P('dp', 'embed')
- positions: int32 [256], P('dp')
- gain_one: float32 [3072], P('embed')
- gain_two: float32 [3072], P('embed')
- w_qkv: bfloat16 [3072, 32, 288], P('embed', 'heads')
- w_out: bfloat16 [3072, 3072], P('heads', 'embed')
- w_gu: bfloat16 [3072, 2, 8192], P('embed', None, 'heads')
- w_down: bfloat16 [8192, 3072], P('heads', 'embed')
- grad_out: bfloat16 [256, 3072], P('dp', 'embed')
Outputs:
- output 1: bfloat16 [256, 3072], P('dp', 'embed')
- output 2: bfloat16 [256, 3072], P('dp', 'embed')
- output 3: float32 [3072], P(('dp', 'embed'))
- output 4: float32 [3072], P(('dp', 'embed'))
- output 5: float32 [3072, 32, 288], P(('dp', 'embed'), 'heads')
- output 6: float32 [3072, 3072], P(('dp', 'heads'), 'embed')
- output 7: float32 [3072, 2, 8192], P(('dp', 'embed'), None, 'heads')
- output 8: float32 [8192, 3072], P(('dp', 'heads'), 'embed')
All inputs are finite; a program needn't handle non-finite values.
Results may differ from the reference program's by a relative error of at most 0.02.
Values are sent between devices in bfloat16 or wider.
A program may use at most 1 GiB of HBM per device.

```python
import jax
import jax.numpy as jnp
from jax import lax

D_MODEL = 3072
N_HEADS = 32
KV_HEADS = 32
HEAD_DIM = 96
FF_DIM = 8192
SEQ_LEN = 256
BATCH = 1

Q_PER_KV = N_HEADS // KV_HEADS
QKV_WIDTH = (Q_PER_KV + 2) * HEAD_DIM
TOKENS = BATCH * SEQ_LEN
EPSILON = 1e-5
ROPE_BASE = 10000.0
TWO_PI = 6.283185307179586


def setup_inputs(seed: int = 0, part: int = 0) -> dict:
    part_keys = jax.random.split(jax.random.fold_in(jax.random.key(seed), part), 5)
    shared_keys = jax.random.split(jax.random.key(seed + 1), 6)
    base_noise = jax.random.normal(part_keys[0], (TOKENS, D_MODEL), jnp.float32)
    token_phase = jax.random.uniform(part_keys[1], (TOKENS, 1), jnp.float32) * TWO_PI
    col_angle = TWO_PI * jnp.arange(D_MODEL, dtype=jnp.float32)[None, :] / D_MODEL
    x_in = (base_noise * jnp.exp(jnp.cos(col_angle - token_phase))).astype(jnp.bfloat16)
    pos_gaps = jax.random.randint(part_keys[2], (SEQ_LEN,), 1, 4)
    offset = jax.random.randint(part_keys[3], (1,), 0, 1024)
    positions = (offset + jnp.cumsum(pos_gaps)).astype(jnp.int32)
    grad_out = jax.random.normal(part_keys[4], (TOKENS, D_MODEL), jnp.float32).astype(jnp.bfloat16)
    gain_one = 1.0 + 0.3 * jax.random.normal(shared_keys[0], (D_MODEL,), jnp.float32)
    gain_two = 1.0 + 0.3 * jax.random.normal(shared_keys[1], (D_MODEL,), jnp.float32)
    w_qkv = (jax.random.normal(shared_keys[2], (D_MODEL, KV_HEADS, QKV_WIDTH), jnp.float32) * D_MODEL ** -0.5).astype(jnp.bfloat16)
    w_out = (jax.random.normal(shared_keys[3], (N_HEADS * HEAD_DIM, D_MODEL), jnp.float32) * (N_HEADS * HEAD_DIM) ** -0.5).astype(jnp.bfloat16)
    w_gu = (jax.random.normal(shared_keys[4], (D_MODEL, 2, FF_DIM), jnp.float32) * D_MODEL ** -0.5).astype(jnp.bfloat16)
    w_down = (jax.random.normal(shared_keys[5], (FF_DIM, D_MODEL), jnp.float32) * FF_DIM ** -0.5).astype(jnp.bfloat16)
    return {'x_in': x_in, 'positions': positions, 'gain_one': gain_one, 'gain_two': gain_two, 'w_qkv': w_qkv, 'w_out': w_out, 'w_gu': w_gu, 'w_down': w_down, 'grad_out': grad_out}


def as_bf16(operand):
    return operand.astype(jnp.bfloat16).astype(jnp.float32)


def rope_tables(positions):
    inv_freq = ROPE_BASE ** (-jnp.arange(0, HEAD_DIM, 2, dtype=jnp.float32) / HEAD_DIM)
    angles = positions.astype(jnp.float32)[:, None] * inv_freq[None, :]
    angles = jnp.concatenate([angles, angles], axis=-1)
    return jnp.cos(angles), jnp.sin(angles)


def apply_rope(operand, cos_t, sin_t):
    half_dim = HEAD_DIM // 2
    rotated = jnp.concatenate([-operand[..., half_dim:], operand[..., :half_dim]], axis=-1)
    return as_bf16(operand * cos_t + rotated * sin_t)


def rms_norm(hidden, gain):
    inv_rms = lax.rsqrt(jnp.mean(hidden * hidden, axis=-1, keepdims=True) + EPSILON)
    return as_bf16(hidden * inv_rms * gain)


def group_attention(group_qkv, cos_t, sin_t):
    q_cut = Q_PER_KV * HEAD_DIM
    queries = group_qkv[..., :q_cut].reshape(BATCH, SEQ_LEN, Q_PER_KV, HEAD_DIM).transpose(0, 2, 1, 3)
    queries = apply_rope(queries, cos_t, sin_t)
    key_rot = apply_rope(group_qkv[..., q_cut:q_cut + HEAD_DIM], cos_t, sin_t)
    values = group_qkv[..., q_cut + HEAD_DIM:]
    scores = jnp.einsum('bgqh,bsh->bgqs', queries, key_rot) * HEAD_DIM ** -0.5
    causal = jnp.arange(SEQ_LEN)[:, None] >= jnp.arange(SEQ_LEN)[None, :]
    attn_probs = as_bf16(jax.nn.softmax(jnp.where(causal, scores, -1e30), axis=-1))
    attn_mix = as_bf16(jnp.einsum('bgqs,bsh->bqgh', attn_probs, values))
    return attn_mix.reshape(BATCH, SEQ_LEN, q_cut)


def reference(x_in, positions, gain_one, gain_two, w_qkv, w_out, w_gu, w_down, grad_out):
    cos_t, sin_t = rope_tables(positions)

    def forward(x_val, gain_a, gain_b, qkv_w, out_w, gu_w, down_w):
        normed = rms_norm(x_val, gain_a)
        qkv_all = as_bf16(jnp.einsum('td,dgc->tgc', normed, qkv_w))
        qkv_all = qkv_all.reshape(BATCH, SEQ_LEN, KV_HEADS, QKV_WIDTH).transpose(2, 0, 1, 3)
        attn_mix = lax.map(jax.checkpoint(lambda group_qkv: group_attention(group_qkv, cos_t, sin_t)), qkv_all)
        attn_mix = attn_mix.transpose(1, 2, 0, 3).reshape(TOKENS, N_HEADS * HEAD_DIM)
        hidden = as_bf16(x_val + as_bf16(jnp.dot(attn_mix, out_w, preferred_element_type=jnp.float32)))
        normed_two = rms_norm(hidden, gain_b)
        gate_up = as_bf16(jnp.einsum('td,dkf->tkf', normed_two, gu_w))
        act_out = as_bf16(jax.nn.silu(gate_up[:, 0]) * gate_up[:, 1])
        return as_bf16(hidden + as_bf16(jnp.dot(act_out, down_w, preferred_element_type=jnp.float32)))

    y_val, pullback = jax.vjp(forward, x_in.astype(jnp.float32), gain_one, gain_two, w_qkv.astype(jnp.float32), w_out.astype(jnp.float32), w_gu.astype(jnp.float32), w_down.astype(jnp.float32))
    grads = pullback(grad_out.astype(jnp.float32))
    return (y_val.astype(jnp.bfloat16), grads[0].astype(jnp.bfloat16), grads[1], grads[2], grads[3], grads[4], grads[5], grads[6])
```

```python
import functools

import jax
import jax.numpy as jnp
from jax import lax
from jax.experimental import pallas as pl
from jax.experimental.pallas import tpu as pltpu
from jax.sharding import PartitionSpec as P

EPSILON = 1e-5
ROPE_BASE = 10000.0
HEAD = 96
HALF = HEAD // 2
GROUP = 3 * HEAD
CHUNKS = 2
MESH = pl.DeviceIdType.MESH
BF = jnp.bfloat16
F32 = jnp.float32

AR_OUT, AR_R2, AR_Y, AR_R1 = range(4)


def dot_nn(lhs, rhs):
    return lax.dot_general(lhs, rhs, (((1,), (0,)), ((), ())), preferred_element_type=F32)


def dot_nt(lhs, rhs):
    return lax.dot_general(lhs, rhs, (((1,), (1,)), ((), ())), preferred_element_type=F32)


def dot_tn(lhs, rhs):
    return lax.dot_general(lhs, rhs, (((0,), (0,)), ((), ())), preferred_element_type=F32)


def add_bf(one, two):
    return (one.astype(F32) + two.astype(F32)).astype(BF)


def step(index, size):
    return pl.ds(pl.multiple_of(index * size, size), size)


def layer_kernel(x_hbm, dy_hbm, g1_ref, g2_ref, cos_ref, sin_ref, wqkv_hbm, wout_hbm, wgu_hbm, wdown_hbm,
                 y_hbm, dx_hbm, dg1_ref, dg2_ref, r1_hbm, dqkv_hbm, mix_hbm, dh_hbm, r2_hbm, dgu_hbm, act_hbm,
                 x_ref, dy_ref, wqkv_ref, wout_ref, wg_ref, wu_ref, wdown_ref, raw_ref,
                 r1_ref, r2_ref, h_ref, dh_ref, act_ref, dgu_ref, rot_ref, prob_ref, mix_ref, dqkv_ref, dx_ref,
                 inv1_ref, inv2_ref,
                 ga_send, ga_recv, qkv_send, qkv_recv, gu_send, gu_recv, gm_send, gm_recv, stat_send, stat_recv,
                 part_ref, sib_ref, half_ref, far_ref, full_ref,
                 load_sem, raw_sem, store_sem,
                 st_s, st_r, ga_s, ga_r, qk_s, qk_r, gu_s, gu_r, gm_s, gm_r, p1_s, p1_r, p2_s, p2_r, p3_s, p3_r):
    tokens, width = x_ref.shape
    full_width = 2 * width
    ff = wdown_ref.shape[0]
    heads = wqkv_ref.shape[0] // GROUP
    half_width = width // 2
    rows = tokens // CHUNKS
    emb = lax.axis_index("embed")
    hid = lax.axis_index("heads")
    core = lax.rem(hid, 2)
    sibling = {"heads": hid + 1 - 2 * core}
    across = {"heads": lax.rem(hid + 2, 4)}
    partner = {"embed": 1 - emb}

    barrier = pltpu.get_barrier_semaphore()
    for peer in (sibling, across, partner):
        pl.semaphore_signal(barrier, inc=1, device_id=peer, device_id_type=MESH)

    def load(src, dst, sem):
        return pltpu.make_async_copy(src, dst, load_sem.at[sem])

    loads = [load(x_hbm, x_ref, 0), load(dy_hbm, dy_ref, 1), load(wdown_hbm, wdown_ref, 2),
             load(wqkv_hbm, wqkv_ref, 3), load(wout_hbm, wout_ref, 4)]
    for copy in loads[:3]:
        copy.start()

    raw_rows = raw_ref.shape[1]
    raw_steps = wgu_hbm.shape[0] // raw_rows

    def raw_load(index, slot):
        return pltpu.make_async_copy(wgu_hbm.at[step(index, raw_rows)], raw_ref.at[slot], raw_sem.at[slot])

    def store(src, dst, sem):
        copy = pltpu.make_async_copy(src, dst, store_sem.at[sem])
        copy.start()
        return copy

    def send(src, dst, s_sem, r_sem, peer):
        return pltpu.make_async_remote_copy(src_ref=src, dst_ref=dst, send_sem=s_sem, recv_sem=r_sem,
                                            device_id=peer, device_id_type=MESH)

    def stat_copy(k):
        return send(stat_send.at[k], stat_recv.at[k], st_s.at[k], st_r.at[k], partner)

    ga_cols = ff // 8

    def ga_copy(k):
        cols = step(k, ga_cols)
        return send(ga_send.at[:, cols], ga_recv.at[:, cols], ga_s.at[k], ga_r.at[k], partner)

    def qkv_copy(j):
        r = step(j, GROUP)
        return send(qkv_send.at[r], qkv_recv.at[r], qk_s.at[j], qk_r.at[j], partner)

    gu_cols = ff // 2

    def gu_copy(c, p):
        col = (p % 2) * ff + (p // 2) * gu_cols
        at = (pl.ds(c * rows, rows), pl.ds(col, gu_cols))
        return send(gu_send.at[at], gu_recv.at[at], gu_s.at[4 * c + p], gu_r.at[4 * c + p], partner)

    def gm_copy(c):
        at = (slice(None), pl.ds(c * rows, rows))
        return send(gm_send.at[at], gm_recv.at[at], gm_s.at[c], gm_r.at[c], partner)

    own = pl.ds(pl.multiple_of(core * half_width, half_width), half_width)
    other = pl.ds(pl.multiple_of((1 - core) * half_width, half_width), half_width)

    def p1_copy(i, c):
        r = pl.ds(c * rows, rows)
        k = i * CHUNKS + c
        return send(part_ref.at[i, r, other], sib_ref.at[i, r], p1_s.at[k], p1_r.at[k], sibling)

    def p2_copy(i, c):
        r = pl.ds(c * rows, rows)
        k = i * CHUNKS + c
        return send(half_ref.at[i, r], far_ref.at[i, r], p2_s.at[k], p2_r.at[k], across)

    def p3_copy(i, c):
        r = pl.ds(c * rows, rows)
        k = i * CHUNKS + c
        return send(full_ref.at[i, r, own], full_ref.at[i, r, own], p3_s.at[k], p3_r.at[k], sibling)

    def stage2(i, c):
        r = pl.ds(c * rows, rows)
        p1_copy(i, c).wait_recv()
        half_ref[i, r, :] = add_bf(part_ref[i, r, own], sib_ref[i, r, :])
        p2_copy(i, c).start()

    def stage3(i, c):
        r = pl.ds(c * rows, rows)
        p2_copy(i, c).wait_recv()
        full_ref[i, r, own] = add_bf(half_ref[i, r, :], far_ref[i, r, :])
        p3_copy(i, c).start()

    def stage4(i, c):
        p3_copy(i, c).wait_recv()

    def stat_put(k, col, n):
        flat = jnp.broadcast_to(col, (n, 128)).T[0:8, :]
        stat_send[k, :, 0:n] = flat
        stat_copy(k).start()

    def stat_get(k, n):
        stat_copy(k).wait_recv()
        total = stat_send[k, 0:1, 0:n] + stat_recv[k, 0:1, 0:n]
        return jnp.broadcast_to(total, (128, n)).T[:, 0:1]

    loads[0].wait()
    x32 = x_ref[...].astype(F32)
    sq1 = jnp.sum(x32 * x32, axis=-1, keepdims=True)
    pl.semaphore_wait(barrier, 3)
    stat_put(0, sq1, tokens)
    for copy in loads[3:]:
        copy.start()
    for slot in range(2):
        raw_load(slot, slot).start()

    loads[1].wait()
    loads[2].wait()

    def ga_body(k, carry):
        cols = step(k, ga_cols)
        ga_send[:, cols] = dot_nt(dy_ref[...], wdown_ref[cols, :]).astype(BF)

        @pl.when(k == 0)
        def _():
            ga_copy(k).start()
        return carry

    lax.fori_loop(0, 8, ga_body, 0)

    inv1 = lax.rsqrt(stat_get(0, tokens) / full_width + EPSILON)
    inv1_ref[...] = inv1
    r1_ref[...] = (x_ref[...].astype(F32) * inv1 * g1_ref[...]).astype(BF)
    stores = [store(r1_ref, r1_hbm, 0)]

    loads[3].wait()

    def qkv_body(j, carry):
        r = step(j, GROUP)
        qkv_send[r, :] = dot_nt(wqkv_ref[r, :], r1_ref[...]).astype(BF)
        qkv_copy(j).start()
        return carry

    lax.fori_loop(0, heads, qkv_body, 0)
    for k in range(1, 5):
        ga_copy(k).start()

    row_i = lax.broadcasted_iota(jnp.int32, (256, 256), 0)
    col_i = lax.broadcasted_iota(jnp.int32, (256, 256), 1)
    perm = (col_i == (row_i % 8) * 32 + row_i // 8).astype(F32).astype(BF)
    blocks = raw_rows // 512

    def raw_body(i, carry):
        slot = lax.rem(i, 2)
        raw_load(i, slot).wait()

        def block_body(b, inner):
            for u in range(4):
                base = pl.multiple_of(b * 2048 + u * 512, 512)
                pair = jnp.concatenate([raw_ref[slot, pl.ds(base, 256), :], raw_ref[slot, pl.ds(base + 256, 256), :]], axis=1)
                out = dot_nn(perm, pair)
                d = pl.ds(pl.multiple_of(i * (raw_rows // 32) + b * 64 + u * 16, 16), 16)
                for t in range(16):
                    for k, dst in ((0, wg_ref), (1, wu_ref)):
                        r = (2 * t + k) * 8
                        both = jnp.concatenate([out[r:r + 8, 0:128], out[r:r + 8, 128:256]], axis=0)
                        dst[d, t * 128:(t + 1) * 128] = both.astype(BF)
            return inner

        lax.fori_loop(0, blocks // 4, block_body, 0)

        @pl.when(i + 2 < raw_steps)
        def _():
            raw_load(i + 2, slot).start()
        return carry

    lax.fori_loop(0, raw_steps, raw_body, 0)

    scale = HEAD ** -0.5
    causal = (lax.broadcasted_iota(jnp.int32, (tokens, tokens), 0) <= lax.broadcasted_iota(jnp.int32, (tokens, tokens), 1))

    def rope(v, cos_t, sin_t):
        v = v.astype(F32)
        one, two = v[0:HALF], v[HALF:HEAD]
        return jnp.concatenate([one * cos_t - two * sin_t, two * cos_t + one * sin_t], axis=0).astype(BF)

    def unrope(v, cos_t, sin_t):
        v = v.astype(F32)
        one, two = v[0:HALF], v[HALF:HEAD]
        return jnp.concatenate([one * cos_t + two * sin_t, two * cos_t - one * sin_t], axis=0).astype(BF)

    def attn_body(j, carry):
        qkv_copy(j).wait_recv()
        base = pl.multiple_of(j * GROUP, 32)
        r_q, r_k, r_v = (pl.ds(base + n * HEAD, HEAD) for n in range(3))
        cos_t, sin_t = cos_ref[...], sin_ref[...]
        q = rope(add_bf(qkv_send[r_q, :], qkv_recv[r_q, :]), cos_t, sin_t)
        k = rope(add_bf(qkv_send[r_k, :], qkv_recv[r_k, :]), cos_t, sin_t)
        v = add_bf(qkv_send[r_v, :], qkv_recv[r_v, :])
        rot_ref[r_q, :] = q
        rot_ref[r_k, :] = k
        rot_ref[r_v, :] = v
        scores = jnp.where(causal, dot_tn(k, q) * scale, -1e30)
        weight = jnp.exp(scores - jnp.max(scores, axis=0, keepdims=True))
        prob = weight / jnp.sum(weight, axis=0, keepdims=True)
        prob_ref[j] = prob
        mix_ref[pl.ds(pl.multiple_of(j * HEAD, 32), HEAD), :] = dot_nn(v, prob.astype(BF)).astype(BF)
        return carry

    lax.fori_loop(0, heads, attn_body, 0)
    stores.append(store(mix_ref, mix_hbm, 1))

    loads[4].wait()
    for c in range(CHUNKS):
        r = pl.ds(c * rows, rows)
        part_ref[AR_OUT, r, :] = dot_tn(mix_ref[:, c * rows:(c + 1) * rows], wout_ref[...]).astype(BF)
        p1_copy(AR_OUT, c).start()
    for c in range(CHUNKS):
        stage2(AR_OUT, c)
    for c in range(CHUNKS):
        stage3(AR_OUT, c)
    for c in range(CHUNKS):
        r = pl.ds(c * rows, rows)
        stage4(AR_OUT, c)
        h = add_bf(x_ref[r, :], full_ref[AR_OUT, r, :])
        h_ref[r, :] = h
        h32 = h.astype(F32)
        stat_put(1 + c, jnp.sum(h32 * h32, axis=-1, keepdims=True), rows)
    for k in range(5, 8):
        ga_copy(k).start()

    tile = 512
    for c in range(CHUNKS):
        r = pl.ds(c * rows, rows)
        inv2 = lax.rsqrt(stat_get(1 + c, rows) / full_width + EPSILON)
        inv2_ref[r, :] = inv2
        r2 = (h_ref[r, :].astype(F32) * inv2 * g2_ref[...]).astype(BF)
        r2_ref[r, :] = r2
        for p in range(4):
            w_ref = (wg_ref, wu_ref)[p % 2]

            def gu_body(n, carry, c=c, p=p, w_ref=w_ref):
                src = pl.ds(pl.multiple_of((p // 2) * gu_cols + n * tile, tile), tile)
                dst = pl.ds(pl.multiple_of((p % 2) * ff + (p // 2) * gu_cols + n * tile, tile), tile)
                gu_send[pl.ds(c * rows, rows), dst] = dot_nn(r2_ref[pl.ds(c * rows, rows), :], w_ref[:, src]).astype(BF)
                return carry

            lax.fori_loop(0, gu_cols // tile, gu_body, 0)
            gu_copy(c, p).start()
    stores.append(store(r2_ref, r2_hbm, 2))

    for k in range(8):
        ga_copy(k).wait_recv()

    def mlp_chunk(c):
        r = pl.ds(c * rows, rows)
        for hf in range(2):
            gu_copy(c, 2 * hf).wait_recv()
            gu_copy(c, 2 * hf + 1).wait_recv()

            def act_body(n, carry, hf=hf):
                cg = pl.ds(pl.multiple_of(hf * gu_cols + n * 256, 256), 256)
                cu = pl.ds(pl.multiple_of(ff + hf * gu_cols + n * 256, 256), 256)
                gate = add_bf(gu_send[r, cg], gu_recv[r, cg]).astype(F32)
                up = add_bf(gu_send[r, cu], gu_recv[r, cu]).astype(F32)
                ga = add_bf(ga_send[r, cg], ga_recv[r, cg]).astype(F32)
                sig = 1.0 / (1.0 + jnp.exp(-gate))
                silu = gate * sig
                act_ref[r, cg] = (silu * up).astype(BF)
                dgu_ref[r, cg] = (ga * up * (sig * (1.0 + gate * (1.0 - sig)))).astype(BF)
                dgu_ref[r, cu] = (ga * silu).astype(BF)
                return carry

            lax.fori_loop(0, gu_cols // 256, act_body, 0)

        def r2_body(n, carry):
            w = step(n, tile)
            part_ref[AR_R2, r, w] = (dot_nt(dgu_ref[r, 0:ff], wg_ref[w, :]) + dot_nt(dgu_ref[r, ff:2 * ff], wu_ref[w, :])).astype(BF)
            return carry

        lax.fori_loop(0, width // tile, r2_body, 0)
        p1_copy(AR_R2, c).start()

    def down_chunk(c):
        r = pl.ds(c * rows, rows)

        def down_body(n, carry):
            w = step(n, tile)
            part_ref[AR_Y, r, w] = dot_nn(act_ref[r, :], wdown_ref[:, w]).astype(BF)
            return carry

        lax.fori_loop(0, width // tile, down_body, 0)
        p1_copy(AR_Y, c).start()

    dg2_ref[...] = jnp.zeros_like(dg2_ref)

    def norm2_back(c):
        r = pl.ds(c * rows, rows)
        stage4(AR_R2, c)
        gin = full_ref[AR_R2, r, :].astype(F32)
        unit = h_ref[r, :].astype(F32) * inv2_ref[r, :]
        dg2_ref[...] += jnp.sum(gin * unit, axis=0, keepdims=True)
        stat_put(3 + c, jnp.sum(gin * g2_ref[...] * unit, axis=-1, keepdims=True), rows)

    def hidden_back(c):
        r = pl.ds(c * rows, rows)
        dots = stat_get(3 + c, rows)
        inv2 = inv2_ref[r, :]
        unit = h_ref[r, :].astype(F32) * inv2
        scaled = full_ref[AR_R2, r, :].astype(F32) * g2_ref[...]
        norm = inv2 * (scaled - unit * (dots / full_width))
        dh_ref[r, :] = (dy_ref[r, :].astype(F32) + norm).astype(BF)
        gm_send[:, c * rows:(c + 1) * rows] = dot_nt(wout_ref[...], dh_ref[r, :]).astype(BF)
        gm_copy(c).start()

    def y_chunk(c):
        r = pl.ds(c * rows, rows)
        stage4(AR_Y, c)
        h_ref[r, :] = add_bf(h_ref[r, :], full_ref[AR_Y, r, :])

    mlp_chunk(0)
    down_chunk(0)
    stage2(AR_R2, 0)
    stage3(AR_R2, 0)
    stage2(AR_Y, 0)
    norm2_back(0)
    stage3(AR_Y, 0)
    mlp_chunk(1)
    stores.append(store(dgu_ref, dgu_hbm, 3))
    stores.append(store(act_ref, act_hbm, 4))
    stage2(AR_R2, 1)
    hidden_back(0)
    stage3(AR_R2, 1)
    norm2_back(1)
    down_chunk(1)
    hidden_back(1)
    stores.append(store(dh_ref, dh_hbm, 5))
    stage2(AR_Y, 1)
    y_chunk(0)
    stage3(AR_Y, 1)
    y_chunk(1)
    stores.append(store(h_ref, y_hbm, 6))

    for c in range(CHUNKS):
        gm_copy(c).wait_recv()

    def back_body(j, carry):
        base = pl.multiple_of(j * GROUP, 32)
        r_q, r_k, r_v = (pl.ds(base + n * HEAD, HEAD) for n in range(3))
        r_a = pl.ds(pl.multiple_of(j * HEAD, 32), HEAD)
        cos_t, sin_t = cos_ref[...], sin_ref[...]
        da = add_bf(gm_send[r_a, :], gm_recv[r_a, :])
        q, k, v = rot_ref[r_q, :], rot_ref[r_k, :], rot_ref[r_v, :]
        prob = prob_ref[j]
        dp = dot_tn(v, da).astype(BF).astype(F32)
        dqkv_ref[r_v, :] = dot_nt(da, prob.astype(BF)).astype(BF)
        weighted = prob * dp
        ds = ((weighted - prob * jnp.sum(weighted, axis=0, keepdims=True)) * scale).astype(BF)
        dqkv_ref[r_q, :] = unrope(dot_nn(k, ds).astype(BF), cos_t, sin_t)
        dqkv_ref[r_k, :] = unrope(dot_nt(q, ds).astype(BF), cos_t, sin_t)
        return carry

    lax.fori_loop(0, heads, back_body, 0)
    stores.append(store(dqkv_ref, dqkv_hbm, 7))

    for c in range(CHUNKS):
        r = pl.ds(c * rows, rows)
        part_ref[AR_R1, r, :] = dot_tn(dqkv_ref[:, c * rows:(c + 1) * rows], wqkv_ref[...]).astype(BF)
        p1_copy(AR_R1, c).start()
    for c in range(CHUNKS):
        stage2(AR_R1, c)
    for c in range(CHUNKS):
        stage3(AR_R1, c)
    dg1_ref[...] = jnp.zeros_like(dg1_ref)
    for c in range(CHUNKS):
        r = pl.ds(c * rows, rows)
        stage4(AR_R1, c)
        gin = full_ref[AR_R1, r, :].astype(F32)
        unit = x_ref[r, :].astype(F32) * inv1_ref[r, :]
        dg1_ref[...] += jnp.sum(gin * unit, axis=0, keepdims=True)
        stat_put(5 + c, jnp.sum(gin * g1_ref[...] * unit, axis=-1, keepdims=True), rows)
    for c in range(CHUNKS):
        r = pl.ds(c * rows, rows)
        dots = stat_get(5 + c, rows)
        inv1 = inv1_ref[r, :]
        unit = x_ref[r, :].astype(F32) * inv1
        scaled = full_ref[AR_R1, r, :].astype(F32) * g1_ref[...]
        norm = inv1 * (scaled - unit * (dots / full_width))
        dx_ref[r, :] = (dh_ref[r, :].astype(F32) + norm).astype(BF)
    stores.append(store(dx_ref, dx_hbm, 8))

    for k in range(7):
        stat_copy(k).wait_send()
    for k in range(8):
        ga_copy(k).wait_send()
    for j in range(heads):
        qkv_copy(j).wait_send()
    for c in range(CHUNKS):
        for p in range(4):
            gu_copy(c, p).wait_send()
        gm_copy(c).wait_send()
        for i in range(4):
            p1_copy(i, c).wait_send()
            p2_copy(i, c).wait_send()
            p3_copy(i, c).wait_send()
    for copy in stores:
        copy.wait()


def run_layer(x_in, cos_t, sin_t, gain_one, gain_two, w_qkv, w_out, w_gu, w_down, grad_out):
    tokens, width = x_in.shape
    ff = w_down.shape[0]
    chans = w_qkv.shape[0]
    mix = w_out.shape[0]
    heads = mix // HEAD
    rows = tokens // CHUNKS
    act = lambda n, dtype=BF: jax.ShapeDtypeStruct((tokens, n), dtype)
    any_spec = pl.BlockSpec(memory_space=pl.ANY)
    vmem_spec = pl.BlockSpec(memory_space=pltpu.VMEM)
    raw_rows = 128 * 32
    scratch = [
        pltpu.VMEM((tokens, width), BF), pltpu.VMEM((tokens, width), BF),
        pltpu.VMEM((chans, width), BF), pltpu.VMEM((mix, width), BF),
        pltpu.VMEM((width, ff), BF), pltpu.VMEM((width, ff), BF), pltpu.VMEM((ff, width), BF),
        pltpu.VMEM((2, raw_rows, 128), BF),
        pltpu.VMEM((tokens, width), BF), pltpu.VMEM((tokens, width), BF), pltpu.VMEM((tokens, width), BF), pltpu.VMEM((tokens, width), BF),
        pltpu.VMEM((tokens, ff), BF), pltpu.VMEM((tokens, 2 * ff), BF),
        pltpu.VMEM((chans, tokens), BF), pltpu.VMEM((heads, tokens, tokens), F32), pltpu.VMEM((mix, tokens), BF), pltpu.VMEM((chans, tokens), BF),
        pltpu.VMEM((tokens, width), BF),
        pltpu.VMEM((tokens, 1), F32), pltpu.VMEM((tokens, 1), F32),
        pltpu.VMEM((tokens, ff), BF), pltpu.VMEM((tokens, ff), BF),
        pltpu.VMEM((chans, tokens), BF), pltpu.VMEM((chans, tokens), BF),
        pltpu.VMEM((tokens, 2 * ff), BF), pltpu.VMEM((tokens, 2 * ff), BF),
        pltpu.VMEM((mix, tokens), BF), pltpu.VMEM((mix, tokens), BF),
        pltpu.VMEM((7, 8, tokens), F32), pltpu.VMEM((7, 8, tokens), F32),
        pltpu.VMEM((4, tokens, width), BF), pltpu.VMEM((4, tokens, width // 2), BF), pltpu.VMEM((4, tokens, width // 2), BF),
        pltpu.VMEM((4, tokens, width // 2), BF), pltpu.VMEM((4, tokens, width), BF),
        pltpu.SemaphoreType.DMA((5,)), pltpu.SemaphoreType.DMA((2,)), pltpu.SemaphoreType.DMA((9,)),
    ]
    for n in (7, 8, heads, 4 * CHUNKS, CHUNKS, 4 * CHUNKS, 4 * CHUNKS, 4 * CHUNKS):
        scratch += [pltpu.SemaphoreType.DMA((n,)), pltpu.SemaphoreType.DMA((n,))]
    vec = jax.ShapeDtypeStruct((1, width), F32)
    return pl.pallas_call(
        layer_kernel,
        name="layer",
        out_shape=(act(width), act(width), vec, vec, act(width), jax.ShapeDtypeStruct((chans, tokens), BF),
                   jax.ShapeDtypeStruct((mix, tokens), BF), act(width), act(width), act(2 * ff), act(ff)),
        in_specs=[any_spec, any_spec, vmem_spec, vmem_spec, vmem_spec, vmem_spec, any_spec, any_spec, any_spec, any_spec],
        out_specs=(any_spec, any_spec, vmem_spec, vmem_spec) + (any_spec,) * 7,
        scratch_shapes=scratch,
        compiler_params=pltpu.CompilerParams(collective_id=0, has_side_effects=True, vmem_limit_bytes=67000000),
    )(x_in, grad_out, gain_one, gain_two, cos_t, sin_t, w_qkv, w_out, w_gu, w_down)


def product_call(lhs, rhs, block, transposed):
    n = lhs.shape[1] if transposed else lhs.shape[0]
    tokens, width = rhs.shape

    def body(lhs_ref, rhs_ref, out_ref):
        out_ref[...] = (dot_tn if transposed else dot_nn)(lhs_ref[...], rhs_ref[...])

    lhs_spec = pl.BlockSpec((tokens, block), lambda i: (0, i)) if transposed else pl.BlockSpec((block, tokens), lambda i: (i, 0))
    return pl.pallas_call(
        body,
        grid=(n // block,),
        in_specs=[lhs_spec, pl.BlockSpec((tokens, width), lambda i: (0, 0))],
        out_specs=pl.BlockSpec((block, width), lambda i: (i, 0)),
        out_shape=jax.ShapeDtypeStruct((n, width), F32),
    )(lhs, rhs)


def gate_up_grad(r2, dgu):
    tokens, width = r2.shape
    ff = dgu.shape[1] // 2
    block = 128
    pad = 40
    steps = width // block

    def body(r2_ref, dgu_ref, out_hbm, stage_ref, sem):
        i = pl.program_id(0)
        slot = lax.rem(i, 2)

        def out_copy(index, s):
            return pltpu.make_async_copy(stage_ref.at[s, :, 0:32, :], out_hbm.at[pl.ds(index * block, block)], sem.at[s])

        @pl.when(i >= 2)
        def _():
            out_copy(i - 2, slot).wait()

        lhs = r2_ref[...].T
        for k in range(2):
            for n in range(ff // 512):
                val = dot_nn(lhs, dgu_ref[:, k * ff + n * 512:k * ff + (n + 1) * 512])
                for t in range(4):
                    row = 2 * (4 * n + t) + k
                    stage_ref[slot, :, row, :] = val[:, t * 128:(t + 1) * 128]
        out_copy(i, slot).start()

        @pl.when(i == steps - 1)
        def _():
            out_copy(i - 1, 1 - slot).wait()
            out_copy(i, slot).wait()

    out = pl.pallas_call(
        body,
        grid=(steps,),
        in_specs=[pl.BlockSpec((tokens, 128), lambda i: (0, i)) if block == 128 else pl.BlockSpec((None, tokens, block), lambda i: (i, 0, 0)),
                  pl.BlockSpec((tokens, 2 * ff), lambda i: (0, 0))],
        out_specs=pl.BlockSpec(memory_space=pl.ANY),
        out_shape=jax.ShapeDtypeStruct((width, 32, 128), F32),
        scratch_shapes=[pltpu.VMEM((2, block, pad, 128), F32), pltpu.SemaphoreType.DMA((2,))],
        compiler_params=pltpu.CompilerParams(vmem_limit_bytes=48 << 20),
    )(r2 if block == 128 else r2.reshape(tokens, steps, block).transpose(1, 0, 2), dgu)
    return out.reshape(width, 16, 2, 128).transpose(0, 2, 1, 3).reshape(width, 2, ff)


def rope_tables(positions):
    inv_freq = ROPE_BASE ** (-jnp.arange(0, HEAD, 2, dtype=F32) / HEAD)
    angles = inv_freq[:, None] * positions.astype(F32)[None, :]
    return jnp.cos(angles), jnp.sin(angles)


def solution(mesh):
    def per_device(x_in, positions, gain_one, gain_two, w_qkv, w_out, w_gu, w_down, grad_out):
        width, groups, chans = w_qkv.shape
        ff = w_down.shape[0]
        cos_t, sin_t = rope_tables(positions)
        qkv_rows = w_qkv.transpose(1, 2, 0).reshape(groups * chans, width)
        gu_rows = w_gu.reshape(width, 2, ff // 128, 128).transpose(0, 2, 1, 3).reshape(width * 2 * (ff // 128), 128)
        y, dx, dg1, dg2, r1, dqkv, mix, dh, r2, dgu, act = run_layer(
            x_in, cos_t, sin_t, gain_one.reshape(1, width), gain_two.reshape(1, width), qkv_rows, w_out, gu_rows, w_down, grad_out)
        d_down = product_call(act, grad_out, 256, True)
        d_gu = gate_up_grad(r2, dgu)
        d_out = product_call(mix, dh, 256, False)
        d_qkv = product_call(dqkv, r1, 256, False).reshape(groups, chans, width).transpose(2, 0, 1)
        return y, dx, dg1.reshape(width), dg2.reshape(width), d_qkv, d_out, d_gu, d_down

    act_spec = P('dp', 'embed')
    in_specs = (act_spec, P('dp'), P('embed'), P('embed'), P('embed', 'heads', None), P('heads', 'embed'), P('embed', None, 'heads'), P('heads', 'embed'), act_spec)
    out_specs = (act_spec, act_spec, P(('dp', 'embed')), P(('dp', 'embed')), P(('dp', 'embed'), 'heads', None), P(('dp', 'heads'), 'embed'), P(('dp', 'embed'), None, 'heads'), P(('dp', 'heads'), 'embed'))
    return jax.shard_map(per_device, mesh=mesh, in_specs=in_specs, out_specs=out_specs, check_vma=False)
```

```python
import math

import jax
import jax.numpy as jnp
from jax import lax
from jax.experimental import pallas as pl
from jax.experimental.pallas import tpu as pltpu
from jax.sharding import PartitionSpec as P

EPSILON = 1e-5
ROPE_BASE = 10000.0
HEAD = 96
HALF = HEAD // 2
GROUP = 3 * HEAD
CHUNKS = 2
MESH = pl.DeviceIdType.MESH
BF = jnp.bfloat16
F32 = jnp.float32

AR_OUT, AR_R2, AR_Y, AR_R1 = range(4)


def dot_nn(lhs, rhs):
    return lax.dot_general(lhs, rhs, (((1,), (0,)), ((), ())), preferred_element_type=F32)


def dot_nt(lhs, rhs):
    return lax.dot_general(lhs, rhs, (((1,), (1,)), ((), ())), preferred_element_type=F32)


def dot_tn(lhs, rhs):
    return lax.dot_general(lhs, rhs, (((0,), (0,)), ((), ())), preferred_element_type=F32)


def add_bf(one, two):
    return (one.astype(F32) + two.astype(F32)).astype(BF)


def step(index, size):
    return pl.ds(pl.multiple_of(index * size, size), size)


def layer_kernel(x_hbm, dy_hbm, g1_in, g2_in, pos_in, wqkv_hbm, wout_hbm, wgu_hbm, wdown_hbm,
                 y_hbm, dx_hbm, dg1_ref, dg2_ref, r1_hbm, dqkv_hbm, mix_hbm, dh_hbm, r2_hbm, dgu_hbm, act_hbm,
                 x_ref, dy_ref, wqkv_ref, wout_ref, wg_ref, wu_ref, wdown_ref, raw_ref,
                 g1_ref, g2_ref, cos_ref, sin_ref, r1_ref, r2_ref, h_ref, dh_ref, act_ref, dgu_ref, rot_ref, prob_ref, mix_ref, dqkv_ref, dx_ref,
                 inv1_ref, inv2_ref,
                 ga_send, ga_recv, qkv_send, qkv_recv, gu_send, gu_recv, gm_send, gm_recv, stat_send, stat_recv,
                 part_ref, sib_ref, half_ref, far_ref, full_ref,
                 load_sem, raw_sem, store_sem,
                 st_s, st_r, ga_s, ga_r, qk_s, qk_r, gu_s, gu_r, gm_s, gm_r, p1_s, p1_r, p2_s, p2_r, p3_s, p3_r):
    tokens, width = x_ref.shape
    full_width = 2 * width
    ff = wdown_ref.shape[0]
    heads = wqkv_ref.shape[0] // GROUP
    half_width = width // 2
    rows = tokens // CHUNKS
    emb = lax.axis_index("embed")
    hid = lax.axis_index("heads")
    core = lax.rem(hid, 2)
    sibling = {"heads": hid + 1 - 2 * core}
    across = {"heads": lax.rem(hid + 2, 4)}
    partner = {"embed": 1 - emb}

    barrier = pltpu.get_barrier_semaphore()
    for peer in (sibling, across, partner):
        pl.semaphore_signal(barrier, inc=1, device_id=peer, device_id_type=MESH)

    def load(src, dst, sem):
        return pltpu.make_async_copy(src, dst, load_sem.at[sem])

    loads = [load(x_hbm, x_ref, 0), load(dy_hbm, dy_ref, 1), load(wdown_hbm, wdown_ref, 2),
             load(wqkv_hbm, wqkv_ref, 3), load(wout_hbm, wout_ref, 4)]
    for copy in loads[:3]:
        copy.start()

    raw_rows = raw_ref.shape[1]
    raw_steps = wgu_hbm.shape[0] // raw_rows

    def raw_load(index, slot):
        return pltpu.make_async_copy(wgu_hbm.at[step(index, raw_rows)], raw_ref.at[slot], raw_sem.at[slot])

    def store(src, dst, sem):
        copy = pltpu.make_async_copy(src, dst, store_sem.at[sem])
        copy.start()
        return copy

    def send(src, dst, s_sem, r_sem, peer):
        return pltpu.make_async_remote_copy(src_ref=src, dst_ref=dst, send_sem=s_sem, recv_sem=r_sem,
                                            device_id=peer, device_id_type=MESH)

    def stat_copy(k):
        return send(stat_send.at[k], stat_recv.at[k], st_s.at[k], st_r.at[k], partner)

    ga_cols = ff // 8

    def ga_copy(k):
        cols = step(k, ga_cols)
        return send(ga_send.at[:, cols], ga_recv.at[:, cols], ga_s.at[k], ga_r.at[k], partner)

    def qkv_copy(j):
        r = step(j, GROUP)
        return send(qkv_send.at[r], qkv_recv.at[r], qk_s.at[j], qk_r.at[j], partner)

    gu_cols = ff // 2

    def gu_copy(c, p):
        col = (p % 2) * ff + (p // 2) * gu_cols
        at = (pl.ds(c * rows, rows), pl.ds(col, gu_cols))
        return send(gu_send.at[at], gu_recv.at[at], gu_s.at[4 * c + p], gu_r.at[4 * c + p], partner)

    def gm_copy(c):
        at = (slice(None), pl.ds(c * rows, rows))
        return send(gm_send.at[at], gm_recv.at[at], gm_s.at[c], gm_r.at[c], partner)

    own = pl.ds(pl.multiple_of(core * half_width, half_width), half_width)
    other = pl.ds(pl.multiple_of((1 - core) * half_width, half_width), half_width)

    def p1_copy(i, c):
        r = pl.ds(c * rows, rows)
        k = i * CHUNKS + c
        return send(part_ref.at[i, r, other], sib_ref.at[i, r], p1_s.at[k], p1_r.at[k], sibling)

    def p2_copy(i, c):
        r = pl.ds(c * rows, rows)
        k = i * CHUNKS + c
        return send(half_ref.at[i, r], far_ref.at[i, r], p2_s.at[k], p2_r.at[k], across)

    def p3_copy(i, c):
        r = pl.ds(c * rows, rows)
        k = i * CHUNKS + c
        return send(full_ref.at[i, r, own], full_ref.at[i, r, own], p3_s.at[k], p3_r.at[k], sibling)

    def stage2(i, c):
        r = pl.ds(c * rows, rows)
        p1_copy(i, c).wait_recv()
        half_ref[i, r, :] = add_bf(part_ref[i, r, own], sib_ref[i, r, :])
        p2_copy(i, c).start()

    def stage3(i, c):
        r = pl.ds(c * rows, rows)
        p2_copy(i, c).wait_recv()
        full_ref[i, r, own] = add_bf(half_ref[i, r, :], far_ref[i, r, :])
        p3_copy(i, c).start()

    def stage4(i, c):
        p3_copy(i, c).wait_recv()

    def stat_put(k, col, n):
        flat = jnp.broadcast_to(col, (n, 128)).T[0:8, :]
        stat_send[k, :, 0:n] = flat
        stat_copy(k).start()

    def stat_get(k, n):
        stat_copy(k).wait_recv()
        total = stat_send[k, 0:1, 0:n] + stat_recv[k, 0:1, 0:n]
        return jnp.broadcast_to(total, (128, n)).T[:, 0:1]

    g1_ref[...] = g1_in[...].reshape(1, width)
    g2_ref[...] = g2_in[...].reshape(1, width)
    loads[0].wait()
    x32 = x_ref[...].astype(F32)
    sq1 = jnp.sum(x32 * x32, axis=-1, keepdims=True)
    pl.semaphore_wait(barrier, 3)
    stat_put(0, sq1, tokens)
    for copy in loads[3:]:
        copy.start()
    for slot in range(2):
        raw_load(slot, slot).start()

    loads[1].wait()
    loads[2].wait()

    def ga_body(k, carry):
        cols = step(k, ga_cols)
        ga_send[:, cols] = dot_nt(dy_ref[...], wdown_ref[cols, :]).astype(BF)

        @pl.when(k == 0)
        def _():
            ga_copy(k).start()
        return carry

    lax.fori_loop(0, 8, ga_body, 0)

    place = pos_in[...].reshape(1, tokens).astype(F32)
    pair_i = lax.broadcasted_iota(jnp.int32, (HALF, 1), 0).astype(F32)
    angles = jnp.exp(pair_i * (-2.0 * math.log(ROPE_BASE) / HEAD)) * place
    cos_ref[...] = jnp.cos(angles)
    sin_ref[...] = jnp.sin(angles)

    inv1 = lax.rsqrt(stat_get(0, tokens) / full_width + EPSILON)
    inv1_ref[...] = inv1
    r1_ref[...] = (x_ref[...].astype(F32) * inv1 * g1_ref[...]).astype(BF)
    stores = [store(r1_ref, r1_hbm, 0)]

    loads[3].wait()

    def qkv_body(j, carry):
        r = step(j, GROUP)
        qkv_send[r, :] = dot_nt(wqkv_ref[r, :], r1_ref[...]).astype(BF)
        qkv_copy(j).start()
        return carry

    lax.fori_loop(0, heads, qkv_body, 0)
    for k in range(1, 5):
        ga_copy(k).start()

    row_i = lax.broadcasted_iota(jnp.int32, (256, 256), 0)
    col_i = lax.broadcasted_iota(jnp.int32, (256, 256), 1)
    perm = (col_i == (row_i % 8) * 32 + row_i // 8).astype(F32).astype(BF)
    blocks = raw_rows // 512

    def raw_body(i, carry):
        slot = lax.rem(i, 2)
        raw_load(i, slot).wait()

        def block_body(b, inner):
            for u in range(4):
                base = pl.multiple_of(b * 2048 + u * 512, 512)
                pair = jnp.concatenate([raw_ref[slot, pl.ds(base, 256), :], raw_ref[slot, pl.ds(base + 256, 256), :]], axis=1)
                out = dot_nn(perm, pair)
                d = pl.ds(pl.multiple_of(i * (raw_rows // 32) + b * 64 + u * 16, 16), 16)
                for t in range(16):
                    for k, dst in ((0, wg_ref), (1, wu_ref)):
                        r = (2 * t + k) * 8
                        both = jnp.concatenate([out[r:r + 8, 0:128], out[r:r + 8, 128:256]], axis=0)
                        dst[d, t * 128:(t + 1) * 128] = both.astype(BF)
            return inner

        lax.fori_loop(0, blocks // 4, block_body, 0)

        @pl.when(i + 2 < raw_steps)
        def _():
            raw_load(i + 2, slot).start()
        return carry

    lax.fori_loop(0, raw_steps, raw_body, 0)

    scale = HEAD ** -0.5
    causal = (lax.broadcasted_iota(jnp.int32, (tokens, tokens), 0) <= lax.broadcasted_iota(jnp.int32, (tokens, tokens), 1))

    def rope(v, cos_t, sin_t):
        v = v.astype(F32)
        one, two = v[0:HALF], v[HALF:HEAD]
        return jnp.concatenate([one * cos_t - two * sin_t, two * cos_t + one * sin_t], axis=0).astype(BF)

    def unrope(v, cos_t, sin_t):
        v = v.astype(F32)
        one, two = v[0:HALF], v[HALF:HEAD]
        return jnp.concatenate([one * cos_t + two * sin_t, two * cos_t - one * sin_t], axis=0).astype(BF)

    def attn_body(j, carry):
        qkv_copy(j).wait_recv()
        base = pl.multiple_of(j * GROUP, 32)
        r_q, r_k, r_v = (pl.ds(base + n * HEAD, HEAD) for n in range(3))
        cos_t, sin_t = cos_ref[...], sin_ref[...]
        q = rope(add_bf(qkv_send[r_q, :], qkv_recv[r_q, :]), cos_t, sin_t)
        k = rope(add_bf(qkv_send[r_k, :], qkv_recv[r_k, :]), cos_t, sin_t)
        v = add_bf(qkv_send[r_v, :], qkv_recv[r_v, :])
        rot_ref[r_q, :] = q
        rot_ref[r_k, :] = k
        rot_ref[r_v, :] = v
        scores = jnp.where(causal, dot_tn(k, q) * scale, -1e30)
        weight = jnp.exp(scores - jnp.max(scores, axis=0, keepdims=True))
        prob = weight / jnp.sum(weight, axis=0, keepdims=True)
        prob_ref[j] = prob
        mix_ref[pl.ds(pl.multiple_of(j * HEAD, 32), HEAD), :] = dot_nn(v, prob.astype(BF)).astype(BF)
        return carry

    lax.fori_loop(0, heads, attn_body, 0)
    stores.append(store(mix_ref, mix_hbm, 1))

    loads[4].wait()
    for c in range(CHUNKS):
        r = pl.ds(c * rows, rows)
        part_ref[AR_OUT, r, :] = dot_tn(mix_ref[:, c * rows:(c + 1) * rows], wout_ref[...]).astype(BF)
        p1_copy(AR_OUT, c).start()
    for c in range(CHUNKS):
        stage2(AR_OUT, c)
    for c in range(CHUNKS):
        stage3(AR_OUT, c)
    for c in range(CHUNKS):
        r = pl.ds(c * rows, rows)
        stage4(AR_OUT, c)
        h = add_bf(x_ref[r, :], full_ref[AR_OUT, r, :])
        h_ref[r, :] = h
        h32 = h.astype(F32)
        stat_put(1 + c, jnp.sum(h32 * h32, axis=-1, keepdims=True), rows)
    for k in range(5, 8):
        ga_copy(k).start()

    tile = 512
    for c in range(CHUNKS):
        r = pl.ds(c * rows, rows)
        inv2 = lax.rsqrt(stat_get(1 + c, rows) / full_width + EPSILON)
        inv2_ref[r, :] = inv2
        r2 = (h_ref[r, :].astype(F32) * inv2 * g2_ref[...]).astype(BF)
        r2_ref[r, :] = r2
        for p in range(4):
            w_ref = (wg_ref, wu_ref)[p % 2]

            def gu_body(n, carry, c=c, p=p, w_ref=w_ref):
                src = pl.ds(pl.multiple_of((p // 2) * gu_cols + n * tile, tile), tile)
                dst = pl.ds(pl.multiple_of((p % 2) * ff + (p // 2) * gu_cols + n * tile, tile), tile)
                gu_send[pl.ds(c * rows, rows), dst] = dot_nn(r2_ref[pl.ds(c * rows, rows), :], w_ref[:, src]).astype(BF)
                return carry

            lax.fori_loop(0, gu_cols // tile, gu_body, 0)
            gu_copy(c, p).start()
    stores.append(store(r2_ref, r2_hbm, 2))

    for k in range(8):
        ga_copy(k).wait_recv()

    def mlp_chunk(c):
        r = pl.ds(c * rows, rows)
        for hf in range(2):
            gu_copy(c, 2 * hf).wait_recv()
            gu_copy(c, 2 * hf + 1).wait_recv()

            def act_body(n, carry, hf=hf):
                cg = pl.ds(pl.multiple_of(hf * gu_cols + n * 256, 256), 256)
                cu = pl.ds(pl.multiple_of(ff + hf * gu_cols + n * 256, 256), 256)
                gate = add_bf(gu_send[r, cg], gu_recv[r, cg]).astype(F32)
                up = add_bf(gu_send[r, cu], gu_recv[r, cu]).astype(F32)
                ga = add_bf(ga_send[r, cg], ga_recv[r, cg]).astype(F32)
                sig = 1.0 / (1.0 + jnp.exp(-gate))
                silu = gate * sig
                act_ref[r, cg] = (silu * up).astype(BF)
                dgu_ref[r, cg] = (ga * up * (sig * (1.0 + gate * (1.0 - sig)))).astype(BF)
                dgu_ref[r, cu] = (ga * silu).astype(BF)
                return carry

            lax.fori_loop(0, gu_cols // 256, act_body, 0)

        def r2_body(n, carry):
            w = step(n, tile)
            part_ref[AR_R2, r, w] = (dot_nt(dgu_ref[r, 0:ff], wg_ref[w, :]) + dot_nt(dgu_ref[r, ff:2 * ff], wu_ref[w, :])).astype(BF)
            return carry

        lax.fori_loop(0, width // tile, r2_body, 0)
        p1_copy(AR_R2, c).start()

    def down_chunk(c):
        r = pl.ds(c * rows, rows)

        def down_body(n, carry):
            w = step(n, tile)
            part_ref[AR_Y, r, w] = dot_nn(act_ref[r, :], wdown_ref[:, w]).astype(BF)
            return carry

        lax.fori_loop(0, width // tile, down_body, 0)
        p1_copy(AR_Y, c).start()

    dg2_ref[...] = jnp.zeros_like(dg2_ref)

    def norm2_back(c):
        r = pl.ds(c * rows, rows)
        stage4(AR_R2, c)
        gin = full_ref[AR_R2, r, :].astype(F32)
        unit = h_ref[r, :].astype(F32) * inv2_ref[r, :]
        dg2_ref[...] += jnp.sum(gin * unit, axis=0, keepdims=True)
        stat_put(3 + c, jnp.sum(gin * g2_ref[...] * unit, axis=-1, keepdims=True), rows)

    def hidden_back(c):
        r = pl.ds(c * rows, rows)
        dots = stat_get(3 + c, rows)
        inv2 = inv2_ref[r, :]
        unit = h_ref[r, :].astype(F32) * inv2
        scaled = full_ref[AR_R2, r, :].astype(F32) * g2_ref[...]
        norm = inv2 * (scaled - unit * (dots / full_width))
        dh_ref[r, :] = (dy_ref[r, :].astype(F32) + norm).astype(BF)
        gm_send[:, c * rows:(c + 1) * rows] = dot_nt(wout_ref[...], dh_ref[r, :]).astype(BF)
        gm_copy(c).start()

    def y_chunk(c):
        r = pl.ds(c * rows, rows)
        stage4(AR_Y, c)
        h_ref[r, :] = add_bf(h_ref[r, :], full_ref[AR_Y, r, :])

    mlp_chunk(0)
    down_chunk(0)
    stage2(AR_R2, 0)
    stage3(AR_R2, 0)
    stage2(AR_Y, 0)
    norm2_back(0)
    stage3(AR_Y, 0)
    mlp_chunk(1)
    stores.append(store(dgu_ref, dgu_hbm, 3))
    stores.append(store(act_ref, act_hbm, 4))
    stage2(AR_R2, 1)
    hidden_back(0)
    stage3(AR_R2, 1)
    norm2_back(1)
    down_chunk(1)
    hidden_back(1)
    stores.append(store(dh_ref, dh_hbm, 5))
    stage2(AR_Y, 1)
    y_chunk(0)
    stage3(AR_Y, 1)
    y_chunk(1)
    stores.append(store(h_ref, y_hbm, 6))

    for c in range(CHUNKS):
        gm_copy(c).wait_recv()

    def back_body(j, carry):
        base = pl.multiple_of(j * GROUP, 32)
        r_q, r_k, r_v = (pl.ds(base + n * HEAD, HEAD) for n in range(3))
        r_a = pl.ds(pl.multiple_of(j * HEAD, 32), HEAD)
        cos_t, sin_t = cos_ref[...], sin_ref[...]
        da = add_bf(gm_send[r_a, :], gm_recv[r_a, :])
        q, k, v = rot_ref[r_q, :], rot_ref[r_k, :], rot_ref[r_v, :]
        prob = prob_ref[j]
        dp = dot_tn(v, da).astype(BF).astype(F32)
        dqkv_ref[r_v, :] = dot_nt(da, prob.astype(BF)).astype(BF)
        weighted = prob * dp
        ds = ((weighted - prob * jnp.sum(weighted, axis=0, keepdims=True)) * scale).astype(BF)
        dqkv_ref[r_q, :] = unrope(dot_nn(k, ds).astype(BF), cos_t, sin_t)
        dqkv_ref[r_k, :] = unrope(dot_nt(q, ds).astype(BF), cos_t, sin_t)
        return carry

    lax.fori_loop(0, heads, back_body, 0)
    stores.append(store(dqkv_ref, dqkv_hbm, 7))

    for c in range(CHUNKS):
        r = pl.ds(c * rows, rows)
        part_ref[AR_R1, r, :] = dot_tn(dqkv_ref[:, c * rows:(c + 1) * rows], wqkv_ref[...]).astype(BF)
        p1_copy(AR_R1, c).start()
    for c in range(CHUNKS):
        stage2(AR_R1, c)
    for c in range(CHUNKS):
        stage3(AR_R1, c)
    dg1_ref[...] = jnp.zeros_like(dg1_ref)
    for c in range(CHUNKS):
        r = pl.ds(c * rows, rows)
        stage4(AR_R1, c)
        gin = full_ref[AR_R1, r, :].astype(F32)
        unit = x_ref[r, :].astype(F32) * inv1_ref[r, :]
        dg1_ref[...] += jnp.sum(gin * unit, axis=0, keepdims=True)
        stat_put(5 + c, jnp.sum(gin * g1_ref[...] * unit, axis=-1, keepdims=True), rows)
    for c in range(CHUNKS):
        r = pl.ds(c * rows, rows)
        dots = stat_get(5 + c, rows)
        inv1 = inv1_ref[r, :]
        unit = x_ref[r, :].astype(F32) * inv1
        scaled = full_ref[AR_R1, r, :].astype(F32) * g1_ref[...]
        norm = inv1 * (scaled - unit * (dots / full_width))
        dx_ref[r, :] = (dh_ref[r, :].astype(F32) + norm).astype(BF)
    stores.append(store(dx_ref, dx_hbm, 8))

    for k in range(7):
        stat_copy(k).wait_send()
    for k in range(8):
        ga_copy(k).wait_send()
    for j in range(heads):
        qkv_copy(j).wait_send()
    for c in range(CHUNKS):
        for p in range(4):
            gu_copy(c, p).wait_send()
        gm_copy(c).wait_send()
        for i in range(4):
            p1_copy(i, c).wait_send()
            p2_copy(i, c).wait_send()
            p3_copy(i, c).wait_send()
    for copy in stores:
        copy.wait()


def run_layer(x_in, positions, gain_one, gain_two, w_qkv, w_out, w_gu, w_down, grad_out):
    tokens, width = x_in.shape
    ff = w_down.shape[0]
    chans = w_qkv.shape[0]
    mix = w_out.shape[0]
    heads = mix // HEAD
    rows = tokens // CHUNKS
    act = lambda n, dtype=BF: jax.ShapeDtypeStruct((tokens, n), dtype)
    any_spec = pl.BlockSpec(memory_space=pl.ANY)
    vmem_spec = pl.BlockSpec(memory_space=pltpu.VMEM)
    raw_rows = 128 * 32
    scratch = [
        pltpu.VMEM((tokens, width), BF), pltpu.VMEM((tokens, width), BF),
        pltpu.VMEM((chans, width), BF), pltpu.VMEM((mix, width), BF),
        pltpu.VMEM((width, ff), BF), pltpu.VMEM((width, ff), BF), pltpu.VMEM((ff, width), BF),
        pltpu.VMEM((2, raw_rows, 128), BF),
        pltpu.VMEM((1, width), F32), pltpu.VMEM((1, width), F32), pltpu.VMEM((HALF, tokens), F32), pltpu.VMEM((HALF, tokens), F32),
        pltpu.VMEM((tokens, width), BF), pltpu.VMEM((tokens, width), BF), pltpu.VMEM((tokens, width), BF), pltpu.VMEM((tokens, width), BF),
        pltpu.VMEM((tokens, ff), BF), pltpu.VMEM((tokens, 2 * ff), BF),
        pltpu.VMEM((chans, tokens), BF), pltpu.VMEM((heads, tokens, tokens), F32), pltpu.VMEM((mix, tokens), BF), pltpu.VMEM((chans, tokens), BF),
        pltpu.VMEM((tokens, width), BF),
        pltpu.VMEM((tokens, 1), F32), pltpu.VMEM((tokens, 1), F32),
        pltpu.VMEM((tokens, ff), BF), pltpu.VMEM((tokens, ff), BF),
        pltpu.VMEM((chans, tokens), BF), pltpu.VMEM((chans, tokens), BF),
        pltpu.VMEM((tokens, 2 * ff), BF), pltpu.VMEM((tokens, 2 * ff), BF),
        pltpu.VMEM((mix, tokens), BF), pltpu.VMEM((mix, tokens), BF),
        pltpu.VMEM((7, 8, tokens), F32), pltpu.VMEM((7, 8, tokens), F32),
        pltpu.VMEM((4, tokens, width), BF), pltpu.VMEM((4, tokens, width // 2), BF), pltpu.VMEM((4, tokens, width // 2), BF),
        pltpu.VMEM((4, tokens, width // 2), BF), pltpu.VMEM((4, tokens, width), BF),
        pltpu.SemaphoreType.DMA((5,)), pltpu.SemaphoreType.DMA((2,)), pltpu.SemaphoreType.DMA((9,)),
    ]
    for n in (7, 8, heads, 4 * CHUNKS, CHUNKS, 4 * CHUNKS, 4 * CHUNKS, 4 * CHUNKS):
        scratch += [pltpu.SemaphoreType.DMA((n,)), pltpu.SemaphoreType.DMA((n,))]
    vec = jax.ShapeDtypeStruct((1, width), F32)
    return pl.pallas_call(
        layer_kernel,
        name="layer",
        out_shape=(act(width), act(width), vec, vec, act(width), jax.ShapeDtypeStruct((chans, tokens), BF),
                   jax.ShapeDtypeStruct((mix, tokens), BF), act(width), act(width), act(2 * ff), act(ff)),
        in_specs=[any_spec, any_spec, vmem_spec, vmem_spec, vmem_spec, any_spec, any_spec, any_spec, any_spec],
        out_specs=(any_spec, any_spec, vmem_spec, vmem_spec) + (any_spec,) * 7,
        scratch_shapes=scratch,
        compiler_params=pltpu.CompilerParams(collective_id=0, has_side_effects=True, vmem_limit_bytes=67000000),
    )(x_in, grad_out, gain_one, gain_two, positions, w_qkv, w_out, w_gu, w_down)


def grads_kernel(act_hbm, dy_hbm, r2_hbm, dgu_hbm, mix_hbm, dh_hbm, dqkv_hbm, r1_hbm, y_in, dx_in, dg1_in, dg2_in,
                 down_out, gu_out, wout_out, qkv_out, y_out, dx_out, dg1_out, dg2_out,
                 act_ref, dy_ref, r2_ref, dgu_ref, mix_ref, dh_ref, dqkv_ref, r1_ref, y_ref, dx_ref, rows_ref, inter_ref,
                 load_sem, rows_sem, inter_sem, end_sem):
    block = rows_ref.shape[1]
    pad = inter_ref.shape[1] // GU_BLOCK
    ff = dgu_ref.shape[1] // 2
    pairs = [(dqkv_hbm, dqkv_ref), (r1_hbm, r1_ref), (r2_hbm, r2_ref), (dgu_hbm, dgu_ref), (mix_hbm, mix_ref), (dh_hbm, dh_ref),
             (act_hbm, act_ref), (dy_hbm, dy_ref), (y_in, y_ref), (dx_in, dx_ref)]
    loads = [pltpu.make_async_copy(src, dst, load_sem.at[n]) for n, (src, dst) in enumerate(pairs)]
    for copy in loads:
        copy.start()
    dg1_out[...] = dg1_in[...].reshape(dg1_out.shape)
    dg2_out[...] = dg2_in[...].reshape(dg2_out.shape)

    slots = rows_ref.shape[0]

    def rows_copy(out, index, slot):
        return pltpu.make_async_copy(rows_ref.at[slot], out.at[step(index, block)], rows_sem.at[slot])

    def product(out, lhs_of, rhs_ref, first):
        def body(i, carry):
            slot = lax.rem(i + first, slots)

            @pl.when(i + first >= slots)
            def _():
                rows_copy(out, 0, slot).wait()
            rows_ref[slot] = lhs_of(i, rhs_ref)
            rows_copy(out, i, slot).start()
            return carry
        count = out.shape[0] // block
        lax.fori_loop(0, count, body, 0)
        return first + count

    def plain_rows(ref):
        return lambda i, rhs_ref: dot_nn(ref[step(i, block), :], rhs_ref[...])

    loads[0].wait()
    loads[1].wait()
    sent = product(qkv_out, plain_rows(dqkv_ref), r1_ref, 0)

    loads[2].wait()
    loads[3].wait()

    def inter_copy(index, slot):
        return pltpu.make_async_copy(inter_ref.at[slot].reshape(GU_BLOCK, pad, 128).at[:, 0:32, :],
                                     gu_out.at[step(index, GU_BLOCK)], inter_sem.at[slot])

    gu_steps = gu_out.shape[0] // GU_BLOCK

    def gu_body(i, carry):
        slot = lax.rem(i, 2)

        @pl.when(i >= 2)
        def _():
            inter_copy(0, slot).wait()
        lhs = r2_ref[:, step(i, GU_BLOCK)].T
        for k in range(2):
            for n in range(ff // 512):
                val = dot_nn(lhs, dgu_ref[:, k * ff + n * 512:k * ff + (n + 1) * 512])
                for t in range(4):
                    row = 2 * (4 * n + t) + k
                    inter_ref[slot, pl.ds(row, GU_BLOCK, stride=pad), :] = val[:, t * 128:(t + 1) * 128]
        inter_copy(i, slot).start()
        return carry

    lax.fori_loop(0, gu_steps, gu_body, 0)

    loads[4].wait()
    loads[5].wait()
    sent = product(wout_out, plain_rows(mix_ref), dh_ref, sent)
    loads[6].wait()
    loads[7].wait()
    sent = product(down_out, lambda i, rhs_ref: dot_tn(act_ref[:, step(i, block)], rhs_ref[...]), dy_ref, sent)
    loads[8].wait()
    loads[9].wait()
    ends = [pltpu.make_async_copy(y_ref, y_out, end_sem.at[0]), pltpu.make_async_copy(dx_ref, dx_out, end_sem.at[1])]
    for copy in ends:
        copy.start()
    for slot in range(slots):
        rows_copy(down_out, 0, slot).wait()
    for slot in range(2):
        inter_copy(0, slot).wait()
    for copy in ends:
        copy.wait()


GU_BLOCK = 128


def weight_grads(act, grad_out, r2, dgu, mix, dh, dqkv, r1, y, dx, dg1, dg2):
    tokens, width = r2.shape
    ff = act.shape[1]
    any_spec = pl.BlockSpec(memory_space=pl.ANY)
    vmem_spec = pl.BlockSpec(memory_space=pltpu.VMEM)
    out = lambda *shape: jax.ShapeDtypeStruct(shape, F32)
    like = lambda a: jax.ShapeDtypeStruct(a.shape, a.dtype)
    arrays = (act, grad_out, r2, dgu, mix, dh, dqkv, r1, y, dx)
    return pl.pallas_call(
        grads_kernel,
        name="weight_grads",
        in_specs=[any_spec] * 10 + [vmem_spec] * 2,
        out_specs=[any_spec] * 6 + [vmem_spec] * 2,
        out_shape=[out(ff, width), out(width, 32, 128), out(mix.shape[0], width), out(dqkv.shape[0], width), like(y), like(dx), out(width), out(width)],
        scratch_shapes=[pltpu.VMEM(a.shape, a.dtype) for a in arrays] + [
            pltpu.VMEM((4, 256, width), F32), pltpu.VMEM((2, GU_BLOCK * 40, 128), F32),
            pltpu.SemaphoreType.DMA((10,)), pltpu.SemaphoreType.DMA((4,)), pltpu.SemaphoreType.DMA((2,)), pltpu.SemaphoreType.DMA((2,))],
        compiler_params=pltpu.CompilerParams(vmem_limit_bytes=56 << 20),
    )(*arrays, dg1, dg2)


def solution(mesh):
    def per_device(x_in, positions, gain_one, gain_two, w_qkv, w_out, w_gu, w_down, grad_out):
        width, groups, chans = w_qkv.shape
        ff = w_down.shape[0]
        qkv_rows = w_qkv.transpose(1, 2, 0).reshape(groups * chans, width)
        gu_rows = w_gu.reshape(width, 2, ff // 128, 128).transpose(0, 2, 1, 3).reshape(width * 2 * (ff // 128), 128)
        y, dx, dg1, dg2, r1, dqkv, mix, dh, r2, dgu, act = run_layer(
            x_in, positions, gain_one, gain_two, qkv_rows, w_out, gu_rows, w_down, grad_out)
        d_down, d_gu, d_out, d_qkv, y, dx, dg1, dg2 = weight_grads(act, grad_out, r2, dgu, mix, dh, dqkv, r1, y, dx, dg1, dg2)
        d_gu = d_gu.reshape(width, ff // 128, 2, 128).transpose(0, 2, 1, 3).reshape(width, 2, ff)
        d_qkv = d_qkv.reshape(groups, chans, width).transpose(2, 0, 1)
        return y, dx, dg1, dg2, d_qkv, d_out, d_gu, d_down

    act_spec = P('dp', 'embed')
    in_specs = (act_spec, P('dp'), P('embed'), P('embed'), P('embed', 'heads', None), P('heads', 'embed'), P('embed', None, 'heads'), P('heads', 'embed'), act_spec)
    out_specs = (act_spec, act_spec, P(('dp', 'embed')), P(('dp', 'embed')), P(('dp', 'embed'), 'heads', None), P(('dp', 'heads'), 'embed'), P(('dp', 'embed'), None, 'heads'), P(('dp', 'heads'), 'embed'))
    return jax.shard_map(per_device, mesh=mesh, in_specs=in_specs, out_specs=out_specs, check_vma=False)
```

```python
import math

import jax
import jax.numpy as jnp
from jax import lax
from jax.experimental import pallas as pl
from jax.experimental.pallas import tpu as pltpu
from jax.sharding import PartitionSpec as P

EPSILON = 1e-5
ROPE_BASE = 10000.0
HEAD = 96
HALF = HEAD // 2
GROUP = 3 * HEAD
CHUNKS = 2
MESH = pl.DeviceIdType.MESH
BF = jnp.bfloat16
F32 = jnp.float32

AR_OUT, AR_R2, AR_Y, AR_R1 = range(4)
SLOT = (0, 1, 2, 0)
GU_PIECES = 4


def dot_nn(lhs, rhs):
    return lax.dot_general(lhs, rhs, (((1,), (0,)), ((), ())), preferred_element_type=F32)


def dot_nt(lhs, rhs):
    return lax.dot_general(lhs, rhs, (((1,), (1,)), ((), ())), preferred_element_type=F32)


def dot_tn(lhs, rhs):
    return lax.dot_general(lhs, rhs, (((0,), (0,)), ((), ())), preferred_element_type=F32)


def add_bf(one, two):
    return (one.astype(F32) + two.astype(F32)).astype(BF)


def step(index, size):
    return pl.ds(pl.multiple_of(index * size, size), size)


def layer_kernel(x_hbm, dy_hbm, g1_in, g2_in, pos_in, wqkv_hbm, wout_hbm, wgu_hbm, wdown_hbm,
                 y_hbm, dx_hbm, dg1_ref, dg2_ref, r1_hbm, dqkv_hbm, mix_hbm, dh_hbm, r2_hbm, dgu_hbm, act_hbm,
                 x_ref, dy_ref, wqkv_ref, wout_ref, wg_ref, wu_ref, wdown_ref, raw_ref,
                 g1_ref, g2_ref, cos_ref, sin_ref, r1_ref, r2_ref, h_ref, dh_ref, act_ref, dgu_ref, rot_ref, late_ref, early_ref, mix_ref, dqkv_ref, dx_ref,
                 kv_part, cot_ref, dots_ref,
                 inv1_ref, inv2_ref,
                 ga_send, ga_recv, qkv_send, qkv_recv, gu_send, gu_recv, gm_send, gm_recv, stat_send, stat_recv,
                 part_ref, sib_ref, half_ref, far_ref, full_ref,
                 load_sem, raw_sem, store_sem,
                 st_s, st_r, ga_s, ga_r, qk_s, qk_r, gu_s, gu_r, gm_s, gm_r, p1_s, p1_r, p2_s, p2_r, p3_s, p3_r, dots_s, dots_r):
    tokens, width = x_ref.shape
    full_width = 2 * width
    ff = wdown_ref.shape[0]
    heads = wqkv_ref.shape[0] // GROUP
    half_width = width // 2
    rows = tokens // CHUNKS
    emb = lax.axis_index("embed")
    hid = lax.axis_index("heads")
    core = lax.rem(hid, 2)
    sibling = {"heads": hid + 1 - 2 * core}
    across = {"heads": lax.rem(hid + 2, 4)}
    partner = {"embed": 1 - emb}

    barrier = pltpu.get_barrier_semaphore()
    others = [{"embed": lax.rem(emb + n // 4, 2), "heads": lax.rem(hid + n, 4)} for n in range(1, 8)]
    for peer in others:
        pl.semaphore_signal(barrier, inc=1, device_id=peer, device_id_type=MESH)

    def load(src, dst, sem):
        return pltpu.make_async_copy(src, dst, load_sem.at[sem])

    loads = [load(x_hbm, x_ref, 0), load(dy_hbm, dy_ref, 1), load(wdown_hbm, wdown_ref, 2),
             load(wqkv_hbm, wqkv_ref, 3), load(wout_hbm, wout_ref, 4)]
    for copy in loads[:3]:
        copy.start()

    raw_rows = raw_ref.shape[1]
    raw_steps = wgu_hbm.shape[0] // raw_rows

    def raw_load(index, slot):
        return pltpu.make_async_copy(wgu_hbm.at[step(index, raw_rows)], raw_ref.at[slot], raw_sem.at[slot])

    def store(src, dst, sem):
        copy = pltpu.make_async_copy(src, dst, store_sem.at[sem])
        copy.start()
        return copy

    def send(src, dst, s_sem, r_sem, peer):
        return pltpu.make_async_remote_copy(src_ref=src, dst_ref=dst, send_sem=s_sem, recv_sem=r_sem,
                                            device_id=peer, device_id_type=MESH)

    def stat_copy(k):
        return send(stat_send.at[k], stat_recv.at[k], st_s.at[k], st_r.at[k], partner)

    ga_cols = ff // 8

    def ga_copy(k):
        cols = step(k, ga_cols)
        return send(ga_send.at[:, cols], ga_recv.at[:, cols], ga_s.at[k], ga_r.at[k], partner)

    def qkv_copy(j):
        r = step(j, GROUP)
        return send(qkv_send.at[r], qkv_recv.at[r], qk_s.at[j], qk_r.at[j], partner)

    gu_cols = ff // GU_PIECES

    def gu_copy(c, q, k):
        at = (pl.ds(c * rows, rows), pl.ds(pl.multiple_of(k * ff + q * gu_cols, gu_cols), gu_cols))
        n = (c * GU_PIECES + q) * 2 + k
        return send(gu_send.at[at], gu_recv.at[at], gu_s.at[n], gu_r.at[n], partner)

    def gm_copy(c):
        at = (slice(None), pl.ds(c * rows, rows))
        return send(gm_send.at[at], gm_recv.at[at], gm_s.at[c], gm_r.at[c], partner)

    own = pl.ds(pl.multiple_of(core * half_width, half_width), half_width)
    other = pl.ds(pl.multiple_of((1 - core) * half_width, half_width), half_width)

    def p1_copy(i, c):
        r = pl.ds(c * rows, rows)
        k = i * CHUNKS + c
        return send(part_ref.at[SLOT[i], r, other], sib_ref.at[SLOT[i], r], p1_s.at[k], p1_r.at[k], sibling)

    def p2_copy(i, c):
        r = pl.ds(c * rows, rows)
        k = i * CHUNKS + c
        return send(half_ref.at[SLOT[i], r], far_ref.at[SLOT[i], r], p2_s.at[k], p2_r.at[k], across)

    def p3_copy(i, c):
        r = pl.ds(c * rows, rows)
        k = i * CHUNKS + c
        return send(full_ref.at[SLOT[i], r, own], full_ref.at[SLOT[i], r, own], p3_s.at[k], p3_r.at[k], sibling)

    def stage2(i, c):
        r = pl.ds(c * rows, rows)
        p1_copy(i, c).wait_recv()
        half_ref[SLOT[i], r, :] = add_bf(part_ref[SLOT[i], r, own], sib_ref[SLOT[i], r, :])
        p2_copy(i, c).start()

    def stage3(i, c):
        r = pl.ds(c * rows, rows)
        p2_copy(i, c).wait_recv()
        full_ref[SLOT[i], r, own] = add_bf(half_ref[SLOT[i], r, :], far_ref[SLOT[i], r, :])
        p3_copy(i, c).start()

    def stage4(i, c):
        p3_copy(i, c).wait_recv()

    def stat_put(k, col, n):
        flat = jnp.broadcast_to(col, (n, 128)).T[0:8, :]
        stat_send[k, :, 0:n] = flat
        stat_copy(k).start()

    def stat_get(k, n):
        stat_copy(k).wait_recv()
        total = stat_send[k, 0:1, 0:n] + stat_recv[k, 0:1, 0:n]
        return jnp.broadcast_to(total, (128, n)).T[:, 0:1]

    me = emb * 4 + hid

    def dots_copy(k, n):
        at = dots_ref.at[k, me]
        return send(at, at, dots_s.at[7 * k + n], dots_r.at[8 * k + me], others[n])

    def dots_put(k, col):
        dots_ref[k, me] = jnp.broadcast_to(col, (rows, 128)).T[0:8, :]
        for n in range(7):
            dots_copy(k, n).start()

    def dots_get(k):
        for n in range(7):
            src = lax.rem(emb + (n + 1) // 4, 2) * 4 + lax.rem(hid + n + 1, 4)
            at = dots_ref.at[k, src]
            send(at, at, dots_s.at[7 * k + n], dots_r.at[8 * k + src], others[n]).wait_recv()
        total = dots_ref[k, 0, 0:1, :]
        for n in range(1, 8):
            total = total + dots_ref[k, n, 0:1, :]
        return jnp.broadcast_to(total, (128, rows)).T[:, 0:1]

    g1_ref[...] = g1_in[...].reshape(1, width)
    g2_ref[...] = g2_in[...].reshape(1, width)
    loads[0].wait()
    x32 = x_ref[...].astype(F32)
    sq1 = jnp.sum(x32 * x32, axis=-1, keepdims=True)
    pl.semaphore_wait(barrier, 7)
    stat_put(0, sq1, tokens)
    for copy in loads[3:]:
        copy.start()
    for slot in range(2):
        raw_load(slot, slot).start()

    loads[1].wait()
    loads[2].wait()

    def ga_body(k, carry):
        cols = step(k, ga_cols)
        ga_send[:, cols] = dot_nt(dy_ref[...], wdown_ref[cols, :]).astype(BF)

        @pl.when(k == 0)
        def _():
            ga_copy(k).start()
        return carry

    lax.fori_loop(0, 8, ga_body, 0)

    place = pos_in[...].reshape(1, tokens).astype(F32)
    pair_i = lax.broadcasted_iota(jnp.int32, (HALF, 1), 0).astype(F32)
    angles = jnp.exp(pair_i * (-2.0 * math.log(ROPE_BASE) / HEAD)) * place
    cos_ref[...] = jnp.cos(angles)
    sin_ref[...] = jnp.sin(angles)

    inv1 = lax.rsqrt(stat_get(0, tokens) / full_width + EPSILON)
    inv1_ref[...] = inv1
    r1_ref[...] = (x_ref[...].astype(F32) * inv1 * g1_ref[...]).astype(BF)
    stores = [store(r1_ref, r1_hbm, 0)]

    loads[3].wait()

    def qkv_body(j, carry):
        r = step(j, GROUP)
        qkv_send[r, :] = dot_nt(wqkv_ref[r, :], r1_ref[...]).astype(BF)
        qkv_copy(j).start()
        return carry

    lax.fori_loop(0, heads, qkv_body, 0)
    for k in range(1, 5):
        ga_copy(k).start()

    row_i = lax.broadcasted_iota(jnp.int32, (256, 256), 0)
    col_i = lax.broadcasted_iota(jnp.int32, (256, 256), 1)
    perm = (col_i == (row_i % 8) * 32 + row_i // 8).astype(F32).astype(BF)
    blocks = raw_rows // 512

    def raw_body(i, carry):
        slot = lax.rem(i, 2)
        raw_load(i, slot).wait()

        def block_body(b, inner):
            for u in range(4):
                base = pl.multiple_of(b * 2048 + u * 512, 512)
                pair = jnp.concatenate([raw_ref[slot, pl.ds(base, 256), :], raw_ref[slot, pl.ds(base + 256, 256), :]], axis=1)
                out = dot_nn(perm, pair)
                d = pl.ds(pl.multiple_of(i * (raw_rows // 32) + b * 64 + u * 16, 16), 16)
                for t in range(16):
                    for k, dst in ((0, wg_ref), (1, wu_ref)):
                        r = (2 * t + k) * 8
                        both = jnp.concatenate([out[r:r + 8, 0:128], out[r:r + 8, 128:256]], axis=0)
                        dst[d, t * 128:(t + 1) * 128] = both.astype(BF)
            return inner

        lax.fori_loop(0, blocks // 4, block_body, 0)

        @pl.when(i + 2 < raw_steps)
        def _():
            raw_load(i + 2, slot).start()
        return carry

    lax.fori_loop(0, raw_steps, raw_body, 0)

    scale = HEAD ** -0.5
    causal = (lax.broadcasted_iota(jnp.int32, (tokens, tokens), 0) <= lax.broadcasted_iota(jnp.int32, (tokens, tokens), 1))

    def rope(v, cos_t, sin_t):
        v = v.astype(F32)
        one, two = v[0:HALF], v[HALF:HEAD]
        return jnp.concatenate([one * cos_t - two * sin_t, two * cos_t + one * sin_t], axis=0).astype(BF)

    def unrope(v, cos_t, sin_t):
        v = v.astype(F32)
        one, two = v[0:HALF], v[HALF:HEAD]
        return jnp.concatenate([one * cos_t + two * sin_t, two * cos_t - one * sin_t], axis=0).astype(BF)

    def attn_body(j, carry):
        qkv_copy(j).wait_recv()
        base = pl.multiple_of(j * GROUP, 32)
        r_q, r_k, r_v = (pl.ds(base + n * HEAD, HEAD) for n in range(3))
        cos_t, sin_t = cos_ref[...], sin_ref[...]
        q = rope(add_bf(qkv_send[r_q, :], qkv_recv[r_q, :]), cos_t, sin_t)
        k = rope(add_bf(qkv_send[r_k, :], qkv_recv[r_k, :]), cos_t, sin_t)
        v = add_bf(qkv_send[r_v, :], qkv_recv[r_v, :])
        rot_ref[r_q, :] = q
        rot_ref[r_k, :] = k
        rot_ref[r_v, :] = v
        scores = jnp.where(causal, dot_tn(k, q) * scale, -1e30)
        weight = jnp.exp(scores - jnp.max(scores, axis=0, keepdims=True))
        prob = weight / jnp.sum(weight, axis=0, keepdims=True)
        late_ref[j] = prob[:, rows:]
        early_ref[j] = prob[0:rows, 0:rows]
        mix_ref[pl.ds(pl.multiple_of(j * HEAD, 32), HEAD), :] = dot_nn(v, prob.astype(BF)).astype(BF)
        return carry

    lax.fori_loop(0, heads, attn_body, 0)
    stores.append(store(mix_ref, mix_hbm, 1))

    loads[4].wait()
    order = tuple(reversed(range(CHUNKS)))
    for c in order:
        r = pl.ds(c * rows, rows)
        part_ref[SLOT[AR_OUT], r, :] = dot_tn(mix_ref[:, c * rows:(c + 1) * rows], wout_ref[...]).astype(BF)
        p1_copy(AR_OUT, c).start()
    for c in order:
        stage2(AR_OUT, c)
    for c in order:
        stage3(AR_OUT, c)
    for c in order:
        r = pl.ds(c * rows, rows)
        stage4(AR_OUT, c)
        h = add_bf(x_ref[r, :], full_ref[SLOT[AR_OUT], r, :])
        h_ref[r, :] = h
        h32 = h.astype(F32)
        stat_put(1 + c, jnp.sum(h32 * h32, axis=-1, keepdims=True), rows)
    for k in range(5, 8):
        ga_copy(k).start()

    tile = 512
    for c in order:
        r = pl.ds(c * rows, rows)
        inv2 = lax.rsqrt(stat_get(1 + c, rows) / full_width + EPSILON)
        inv2_ref[r, :] = inv2
        r2_ref[r, :] = (h_ref[r, :].astype(F32) * inv2 * g2_ref[...]).astype(BF)

        def gu_body(q, carry, c=c, r=r):
            for k, w_ref in ((0, wg_ref), (1, wu_ref)):
                dst = pl.ds(pl.multiple_of(k * ff + q * gu_cols, gu_cols), gu_cols)
                gu_send[r, dst] = dot_nn(r2_ref[r, :], w_ref[:, step(q, gu_cols)]).astype(BF)
                gu_copy(c, q, k).start()
            return carry

        lax.fori_loop(0, GU_PIECES, gu_body, 0)
    stores.append(store(r2_ref, r2_hbm, 2))

    for k in range(8):
        ga_copy(k).wait_recv()
    for c in order:
        p1_copy(AR_OUT, c).wait_send()
        p2_copy(AR_OUT, c).wait_send()
        p3_copy(AR_OUT, c).wait_send()

    def mlp_chunk(c):
        r = pl.ds(c * rows, rows)
        cot_ref[...] = jnp.zeros_like(cot_ref)

        def piece(q, carry):
            gu_copy(c, q, 0).wait_recv()
            gu_copy(c, q, 1).wait_recv()
            for n in range(gu_cols // 256):
                cg = pl.ds(pl.multiple_of(q * gu_cols + n * 256, 256), 256)
                cu = pl.ds(pl.multiple_of(ff + q * gu_cols + n * 256, 256), 256)
                gate = add_bf(gu_send[r, cg], gu_recv[r, cg]).astype(F32)
                up = add_bf(gu_send[r, cu], gu_recv[r, cu]).astype(F32)
                ga = add_bf(ga_send[r, cg], ga_recv[r, cg]).astype(F32)
                sig = 1.0 / (1.0 + jnp.exp(-gate))
                silu = gate * sig
                act_ref[r, cg] = (silu * up).astype(BF)
                dgu_ref[r, cg] = (ga * up * (sig * (1.0 + gate * (1.0 - sig)))).astype(BF)
                dgu_ref[r, cu] = (ga * silu).astype(BF)
            at_g = step(q, gu_cols)
            at_u = pl.ds(pl.multiple_of(ff + q * gu_cols, gu_cols), gu_cols)
            for n in range(width // tile):
                w = slice(n * tile, (n + 1) * tile)
                cot_ref[:, w] += dot_nt(dgu_ref[r, at_g], wg_ref[w, at_g]) + dot_nt(dgu_ref[r, at_u], wu_ref[w, at_g])
            return carry

        lax.fori_loop(0, GU_PIECES, piece, 0)
        part_ref[SLOT[AR_R2], r, :] = cot_ref[...].astype(BF)
        p1_copy(AR_R2, c).start()
        unit = h_ref[r, :].astype(F32) * inv2_ref[r, :]
        dots_put(c, jnp.sum(cot_ref[...] * g2_ref[...] * unit, axis=-1, keepdims=True))

    def down_chunk(c):
        r = pl.ds(c * rows, rows)

        def down_body(n, carry):
            w = step(n, tile)
            part_ref[SLOT[AR_Y], r, w] = dot_nn(act_ref[r, :], wdown_ref[:, w]).astype(BF)
            return carry

        lax.fori_loop(0, width // tile, down_body, 0)
        p1_copy(AR_Y, c).start()

    dg1_ref[...] = jnp.zeros_like(dg1_ref)
    dg2_ref[...] = jnp.zeros_like(dg2_ref)

    def hidden_back(c):
        r = pl.ds(c * rows, rows)
        dots = dots_get(c)
        stage4(AR_R2, c)
        inv2 = inv2_ref[r, :]
        unit = h_ref[r, :].astype(F32) * inv2
        gin = full_ref[SLOT[AR_R2], r, :].astype(F32)
        norm = inv2 * (gin * g2_ref[...] - unit * (dots / full_width))
        dh_ref[r, :] = (dy_ref[r, :].astype(F32) + norm).astype(BF)
        gm_send[:, c * rows:(c + 1) * rows] = dot_nt(wout_ref[...], dh_ref[r, :]).astype(BF)
        gm_copy(c).start()
        dg2_ref[...] += jnp.sum(gin * unit, axis=0, keepdims=True)

    def y_chunk(c):
        r = pl.ds(c * rows, rows)
        stage4(AR_Y, c)
        h_ref[r, :] = add_bf(h_ref[r, :], full_ref[SLOT[AR_Y], r, :])

    def scores_back(v, da, prob):
        dp = dot_tn(v, da).astype(BF).astype(F32)
        weighted = prob * dp
        return ((weighted - prob * jnp.sum(weighted, axis=0, keepdims=True)) * scale).astype(BF)

    def late_body(j, carry):
        base = pl.multiple_of(j * GROUP, 32)
        r_q, r_k, r_v = (pl.ds(base + n * HEAD, HEAD) for n in range(3))
        r_a = pl.ds(pl.multiple_of(j * HEAD, 32), HEAD)
        cos_t, sin_t = cos_ref[:, rows:], sin_ref[:, rows:]
        da = add_bf(gm_send[r_a, rows:], gm_recv[r_a, rows:])
        prob = late_ref[j]
        k = rot_ref[r_k, :]
        ds = scores_back(rot_ref[r_v, :], da, prob)
        dv = dot_nt(da, prob.astype(BF))
        dk = dot_nt(rot_ref[r_q, rows:], ds)
        dqkv_ref[r_q, rows:] = unrope(dot_nn(k, ds).astype(BF), cos_t, sin_t)
        dqkv_ref[r_k, rows:] = unrope(dk[:, rows:].astype(BF), cos_t, sin_t)
        dqkv_ref[r_v, rows:] = dv[:, rows:].astype(BF)
        kv_part[0, r_a, :] = dk[:, 0:rows]
        kv_part[1, r_a, :] = dv[:, 0:rows]
        return carry

    def early_body(j, carry):
        base = pl.multiple_of(j * GROUP, 32)
        r_q, r_k, r_v = (pl.ds(base + n * HEAD, HEAD) for n in range(3))
        r_a = pl.ds(pl.multiple_of(j * HEAD, 32), HEAD)
        cos_t, sin_t = cos_ref[:, 0:rows], sin_ref[:, 0:rows]
        da = add_bf(gm_send[r_a, 0:rows], gm_recv[r_a, 0:rows])
        prob = early_ref[j]
        ds = scores_back(rot_ref[r_v, 0:rows], da, prob)
        dv = kv_part[1, r_a, :] + dot_nt(da, prob.astype(BF))
        dk = kv_part[0, r_a, :] + dot_nt(rot_ref[r_q, 0:rows], ds)
        dqkv_ref[r_q, 0:rows] = unrope(dot_nn(rot_ref[r_k, 0:rows], ds).astype(BF), cos_t, sin_t)
        dqkv_ref[r_k, 0:rows] = unrope(dk.astype(BF), cos_t, sin_t)
        dqkv_ref[r_v, 0:rows] = dv.astype(BF)
        return carry

    def attn_back(c):
        gm_copy(c).wait_recv()
        lax.fori_loop(0, heads, late_body if c else early_body, 0)
        r = pl.ds(c * rows, rows)
        cot = dot_tn(dqkv_ref[:, c * rows:(c + 1) * rows], wqkv_ref[...])
        part_ref[SLOT[AR_R1], r, :] = cot.astype(BF)
        p1_copy(AR_R1, c).start()
        unit = x_ref[r, :].astype(F32) * inv1_ref[r, :]
        dots_put(CHUNKS + c, jnp.sum(cot * g1_ref[...] * unit, axis=-1, keepdims=True))

    def input_back(c):
        r = pl.ds(c * rows, rows)
        dots = dots_get(CHUNKS + c)
        stage4(AR_R1, c)
        inv1 = inv1_ref[r, :]
        unit = x_ref[r, :].astype(F32) * inv1
        gin = full_ref[SLOT[AR_R1], r, :].astype(F32)
        norm = inv1 * (gin * g1_ref[...] - unit * (dots / full_width))
        dx_ref[r, :] = (dh_ref[r, :].astype(F32) + norm).astype(BF)
        stores.append(store(dx_ref.at[r], dx_hbm.at[r], 8 + c))
        dg1_ref[...] += jnp.sum(gin * unit, axis=0, keepdims=True)

    mlp_chunk(1)
    stage2(AR_R2, 1)
    down_chunk(1)
    stage3(AR_R2, 1)
    stage2(AR_Y, 1)
    hidden_back(1)
    stage3(AR_Y, 1)
    mlp_chunk(0)
    stage2(AR_R2, 0)
    stores.append(store(dgu_ref, dgu_hbm, 3))
    stores.append(store(act_ref, act_hbm, 4))
    attn_back(1)
    stage3(AR_R2, 0)
    stage2(AR_R1, 1)
    hidden_back(0)
    stores.append(store(dh_ref, dh_hbm, 5))
    down_chunk(0)
    stage3(AR_R1, 1)
    stage2(AR_Y, 0)
    y_chunk(1)
    attn_back(0)
    stores.append(store(dqkv_ref, dqkv_hbm, 7))
    stage2(AR_R1, 0)
    stage3(AR_Y, 0)
    input_back(1)
    y_chunk(0)
    stores.append(store(h_ref, y_hbm, 6))
    stage3(AR_R1, 0)
    input_back(0)

    for k in range(3):
        stat_copy(k).wait_send()
    for k in range(2 * CHUNKS):
        for n in range(7):
            dots_copy(k, n).wait_send()
    for k in range(8):
        ga_copy(k).wait_send()
    for j in range(heads):
        qkv_copy(j).wait_send()
    for c in range(CHUNKS):
        for q in range(GU_PIECES):
            for k in range(2):
                gu_copy(c, q, k).wait_send()
        gm_copy(c).wait_send()
        for i in range(1, 4):
            p1_copy(i, c).wait_send()
            p2_copy(i, c).wait_send()
            p3_copy(i, c).wait_send()
    for copy in stores:
        copy.wait()


def run_layer(x_in, positions, gain_one, gain_two, w_qkv, w_out, w_gu, w_down, grad_out):
    tokens, width = x_in.shape
    ff = w_down.shape[0]
    chans = w_qkv.shape[0]
    mix = w_out.shape[0]
    heads = mix // HEAD
    rows = tokens // CHUNKS
    act = lambda n, dtype=BF: jax.ShapeDtypeStruct((tokens, n), dtype)
    any_spec = pl.BlockSpec(memory_space=pl.ANY)
    vmem_spec = pl.BlockSpec(memory_space=pltpu.VMEM)
    raw_rows = 128 * 32
    scratch = [
        pltpu.VMEM((tokens, width), BF), pltpu.VMEM((tokens, width), BF),
        pltpu.VMEM((chans, width), BF), pltpu.VMEM((mix, width), BF),
        pltpu.VMEM((width, ff), BF), pltpu.VMEM((width, ff), BF), pltpu.VMEM((ff, width), BF),
        pltpu.VMEM((2, raw_rows, 128), BF),
        pltpu.VMEM((1, width), F32), pltpu.VMEM((1, width), F32), pltpu.VMEM((HALF, tokens), F32), pltpu.VMEM((HALF, tokens), F32),
        pltpu.VMEM((tokens, width), BF), pltpu.VMEM((tokens, width), BF), pltpu.VMEM((tokens, width), BF), pltpu.VMEM((tokens, width), BF),
        pltpu.VMEM((tokens, ff), BF), pltpu.VMEM((tokens, 2 * ff), BF),
        pltpu.VMEM((chans, tokens), BF), pltpu.VMEM((heads, tokens, rows), F32), pltpu.VMEM((heads, rows, rows), F32), pltpu.VMEM((mix, tokens), BF), pltpu.VMEM((chans, tokens), BF),
        pltpu.VMEM((tokens, width), BF),
        pltpu.VMEM((2, mix, rows), F32), pltpu.VMEM((rows, width), F32), pltpu.VMEM((2 * CHUNKS, 8, 8, rows), F32),
        pltpu.VMEM((tokens, 1), F32), pltpu.VMEM((tokens, 1), F32),
        pltpu.VMEM((tokens, ff), BF), pltpu.VMEM((tokens, ff), BF),
        pltpu.VMEM((chans, tokens), BF), pltpu.VMEM((chans, tokens), BF),
        pltpu.VMEM((tokens, 2 * ff), BF), pltpu.VMEM((tokens, 2 * ff), BF),
        pltpu.VMEM((mix, tokens), BF), pltpu.VMEM((mix, tokens), BF),
        pltpu.VMEM((3, 8, tokens), F32), pltpu.VMEM((3, 8, tokens), F32),
        pltpu.VMEM((3, tokens, width), BF), pltpu.VMEM((3, tokens, width // 2), BF), pltpu.VMEM((3, tokens, width // 2), BF),
        pltpu.VMEM((3, tokens, width // 2), BF), pltpu.VMEM((3, tokens, width), BF),
        pltpu.SemaphoreType.DMA((5,)), pltpu.SemaphoreType.DMA((2,)), pltpu.SemaphoreType.DMA((8 + CHUNKS,)),
    ]
    for n in (3, 8, heads, 2 * GU_PIECES * CHUNKS, CHUNKS, 4 * CHUNKS, 4 * CHUNKS, 4 * CHUNKS):
        scratch += [pltpu.SemaphoreType.DMA((n,)), pltpu.SemaphoreType.DMA((n,))]
    scratch += [pltpu.SemaphoreType.DMA((7 * 2 * CHUNKS,)), pltpu.SemaphoreType.DMA((8 * 2 * CHUNKS,))]
    vec = jax.ShapeDtypeStruct((1, width), F32)
    return pl.pallas_call(
        layer_kernel,
        name="layer",
        out_shape=(act(width), act(width), vec, vec, act(width), jax.ShapeDtypeStruct((chans, tokens), BF),
                   jax.ShapeDtypeStruct((mix, tokens), BF), act(width), act(width), act(2 * ff), act(ff)),
        in_specs=[any_spec, any_spec, vmem_spec, vmem_spec, vmem_spec, any_spec, any_spec, any_spec, any_spec],
        out_specs=(any_spec, any_spec, vmem_spec, vmem_spec) + (any_spec,) * 7,
        scratch_shapes=scratch,
        compiler_params=pltpu.CompilerParams(collective_id=0, has_side_effects=True, vmem_limit_bytes=67000000),
    )(x_in, grad_out, gain_one, gain_two, positions, w_qkv, w_out, w_gu, w_down)


def grads_kernel(act_hbm, dy_hbm, r2_hbm, dgu_hbm, mix_hbm, dh_hbm, dqkv_hbm, r1_hbm, y_in, dx_in, dg1_in, dg2_in,
                 down_out, gu_out, wout_out, qkv_out, y_out, dx_out, dg1_out, dg2_out,
                 act_ref, dy_ref, r2_ref, dgu_ref, mix_ref, dh_ref, dqkv_ref, r1_ref, y_ref, dx_ref, rows_ref, inter_ref,
                 load_sem, rows_sem, inter_sem, end_sem):
    block = rows_ref.shape[1]
    pad = inter_ref.shape[1] // GU_BLOCK
    ff = dgu_ref.shape[1] // 2
    pairs = [(dqkv_hbm, dqkv_ref), (r1_hbm, r1_ref), (r2_hbm, r2_ref), (dgu_hbm, dgu_ref), (mix_hbm, mix_ref), (dh_hbm, dh_ref),
             (act_hbm, act_ref), (dy_hbm, dy_ref), (y_in, y_ref), (dx_in, dx_ref)]
    loads = [pltpu.make_async_copy(src, dst, load_sem.at[n]) for n, (src, dst) in enumerate(pairs)]
    for copy in loads:
        copy.start()
    dg1_out[...] = dg1_in[...].reshape(dg1_out.shape)
    dg2_out[...] = dg2_in[...].reshape(dg2_out.shape)

    slots = rows_ref.shape[0]

    def rows_copy(out, index, slot):
        return pltpu.make_async_copy(rows_ref.at[slot], out.at[step(index, block)], rows_sem.at[slot])

    def product(out, lhs_of, rhs_ref, first):
        def body(i, carry):
            slot = lax.rem(i + first, slots)

            @pl.when(i + first >= slots)
            def _():
                rows_copy(out, 0, slot).wait()
            rows_ref[slot] = lhs_of(i, rhs_ref)
            rows_copy(out, i, slot).start()
            return carry
        count = out.shape[0] // block
        lax.fori_loop(0, count, body, 0)
        return first + count

    def plain_rows(ref):
        return lambda i, rhs_ref: dot_nn(ref[step(i, block), :], rhs_ref[...])

    loads[0].wait()
    loads[1].wait()
    sent = product(qkv_out, plain_rows(dqkv_ref), r1_ref, 0)

    loads[2].wait()
    loads[3].wait()

    def inter_copy(index, slot):
        return pltpu.make_async_copy(inter_ref.at[slot].reshape(GU_BLOCK, pad, 128).at[:, 0:32, :],
                                     gu_out.at[step(index, GU_BLOCK)], inter_sem.at[slot])

    gu_steps = gu_out.shape[0] // GU_BLOCK

    def gu_body(i, carry):
        slot = lax.rem(i, 2)

        @pl.when(i >= 2)
        def _():
            inter_copy(0, slot).wait()
        lhs = r2_ref[:, step(i, GU_BLOCK)].T
        for k in range(2):
            for n in range(ff // 512):
                val = dot_nn(lhs, dgu_ref[:, k * ff + n * 512:k * ff + (n + 1) * 512])
                for t in range(4):
                    row = 2 * (4 * n + t) + k
                    inter_ref[slot, pl.ds(row, GU_BLOCK, stride=pad), :] = val[:, t * 128:(t + 1) * 128]
        inter_copy(i, slot).start()
        return carry

    lax.fori_loop(0, gu_steps, gu_body, 0)

    loads[4].wait()
    loads[5].wait()
    sent = product(wout_out, plain_rows(mix_ref), dh_ref, sent)
    loads[6].wait()
    loads[7].wait()
    sent = product(down_out, lambda i, rhs_ref: dot_tn(act_ref[:, step(i, block)], rhs_ref[...]), dy_ref, sent)
    loads[8].wait()
    loads[9].wait()
    ends = [pltpu.make_async_copy(y_ref, y_out, end_sem.at[0]), pltpu.make_async_copy(dx_ref, dx_out, end_sem.at[1])]
    for copy in ends:
        copy.start()
    for slot in range(slots):
        rows_copy(down_out, 0, slot).wait()
    for slot in range(2):
        inter_copy(0, slot).wait()
    for copy in ends:
        copy.wait()


GU_BLOCK = 128


def weight_grads(act, grad_out, r2, dgu, mix, dh, dqkv, r1, y, dx, dg1, dg2):
    tokens, width = r2.shape
    ff = act.shape[1]
    any_spec = pl.BlockSpec(memory_space=pl.ANY)
    vmem_spec = pl.BlockSpec(memory_space=pltpu.VMEM)
    out = lambda *shape: jax.ShapeDtypeStruct(shape, F32)
    like = lambda a: jax.ShapeDtypeStruct(a.shape, a.dtype)
    arrays = (act, grad_out, r2, dgu, mix, dh, dqkv, r1, y, dx)
    return pl.pallas_call(
        grads_kernel,
        name="weight_grads",
        in_specs=[any_spec] * 10 + [vmem_spec] * 2,
        out_specs=[any_spec] * 6 + [vmem_spec] * 2,
        out_shape=[out(ff, width), out(width, 32, 128), out(mix.shape[0], width), out(dqkv.shape[0], width), like(y), like(dx), out(width), out(width)],
        scratch_shapes=[pltpu.VMEM(a.shape, a.dtype) for a in arrays] + [
            pltpu.VMEM((4, 256, width), F32), pltpu.VMEM((2, GU_BLOCK * 40, 128), F32),
            pltpu.SemaphoreType.DMA((10,)), pltpu.SemaphoreType.DMA((4,)), pltpu.SemaphoreType.DMA((2,)), pltpu.SemaphoreType.DMA((2,))],
        compiler_params=pltpu.CompilerParams(vmem_limit_bytes=56 << 20),
    )(*arrays, dg1, dg2)


def solution(mesh):
    def per_device(x_in, positions, gain_one, gain_two, w_qkv, w_out, w_gu, w_down, grad_out):
        width, groups, chans = w_qkv.shape
        ff = w_down.shape[0]
        qkv_rows = w_qkv.transpose(1, 2, 0).reshape(groups * chans, width)
        gu_rows = w_gu.reshape(width, 2, ff // 128, 128).transpose(0, 2, 1, 3).reshape(width * 2 * (ff // 128), 128)
        y, dx, dg1, dg2, r1, dqkv, mix, dh, r2, dgu, act = run_layer(
            x_in, positions, gain_one, gain_two, qkv_rows, w_out, gu_rows, w_down, grad_out)
        d_down, d_gu, d_out, d_qkv, y, dx, dg1, dg2 = weight_grads(act, grad_out, r2, dgu, mix, dh, dqkv, r1, y, dx, dg1, dg2)
        d_gu = d_gu.reshape(width, ff // 128, 2, 128).transpose(0, 2, 1, 3).reshape(width, 2, ff)
        d_qkv = d_qkv.reshape(groups, chans, width).transpose(2, 0, 1)
        return y, dx, dg1, dg2, d_qkv, d_out, d_gu, d_down

    act_spec = P('dp', 'embed')
    in_specs = (act_spec, P('dp'), P('embed'), P('embed'), P('embed', 'heads', None), P('heads', 'embed'), P('embed', None, 'heads'), P('heads', 'embed'), act_spec)
    out_specs = (act_spec, act_spec, P(('dp', 'embed')), P(('dp', 'embed')), P(('dp', 'embed'), 'heads', None), P(('dp', 'heads'), 'embed'), P(('dp', 'embed'), None, 'heads'), P(('dp', 'heads'), 'embed'))
    return jax.shard_map(per_device, mesh=mesh, in_specs=in_specs, out_specs=out_specs, check_vma=False)
```

```python
import math

import jax
import jax.numpy as jnp
from jax import lax
from jax.experimental import pallas as pl
from jax.experimental.pallas import tpu as pltpu
from jax.sharding import PartitionSpec as P

EPSILON = 1e-5
ROPE_BASE = 10000.0
HEAD = 96
HALF = HEAD // 2
GROUP = 3 * HEAD
CHUNKS = 2
MESH = pl.DeviceIdType.MESH
BF = jnp.bfloat16
F32 = jnp.float32

AR_OUT, AR_R2, AR_Y, AR_R1 = range(4)
SLOT = (0, 1, 2, 0)
GU_PIECES = 4


def dot_nn(lhs, rhs):
    return lax.dot_general(lhs, rhs, (((1,), (0,)), ((), ())), preferred_element_type=F32)


def dot_nt(lhs, rhs):
    return lax.dot_general(lhs, rhs, (((1,), (1,)), ((), ())), preferred_element_type=F32)


def dot_tn(lhs, rhs):
    return lax.dot_general(lhs, rhs, (((0,), (0,)), ((), ())), preferred_element_type=F32)


def add_bf(one, two):
    return (one.astype(F32) + two.astype(F32)).astype(BF)


def step(index, size):
    return pl.ds(pl.multiple_of(index * size, size), size)


def layer_kernel(x_hbm, dy_hbm, g1_in, g2_in, pos_in, wqkv_hbm, wout_hbm, wgu_hbm, wdown_hbm,
                 y_hbm, dx_hbm, dg1_ref, dg2_ref, r1_hbm, dqkv_hbm, mix_hbm, dh_hbm, r2_hbm, dgu_hbm, act_hbm,
                 x_ref, dy_ref, wqkv_ref, wout_ref, wg_ref, wu_ref, wdown_ref, raw_ref,
                 g1_ref, g2_ref, cos_ref, sin_ref, r1_ref, r2_ref, h_ref, dh_ref, act_ref, dgu_ref, rot_ref, late_ref, early_ref, mix_ref, dqkv_ref, dx_ref,
                 kv_part, cot_ref, dots_ref,
                 inv1_ref, inv2_ref,
                 ga_send, ga_recv, qkv_send, qkv_recv, gu_send, gu_recv, gm_send, gm_recv, stat_send, stat_recv,
                 part_ref, sib_ref, half_ref, far_ref, full_ref,
                 load_sem, raw_sem, store_sem,
                 st_s, st_r, ga_s, ga_r, qk_s, qk_r, gu_s, gu_r, gm_s, gm_r, p1_s, p1_r, p2_s, p2_r, p3_s, p3_r, dots_s, dots_r):
    tokens, width = x_ref.shape
    full_width = 2 * width
    ff = wdown_ref.shape[0]
    heads = wqkv_ref.shape[0] // GROUP
    half_width = width // 2
    rows = tokens // CHUNKS
    emb = lax.axis_index("embed")
    hid = lax.axis_index("heads")
    core = lax.rem(hid, 2)
    sibling = {"heads": hid + 1 - 2 * core}
    across = {"heads": lax.rem(hid + 2, 4)}
    partner = {"embed": 1 - emb}

    barrier = pltpu.get_barrier_semaphore()
    others = [{"embed": lax.rem(emb + n // 4, 2), "heads": lax.rem(hid + n, 4)} for n in range(1, 8)]
    for peer in others:
        pl.semaphore_signal(barrier, inc=1, device_id=peer, device_id_type=MESH)

    def load(src, dst, sem):
        return pltpu.make_async_copy(src, dst, load_sem.at[sem])

    loads = [load(x_hbm, x_ref, 0), load(dy_hbm, dy_ref, 1), load(wdown_hbm, wdown_ref, 2),
             load(wqkv_hbm, wqkv_ref, 3), load(wout_hbm, wout_ref, 4)]
    for copy in loads[:3]:
        copy.start()

    raw_rows = raw_ref.shape[1]
    raw_steps = wgu_hbm.shape[0] // raw_rows

    def raw_load(index, slot):
        return pltpu.make_async_copy(wgu_hbm.at[step(index, raw_rows)], raw_ref.at[slot], raw_sem.at[slot])

    def store(src, dst, sem):
        copy = pltpu.make_async_copy(src, dst, store_sem.at[sem])
        copy.start()
        return copy

    def send(src, dst, s_sem, r_sem, peer):
        return pltpu.make_async_remote_copy(src_ref=src, dst_ref=dst, send_sem=s_sem, recv_sem=r_sem,
                                            device_id=peer, device_id_type=MESH)

    def stat_copy(k):
        return send(stat_send.at[k], stat_recv.at[k], st_s.at[k], st_r.at[k], partner)

    ga_cols = ff // 8

    def ga_copy(k):
        cols = step(k, ga_cols)
        return send(ga_send.at[:, cols], ga_recv.at[:, cols], ga_s.at[k], ga_r.at[k], partner)

    def qkv_copy(j):
        r = step(j, GROUP)
        return send(qkv_send.at[r], qkv_recv.at[r], qk_s.at[j], qk_r.at[j], partner)

    gu_cols = ff // GU_PIECES

    def gu_copy(c, q, k):
        at = (pl.ds(c * rows, rows), pl.ds(pl.multiple_of(k * ff + q * gu_cols, gu_cols), gu_cols))
        n = (c * GU_PIECES + q) * 2 + k
        return send(gu_send.at[at], gu_recv.at[at], gu_s.at[n], gu_r.at[n], partner)

    gm_rows = gm_send.shape[0] // 2

    def gm_copy(c, hf):
        at = (pl.ds(hf * gm_rows, gm_rows), pl.ds(c * rows, rows))
        return send(gm_send.at[at], gm_recv.at[at], gm_s.at[2 * c + hf], gm_r.at[2 * c + hf], partner)

    own = pl.ds(pl.multiple_of(core * half_width, half_width), half_width)
    other = pl.ds(pl.multiple_of((1 - core) * half_width, half_width), half_width)

    def p1_copy(i, c):
        r = pl.ds(c * rows, rows)
        k = i * CHUNKS + c
        return send(part_ref.at[SLOT[i], r, other], sib_ref.at[SLOT[i], r], p1_s.at[k], p1_r.at[k], sibling)

    def p2_copy(i, c):
        r = pl.ds(c * rows, rows)
        k = i * CHUNKS + c
        return send(half_ref.at[SLOT[i], r], far_ref.at[SLOT[i], r], p2_s.at[k], p2_r.at[k], across)

    def p3_copy(i, c):
        r = pl.ds(c * rows, rows)
        k = i * CHUNKS + c
        return send(full_ref.at[SLOT[i], r, own], full_ref.at[SLOT[i], r, own], p3_s.at[k], p3_r.at[k], sibling)

    def stage2(i, c):
        r = pl.ds(c * rows, rows)
        p1_copy(i, c).wait_recv()
        half_ref[SLOT[i], r, :] = add_bf(part_ref[SLOT[i], r, own], sib_ref[SLOT[i], r, :])
        p2_copy(i, c).start()

    def stage3(i, c):
        r = pl.ds(c * rows, rows)
        p2_copy(i, c).wait_recv()
        full_ref[SLOT[i], r, own] = add_bf(half_ref[SLOT[i], r, :], far_ref[SLOT[i], r, :])
        p3_copy(i, c).start()

    def stage4(i, c):
        p3_copy(i, c).wait_recv()

    def stat_put(k, col, n):
        flat = jnp.broadcast_to(col, (n, 128)).T[0:8, :]
        stat_send[k, :, 0:n] = flat
        stat_copy(k).start()

    def stat_get(k, n):
        stat_copy(k).wait_recv()
        total = stat_send[k, 0:1, 0:n] + stat_recv[k, 0:1, 0:n]
        return jnp.broadcast_to(total, (128, n)).T[:, 0:1]

    me = emb * 4 + hid

    def dots_copy(k, n):
        at = dots_ref.at[k, me]
        return send(at, at, dots_s.at[7 * k + n], dots_r.at[8 * k + me], others[n])

    def dots_put(k, col):
        dots_ref[k, me] = jnp.broadcast_to(col, (rows, 128)).T[0:8, :]
        for n in range(7):
            dots_copy(k, n).start()

    def dots_get(k):
        for n in range(7):
            src = lax.rem(emb + (n + 1) // 4, 2) * 4 + lax.rem(hid + n + 1, 4)
            at = dots_ref.at[k, src]
            send(at, at, dots_s.at[7 * k + n], dots_r.at[8 * k + src], others[n]).wait_recv()
        total = dots_ref[k, 0, 0:1, :]
        for n in range(1, 8):
            total = total + dots_ref[k, n, 0:1, :]
        return jnp.broadcast_to(total, (128, rows)).T[:, 0:1]

    place = pos_in[...].reshape(1, tokens).astype(F32)
    pair_i = lax.broadcasted_iota(jnp.int32, (HALF, 1), 0).astype(F32)
    angles = jnp.exp(pair_i * (-2.0 * math.log(ROPE_BASE) / HEAD)) * place
    cos_ref[...] = jnp.cos(angles)
    sin_ref[...] = jnp.sin(angles)
    g1_ref[...] = g1_in[...].reshape(1, width)
    g2_ref[...] = g2_in[...].reshape(1, width)
    loads[0].wait()
    x32 = x_ref[...].astype(F32)
    sq1 = jnp.sum(x32 * x32, axis=-1, keepdims=True)
    for copy in loads[3:]:
        copy.start()
    for slot in range(2):
        raw_load(slot, slot).start()

    def ga_body(k, carry):
        cols = step(k, ga_cols)
        ga_send[:, cols] = dot_nt(dy_ref[...], wdown_ref[cols, :]).astype(BF)
        return carry

    loads[1].wait()
    loads[2].wait()
    lax.fori_loop(0, 4, ga_body, 0)
    pl.semaphore_wait(barrier, 7)
    stat_put(0, sq1, tokens)
    ga_copy(0).start()
    lax.fori_loop(4, 8, ga_body, 0)
    inv1 = lax.rsqrt(stat_get(0, tokens) / full_width + EPSILON)
    inv1_ref[...] = inv1
    r1_ref[...] = (x_ref[...].astype(F32) * inv1 * g1_ref[...]).astype(BF)
    stores = [store(r1_ref, r1_hbm, 0)]

    loads[3].wait()

    def qkv_body(j, carry):
        r = step(j, GROUP)
        qkv_send[r, :] = dot_nt(wqkv_ref[r, :], r1_ref[...]).astype(BF)
        qkv_copy(j).start()
        return carry

    lax.fori_loop(0, heads, qkv_body, 0)

    row_i = lax.broadcasted_iota(jnp.int32, (256, 256), 0)
    col_i = lax.broadcasted_iota(jnp.int32, (256, 256), 1)
    perm = (col_i == (row_i % 8) * 32 + row_i // 8).astype(F32).astype(BF)
    blocks = raw_rows // 512

    def raw_body(i, carry):
        slot = lax.rem(i, 2)
        raw_load(i, slot).wait()

        def block_body(b, inner):
            for u in range(4):
                base = pl.multiple_of(b * 2048 + u * 512, 512)
                pair = jnp.concatenate([raw_ref[slot, pl.ds(base, 256), :], raw_ref[slot, pl.ds(base + 256, 256), :]], axis=1)
                out = dot_nn(perm, pair)
                d = pl.ds(pl.multiple_of(i * (raw_rows // 32) + b * 64 + u * 16, 16), 16)
                for t in range(16):
                    for k, dst in ((0, wg_ref), (1, wu_ref)):
                        r = (2 * t + k) * 8
                        both = jnp.concatenate([out[r:r + 8, 0:128], out[r:r + 8, 128:256]], axis=0)
                        dst[d, t * 128:(t + 1) * 128] = both.astype(BF)
            return inner

        lax.fori_loop(0, blocks // 4, block_body, 0)

        @pl.when(i + 2 < raw_steps)
        def _():
            raw_load(i + 2, slot).start()
        return carry

    lax.fori_loop(0, raw_steps, raw_body, 0)

    scale = HEAD ** -0.5
    causal = (lax.broadcasted_iota(jnp.int32, (tokens, tokens), 0) <= lax.broadcasted_iota(jnp.int32, (tokens, tokens), 1))

    def rope(v, cos_t, sin_t):
        v = v.astype(F32)
        one, two = v[0:HALF], v[HALF:HEAD]
        return jnp.concatenate([one * cos_t - two * sin_t, two * cos_t + one * sin_t], axis=0).astype(BF)

    def unrope(v, cos_t, sin_t):
        v = v.astype(F32)
        one, two = v[0:HALF], v[HALF:HEAD]
        return jnp.concatenate([one * cos_t + two * sin_t, two * cos_t - one * sin_t], axis=0).astype(BF)

    def attn_body(j, carry):
        @pl.when(j == heads - 1)
        def _():
            qkv_copy(j).wait_send()
            for n in range(1, 5):
                ga_copy(n).start()
        qkv_copy(j).wait_recv()
        base = pl.multiple_of(j * GROUP, 32)
        r_q, r_k, r_v = (pl.ds(base + n * HEAD, HEAD) for n in range(3))
        cos_t, sin_t = cos_ref[...], sin_ref[...]
        q = rope(add_bf(qkv_send[r_q, :], qkv_recv[r_q, :]), cos_t, sin_t)
        k = rope(add_bf(qkv_send[r_k, :], qkv_recv[r_k, :]), cos_t, sin_t)
        v = add_bf(qkv_send[r_v, :], qkv_recv[r_v, :])
        rot_ref[r_q, :] = q
        rot_ref[r_k, :] = k
        rot_ref[r_v, :] = v
        scores = jnp.where(causal, dot_tn(k, q) * scale, -1e30)
        weight = jnp.exp(scores - jnp.max(scores, axis=0, keepdims=True))
        prob = weight / jnp.sum(weight, axis=0, keepdims=True)
        late_ref[j] = prob[:, rows:]
        early_ref[j] = prob[0:rows, 0:rows]
        mix_ref[pl.ds(pl.multiple_of(j * HEAD, 32), HEAD), :] = dot_nn(v, prob.astype(BF)).astype(BF)
        return carry

    lax.fori_loop(0, heads, attn_body, 0)
    stores.append(store(mix_ref, mix_hbm, 1))

    loads[4].wait()
    order = tuple(reversed(range(CHUNKS)))
    for c in order:
        r = pl.ds(c * rows, rows)
        part_ref[SLOT[AR_OUT], r, :] = dot_tn(mix_ref[:, c * rows:(c + 1) * rows], wout_ref[...]).astype(BF)
        p1_copy(AR_OUT, c).start()
    def gu_start(c, q):
        for k in range(2):
            gu_copy(c, q, k).start()

    def hidden_fwd(c):
        r = pl.ds(c * rows, rows)
        stage4(AR_OUT, c)
        h = add_bf(x_ref[r, :], full_ref[SLOT[AR_OUT], r, :])
        h_ref[r, :] = h
        h32 = h.astype(F32)
        stat_put(1 + c, jnp.sum(h32 * h32, axis=-1, keepdims=True), rows)

    def gate_up(c, at_once):
        r = pl.ds(c * rows, rows)
        inv2 = lax.rsqrt(stat_get(1 + c, rows) / full_width + EPSILON)
        inv2_ref[r, :] = inv2
        r2_ref[r, :] = (h_ref[r, :].astype(F32) * inv2 * g2_ref[...]).astype(BF)

        def gu_body(q, carry):
            for k, w_ref in ((0, wg_ref), (1, wu_ref)):
                dst = pl.ds(pl.multiple_of(k * ff + q * gu_cols, gu_cols), gu_cols)
                gu_send[r, dst] = dot_nn(r2_ref[r, :], w_ref[:, step(q, gu_cols)]).astype(BF)

            @pl.when(q < at_once)
            def _():
                gu_start(c, q)
            return carry

        lax.fori_loop(0, GU_PIECES, gu_body, 0)

    stage2(AR_OUT, 1)
    p2_copy(AR_OUT, 1).wait_send()
    stage2(AR_OUT, 0)
    stage3(AR_OUT, 1)
    hidden_fwd(1)
    for k in range(5, 8):
        ga_copy(k).start()
    gate_up(1, 2)
    stage3(AR_OUT, 0)
    hidden_fwd(0)
    gu_start(1, 2)
    gu_start(1, 3)
    gate_up(0, 0)
    tile = 512
    stores.append(store(r2_ref, r2_hbm, 2))

    for k in range(8):
        ga_copy(k).wait_recv()
    for c in order:
        p1_copy(AR_OUT, c).wait_send()
        p3_copy(AR_OUT, c).wait_send()
    p2_copy(AR_OUT, 0).wait_send()

    def mlp_pieces(c, lo, hi, then_at=None):
        r = pl.ds(c * rows, rows)
        if lo == 0:
            cot_ref[...] = jnp.zeros_like(cot_ref)

        def piece(q, carry):
            gu_copy(c, q, 0).wait_recv()
            gu_copy(c, q, 1).wait_recv()
            if then_at is not None:
                @pl.when(q == then_at)
                def _():
                    gu_start(0, 0)
            for n in range(gu_cols // 256):
                cg = pl.ds(pl.multiple_of(q * gu_cols + n * 256, 256), 256)
                cu = pl.ds(pl.multiple_of(ff + q * gu_cols + n * 256, 256), 256)
                gate = add_bf(gu_send[r, cg], gu_recv[r, cg]).astype(F32)
                up = add_bf(gu_send[r, cu], gu_recv[r, cu]).astype(F32)
                ga = add_bf(ga_send[r, cg], ga_recv[r, cg]).astype(F32)
                sig = 1.0 / (1.0 + jnp.exp(-gate))
                silu = gate * sig
                act_ref[r, cg] = (silu * up).astype(BF)
                dgu_ref[r, cg] = (ga * up * (sig * (1.0 + gate * (1.0 - sig)))).astype(BF)
                dgu_ref[r, cu] = (ga * silu).astype(BF)
            at_g = step(q, gu_cols)
            at_u = pl.ds(pl.multiple_of(ff + q * gu_cols, gu_cols), gu_cols)
            for n in range(width // tile):
                w = slice(n * tile, (n + 1) * tile)
                cot_ref[:, w] += dot_nt(dgu_ref[r, at_g], wg_ref[w, at_g]) + dot_nt(dgu_ref[r, at_u], wu_ref[w, at_g])
            return carry

        lax.fori_loop(lo, hi, piece, 0)

    def mlp_end(c):
        r = pl.ds(c * rows, rows)
        part_ref[SLOT[AR_R2], r, :] = cot_ref[...].astype(BF)
        p1_copy(AR_R2, c).start()
        unit = h_ref[r, :].astype(F32) * inv2_ref[r, :]
        dots_put(c, jnp.sum(cot_ref[...] * g2_ref[...] * unit, axis=-1, keepdims=True))

    def down_chunk(c):
        r = pl.ds(c * rows, rows)

        def down_body(n, carry):
            w = step(n, tile)
            part_ref[SLOT[AR_Y], r, w] = dot_nn(act_ref[r, :], wdown_ref[:, w]).astype(BF)
            return carry

        lax.fori_loop(0, width // tile, down_body, 0)
        p1_copy(AR_Y, c).start()

    dg1_ref[...] = jnp.zeros_like(dg1_ref)
    dg2_ref[...] = jnp.zeros_like(dg2_ref)

    def hidden_back(c, then=lambda: None):
        r = pl.ds(c * rows, rows)
        dots = dots_get(c)
        stage4(AR_R2, c)
        inv2 = inv2_ref[r, :]
        unit = h_ref[r, :].astype(F32) * inv2
        gin = full_ref[SLOT[AR_R2], r, :].astype(F32)
        norm = inv2 * (gin * g2_ref[...] - unit * (dots / full_width))
        dh_ref[r, :] = (dy_ref[r, :].astype(F32) + norm).astype(BF)
        gm_send[:, c * rows:(c + 1) * rows] = dot_nt(wout_ref[...], dh_ref[r, :]).astype(BF)
        for hf in range(2):
            gm_copy(c, hf).start()
        then()
        dg2_ref[...] += jnp.sum(gin * unit, axis=0, keepdims=True)

    def y_chunk(c):
        r = pl.ds(c * rows, rows)
        stage4(AR_Y, c)
        h_ref[r, :] = add_bf(h_ref[r, :], full_ref[SLOT[AR_Y], r, :])

    def scores_back(v, da, prob):
        dp = dot_tn(v, da).astype(BF).astype(F32)
        weighted = prob * dp
        return ((weighted - prob * jnp.sum(weighted, axis=0, keepdims=True)) * scale).astype(BF)

    def late_body(j, carry):
        base = pl.multiple_of(j * GROUP, 32)
        r_q, r_k, r_v = (pl.ds(base + n * HEAD, HEAD) for n in range(3))
        r_a = pl.ds(pl.multiple_of(j * HEAD, 32), HEAD)
        cos_t, sin_t = cos_ref[:, rows:], sin_ref[:, rows:]
        da = add_bf(gm_send[r_a, rows:], gm_recv[r_a, rows:])
        prob = late_ref[j]
        k = rot_ref[r_k, :]
        ds = scores_back(rot_ref[r_v, :], da, prob)
        dv = dot_nt(da, prob.astype(BF))
        dk = dot_nt(rot_ref[r_q, rows:], ds)
        dqkv_ref[r_q, rows:] = unrope(dot_nn(k, ds).astype(BF), cos_t, sin_t)
        dqkv_ref[r_k, rows:] = unrope(dk[:, rows:].astype(BF), cos_t, sin_t)
        dqkv_ref[r_v, rows:] = dv[:, rows:].astype(BF)
        kv_part[0, r_a, :] = dk[:, 0:rows]
        kv_part[1, r_a, :] = dv[:, 0:rows]
        return carry

    def early_body(j, carry):
        base = pl.multiple_of(j * GROUP, 32)
        r_q, r_k, r_v = (pl.ds(base + n * HEAD, HEAD) for n in range(3))
        r_a = pl.ds(pl.multiple_of(j * HEAD, 32), HEAD)
        cos_t, sin_t = cos_ref[:, 0:rows], sin_ref[:, 0:rows]
        da = add_bf(gm_send[r_a, 0:rows], gm_recv[r_a, 0:rows])
        prob = early_ref[j]
        ds = scores_back(rot_ref[r_v, 0:rows], da, prob)
        dv = kv_part[1, r_a, :] + dot_nt(da, prob.astype(BF))
        dk = kv_part[0, r_a, :] + dot_nt(rot_ref[r_q, 0:rows], ds)
        dqkv_ref[r_q, 0:rows] = unrope(dot_nn(rot_ref[r_k, 0:rows], ds).astype(BF), cos_t, sin_t)
        dqkv_ref[r_k, 0:rows] = unrope(dk.astype(BF), cos_t, sin_t)
        dqkv_ref[r_v, 0:rows] = dv.astype(BF)
        return carry

    def attn_back(c):
        for hf in range(2):
            gm_copy(c, hf).wait_recv()
            lax.fori_loop(hf * heads // 2, (hf + 1) * heads // 2, late_body if c else early_body, 0)
        r = pl.ds(c * rows, rows)
        cot = dot_tn(dqkv_ref[:, c * rows:(c + 1) * rows], wqkv_ref[...])
        part_ref[SLOT[AR_R1], r, :] = cot.astype(BF)
        p1_copy(AR_R1, c).start()
        unit = x_ref[r, :].astype(F32) * inv1_ref[r, :]
        dots_put(CHUNKS + c, jnp.sum(cot * g1_ref[...] * unit, axis=-1, keepdims=True))

    def input_back(c):
        r = pl.ds(c * rows, rows)
        dots = dots_get(CHUNKS + c)
        stage4(AR_R1, c)
        inv1 = inv1_ref[r, :]
        unit = x_ref[r, :].astype(F32) * inv1
        gin = full_ref[SLOT[AR_R1], r, :].astype(F32)
        norm = inv1 * (gin * g1_ref[...] - unit * (dots / full_width))
        dx_ref[r, :] = (dh_ref[r, :].astype(F32) + norm).astype(BF)
        stores.append(store(dx_ref.at[r], dx_hbm.at[r], 8 + c))
        dg1_ref[...] += jnp.sum(gin * unit, axis=0, keepdims=True)

    def rest_of_gate_up():
        gu_start(0, 2)
        gu_start(0, 3)

    mlp_pieces(1, 0, 4, then_at=2)
    mlp_end(1)
    gu_start(0, 1)
    stage2(AR_R2, 1)
    down_chunk(1)
    stage3(AR_R2, 1)
    stage2(AR_Y, 1)
    hidden_back(1, rest_of_gate_up)
    mlp_pieces(0, 0, 2)
    stage3(AR_Y, 1)
    attn_back(1)
    mlp_pieces(0, 2, 3)
    stage2(AR_R1, 1)
    mlp_pieces(0, 3, 4)
    mlp_end(0)
    stores.append(store(dgu_ref, dgu_hbm, 3))
    stores.append(store(act_ref, act_hbm, 4))
    stage2(AR_R2, 0)
    down_chunk(0)
    stage3(AR_R1, 1)
    y_chunk(1)
    stage3(AR_R2, 0)
    hidden_back(0)
    stores.append(store(dh_ref, dh_hbm, 5))
    stage2(AR_Y, 0)
    input_back(1)
    attn_back(0)
    stores.append(store(dqkv_ref, dqkv_hbm, 7))
    stage2(AR_R1, 0)
    stage3(AR_Y, 0)
    y_chunk(0)
    stores.append(store(h_ref, y_hbm, 6))
    stage3(AR_R1, 0)
    input_back(0)

    for k in range(3):
        stat_copy(k).wait_send()
    for k in range(2 * CHUNKS):
        for n in range(7):
            dots_copy(k, n).wait_send()
    for k in range(8):
        ga_copy(k).wait_send()
    for j in range(heads - 1):
        qkv_copy(j).wait_send()
    for c in range(CHUNKS):
        for q in range(GU_PIECES):
            for k in range(2):
                gu_copy(c, q, k).wait_send()
        for hf in range(2):
            gm_copy(c, hf).wait_send()
        for i in range(1, 4):
            p1_copy(i, c).wait_send()
            p2_copy(i, c).wait_send()
            p3_copy(i, c).wait_send()
    for copy in stores:
        copy.wait()


def run_layer(x_in, positions, gain_one, gain_two, w_qkv, w_out, w_gu, w_down, grad_out):
    tokens, width = x_in.shape
    ff = w_down.shape[0]
    chans = w_qkv.shape[0]
    mix = w_out.shape[0]
    heads = mix // HEAD
    rows = tokens // CHUNKS
    act = lambda n, dtype=BF: jax.ShapeDtypeStruct((tokens, n), dtype)
    any_spec = pl.BlockSpec(memory_space=pl.ANY)
    vmem_spec = pl.BlockSpec(memory_space=pltpu.VMEM)
    raw_rows = 128 * 32
    scratch = [
        pltpu.VMEM((tokens, width), BF), pltpu.VMEM((tokens, width), BF),
        pltpu.VMEM((chans, width), BF), pltpu.VMEM((mix, width), BF),
        pltpu.VMEM((width, ff), BF), pltpu.VMEM((width, ff), BF), pltpu.VMEM((ff, width), BF),
        pltpu.VMEM((2, raw_rows, 128), BF),
        pltpu.VMEM((1, width), F32), pltpu.VMEM((1, width), F32), pltpu.VMEM((HALF, tokens), F32), pltpu.VMEM((HALF, tokens), F32),
        pltpu.VMEM((tokens, width), BF), pltpu.VMEM((tokens, width), BF), pltpu.VMEM((tokens, width), BF), pltpu.VMEM((tokens, width), BF),
        pltpu.VMEM((tokens, ff), BF), pltpu.VMEM((tokens, 2 * ff), BF),
        pltpu.VMEM((chans, tokens), BF), pltpu.VMEM((heads, tokens, rows), F32), pltpu.VMEM((heads, rows, rows), F32), pltpu.VMEM((mix, tokens), BF), pltpu.VMEM((chans, tokens), BF),
        pltpu.VMEM((tokens, width), BF),
        pltpu.VMEM((2, mix, rows), F32), pltpu.VMEM((rows, width), F32), pltpu.VMEM((2 * CHUNKS, 8, 8, rows), F32),
        pltpu.VMEM((tokens, 1), F32), pltpu.VMEM((tokens, 1), F32),
        pltpu.VMEM((tokens, ff), BF), pltpu.VMEM((tokens, ff), BF),
        pltpu.VMEM((chans, tokens), BF), pltpu.VMEM((chans, tokens), BF),
        pltpu.VMEM((tokens, 2 * ff), BF), pltpu.VMEM((tokens, 2 * ff), BF),
        pltpu.VMEM((mix, tokens), BF), pltpu.VMEM((mix, tokens), BF),
        pltpu.VMEM((3, 8, tokens), F32), pltpu.VMEM((3, 8, tokens), F32),
        pltpu.VMEM((3, tokens, width), BF), pltpu.VMEM((3, tokens, width // 2), BF), pltpu.VMEM((3, tokens, width // 2), BF),
        pltpu.VMEM((3, tokens, width // 2), BF), pltpu.VMEM((3, tokens, width), BF),
        pltpu.SemaphoreType.DMA((5,)), pltpu.SemaphoreType.DMA((2,)), pltpu.SemaphoreType.DMA((8 + CHUNKS,)),
    ]
    for n in (3, 8, heads, 2 * GU_PIECES * CHUNKS, 2 * CHUNKS, 4 * CHUNKS, 4 * CHUNKS, 4 * CHUNKS):
        scratch += [pltpu.SemaphoreType.DMA((n,)), pltpu.SemaphoreType.DMA((n,))]
    scratch += [pltpu.SemaphoreType.DMA((7 * 2 * CHUNKS,)), pltpu.SemaphoreType.DMA((8 * 2 * CHUNKS,))]
    vec = jax.ShapeDtypeStruct((1, width), F32)
    return pl.pallas_call(
        layer_kernel,
        name="layer",
        out_shape=(act(width), act(width), vec, vec, act(width), jax.ShapeDtypeStruct((chans, tokens), BF),
                   jax.ShapeDtypeStruct((mix, tokens), BF), act(width), act(width), act(2 * ff), act(ff)),
        in_specs=[any_spec, any_spec, vmem_spec, vmem_spec, vmem_spec, any_spec, any_spec, any_spec, any_spec],
        out_specs=(any_spec, any_spec, vmem_spec, vmem_spec) + (any_spec,) * 7,
        scratch_shapes=scratch,
        compiler_params=pltpu.CompilerParams(collective_id=0, has_side_effects=True, vmem_limit_bytes=67000000),
    )(x_in, grad_out, gain_one, gain_two, positions, w_qkv, w_out, w_gu, w_down)


def grads_kernel(act_hbm, dy_hbm, r2_hbm, dgu_hbm, mix_hbm, dh_hbm, dqkv_hbm, r1_hbm, y_in, dx_in, dg1_in, dg2_in,
                 down_out, gu_out, wout_out, qkv_out, y_out, dx_out, dg1_out, dg2_out,
                 act_ref, dy_ref, r2_ref, dgu_ref, mix_ref, dh_ref, dqkv_ref, r1_ref, y_ref, dx_ref, rows_ref, inter_ref,
                 load_sem, rows_sem, inter_sem, end_sem):
    block = rows_ref.shape[1]
    pad = inter_ref.shape[1] // GU_BLOCK
    ff = dgu_ref.shape[1] // 2
    pairs = [(dqkv_hbm, dqkv_ref), (r1_hbm, r1_ref), (r2_hbm, r2_ref), (dgu_hbm, dgu_ref), (mix_hbm, mix_ref), (dh_hbm, dh_ref),
             (act_hbm, act_ref), (dy_hbm, dy_ref), (y_in, y_ref), (dx_in, dx_ref)]
    loads = [pltpu.make_async_copy(src, dst, load_sem.at[n]) for n, (src, dst) in enumerate(pairs)]
    for copy in loads:
        copy.start()
    dg1_out[...] = dg1_in[...].reshape(dg1_out.shape)
    dg2_out[...] = dg2_in[...].reshape(dg2_out.shape)

    slots = rows_ref.shape[0]

    def rows_copy(out, index, slot):
        return pltpu.make_async_copy(rows_ref.at[slot], out.at[step(index, block)], rows_sem.at[slot])

    def product(out, lhs_of, rhs_ref, first):
        def body(i, carry):
            slot = lax.rem(i + first, slots)

            @pl.when(i + first >= slots)
            def _():
                rows_copy(out, 0, slot).wait()
            rows_ref[slot] = lhs_of(i, rhs_ref)
            rows_copy(out, i, slot).start()
            return carry
        count = out.shape[0] // block
        lax.fori_loop(0, count, body, 0)
        return first + count

    def plain_rows(ref):
        return lambda i, rhs_ref: dot_nn(ref[step(i, block), :], rhs_ref[...])

    loads[0].wait()
    loads[1].wait()
    sent = product(qkv_out, plain_rows(dqkv_ref), r1_ref, 0)

    loads[2].wait()
    loads[3].wait()

    def inter_copy(index, slot):
        return pltpu.make_async_copy(inter_ref.at[slot].reshape(GU_BLOCK, pad, 128).at[:, 0:32, :],
                                     gu_out.at[step(index, GU_BLOCK)], inter_sem.at[slot])

    gu_steps = gu_out.shape[0] // GU_BLOCK

    def gu_body(i, carry):
        slot = lax.rem(i, 2)

        @pl.when(i >= 2)
        def _():
            inter_copy(0, slot).wait()
        lhs = r2_ref[:, step(i, GU_BLOCK)].T
        for k in range(2):
            for n in range(ff // 512):
                val = dot_nn(lhs, dgu_ref[:, k * ff + n * 512:k * ff + (n + 1) * 512])
                for t in range(4):
                    row = 2 * (4 * n + t) + k
                    inter_ref[slot, pl.ds(row, GU_BLOCK, stride=pad), :] = val[:, t * 128:(t + 1) * 128]
        inter_copy(i, slot).start()
        return carry

    lax.fori_loop(0, gu_steps, gu_body, 0)

    loads[4].wait()
    loads[5].wait()
    sent = product(wout_out, plain_rows(mix_ref), dh_ref, sent)
    loads[6].wait()
    loads[7].wait()
    sent = product(down_out, lambda i, rhs_ref: dot_tn(act_ref[:, step(i, block)], rhs_ref[...]), dy_ref, sent)
    loads[8].wait()
    loads[9].wait()
    ends = [pltpu.make_async_copy(y_ref, y_out, end_sem.at[0]), pltpu.make_async_copy(dx_ref, dx_out, end_sem.at[1])]
    for copy in ends:
        copy.start()
    for slot in range(slots):
        rows_copy(down_out, 0, slot).wait()
    for slot in range(2):
        inter_copy(0, slot).wait()
    for copy in ends:
        copy.wait()


GU_BLOCK = 128


def weight_grads(act, grad_out, r2, dgu, mix, dh, dqkv, r1, y, dx, dg1, dg2):
    tokens, width = r2.shape
    ff = act.shape[1]
    any_spec = pl.BlockSpec(memory_space=pl.ANY)
    vmem_spec = pl.BlockSpec(memory_space=pltpu.VMEM)
    out = lambda *shape: jax.ShapeDtypeStruct(shape, F32)
    like = lambda a: jax.ShapeDtypeStruct(a.shape, a.dtype)
    arrays = (act, grad_out, r2, dgu, mix, dh, dqkv, r1, y, dx)
    return pl.pallas_call(
        grads_kernel,
        name="weight_grads",
        in_specs=[any_spec] * 10 + [vmem_spec] * 2,
        out_specs=[any_spec] * 6 + [vmem_spec] * 2,
        out_shape=[out(ff, width), out(width, 32, 128), out(mix.shape[0], width), out(dqkv.shape[0], width), like(y), like(dx), out(width), out(width)],
        scratch_shapes=[pltpu.VMEM(a.shape, a.dtype) for a in arrays] + [
            pltpu.VMEM((4, 256, width), F32), pltpu.VMEM((2, GU_BLOCK * 40, 128), F32),
            pltpu.SemaphoreType.DMA((10,)), pltpu.SemaphoreType.DMA((4,)), pltpu.SemaphoreType.DMA((2,)), pltpu.SemaphoreType.DMA((2,))],
        compiler_params=pltpu.CompilerParams(vmem_limit_bytes=56 << 20),
    )(*arrays, dg1, dg2)


def solution(mesh):
    def per_device(x_in, positions, gain_one, gain_two, w_qkv, w_out, w_gu, w_down, grad_out):
        width, groups, chans = w_qkv.shape
        ff = w_down.shape[0]
        qkv_rows = w_qkv.transpose(1, 2, 0).reshape(groups * chans, width)
        gu_rows = w_gu.reshape(width, 2, ff // 128, 128).transpose(0, 2, 1, 3).reshape(width * 2 * (ff // 128), 128)
        y, dx, dg1, dg2, r1, dqkv, mix, dh, r2, dgu, act = run_layer(
            x_in, positions, gain_one, gain_two, qkv_rows, w_out, gu_rows, w_down, grad_out)
        d_down, d_gu, d_out, d_qkv, y, dx, dg1, dg2 = weight_grads(act, grad_out, r2, dgu, mix, dh, dqkv, r1, y, dx, dg1, dg2)
        d_gu = d_gu.reshape(width, ff // 128, 2, 128).transpose(0, 2, 1, 3).reshape(width, 2, ff)
        d_qkv = d_qkv.reshape(groups, chans, width).transpose(2, 0, 1)
        return y, dx, dg1, dg2, d_qkv, d_out, d_gu, d_down

    act_spec = P('dp', 'embed')
    in_specs = (act_spec, P('dp'), P('embed'), P('embed'), P('embed', 'heads', None), P('heads', 'embed'), P('embed', None, 'heads'), P('heads', 'embed'), act_spec)
    out_specs = (act_spec, act_spec, P(('dp', 'embed')), P(('dp', 'embed')), P(('dp', 'embed'), 'heads', None), P(('dp', 'heads'), 'embed'), P(('dp', 'embed'), None, 'heads'), P(('dp', 'heads'), 'embed'))
    return jax.shard_map(per_device, mesh=mesh, in_specs=in_specs, out_specs=out_specs, check_vma=False)
```

```python
import math

import jax
import jax.numpy as jnp
from jax import lax
from jax.experimental import pallas as pl
from jax.experimental.pallas import tpu as pltpu
from jax.sharding import PartitionSpec as P

EPSILON = 1e-5
ROPE_BASE = 10000.0
HEAD = 96
HALF = HEAD // 2
GROUP = 3 * HEAD
CHUNKS = 2
MESH = pl.DeviceIdType.MESH
BF = jnp.bfloat16
F32 = jnp.float32

AR_OUT, AR_R2, AR_Y, AR_R1 = range(4)
SLOT = (0, 1, 2, 0)
GU_PIECES = 4
EARLY, LATE = 0, 1


def dot_nn(lhs, rhs):
    return lax.dot_general(lhs, rhs, (((1,), (0,)), ((), ())), preferred_element_type=F32)


def dot_nt(lhs, rhs):
    return lax.dot_general(lhs, rhs, (((1,), (1,)), ((), ())), preferred_element_type=F32)


def dot_tn(lhs, rhs):
    return lax.dot_general(lhs, rhs, (((0,), (0,)), ((), ())), preferred_element_type=F32)


def add_bf(one, two):
    return (one.astype(F32) + two.astype(F32)).astype(BF)


def step(index, size):
    return pl.ds(pl.multiple_of(index * size, size), size)


def layer_kernel(x_hbm, dy_hbm, g1_in, g2_in, pos_in, wqkv_hbm, wout_hbm, wgu_hbm, wdown_hbm,
                 y_hbm, dx_hbm, dg1_ref, dg2_ref, r1_hbm, dqkv_hbm, mix_hbm, dh_hbm, r2_hbm, dgu_hbm, act_hbm,
                 x_ref, dy_ref, wqkv_ref, wout_ref, wg_ref, wu_ref, wdown_ref, raw_ref,
                 g1_ref, g2_ref, cos_ref, sin_ref, r1_ref, r2_ref, h_ref, dh_ref, act_ref, dgu_ref, rot_ref, late_ref, early_ref, mix_ref, dqkv_ref, dx_ref,
                 kv_part, cot_ref, dots_ref,
                 inv1_ref, inv2_ref,
                 ga_send, ga_recv, qkv_send, qkv_recv, gu_send, gu_recv, gm_send, gm_recv, stat_send, stat_recv,
                 part_ref, sib_ref, half_ref, far_ref, full_ref,
                 load_sem, raw_sem, store_sem,
                 st_s, st_r, ga_s, ga_r, qk_s, qk_r, gu_s, gu_r, gm_s, gm_r, p1_s, p1_r, p2_s, p2_r, p3_s, p3_r, dots_s, dots_r, mx_s, mx_r, rt_s, rt_r):
    tokens, width = x_ref.shape
    full_width = 2 * width
    ff = wdown_ref.shape[0]
    heads = wqkv_ref.shape[0] // GROUP
    half_width = width // 2
    rows = tokens // CHUNKS
    emb = lax.axis_index("embed")
    hid = lax.axis_index("heads")
    core = lax.rem(hid, 2)
    sibling = {"heads": hid + 1 - 2 * core}
    across = {"heads": lax.rem(hid + 2, 4)}
    partner = {"embed": 1 - emb}

    barrier = pltpu.get_barrier_semaphore()
    others = [{"embed": lax.rem(emb + n // 4, 2), "heads": lax.rem(hid + n, 4)} for n in range(1, 8)]
    for peer in others:
        pl.semaphore_signal(barrier, inc=1, device_id=peer, device_id_type=MESH)

    def load(src, dst, sem):
        return pltpu.make_async_copy(src, dst, load_sem.at[sem])

    loads = [load(x_hbm, x_ref, 0), load(dy_hbm, dy_ref, 1), load(wdown_hbm, wdown_ref, 2),
             load(wqkv_hbm, wqkv_ref, 3), load(wout_hbm, wout_ref, 4)]
    for copy in loads[:3]:
        copy.start()

    raw_rows = raw_ref.shape[1]
    raw_steps = wgu_hbm.shape[0] // raw_rows

    def raw_load(index, slot):
        return pltpu.make_async_copy(wgu_hbm.at[step(index, raw_rows)], raw_ref.at[slot], raw_sem.at[slot])

    def store(src, dst, sem):
        copy = pltpu.make_async_copy(src, dst, store_sem.at[sem])
        copy.start()
        return copy

    def send(src, dst, s_sem, r_sem, peer):
        return pltpu.make_async_remote_copy(src_ref=src, dst_ref=dst, send_sem=s_sem, recv_sem=r_sem,
                                            device_id=peer, device_id_type=MESH)

    def stat_copy(k):
        return send(stat_send.at[k], stat_recv.at[k], st_s.at[k], st_r.at[k], partner)

    ga_cols = ff // 8

    def ga_copy(k):
        cols = step(k, ga_cols)
        return send(ga_send.at[:, cols], ga_recv.at[:, cols], ga_s.at[k], ga_r.at[k], partner)

    def qkv_copy(j):
        r = step(j, GROUP)
        return send(qkv_send.at[r], qkv_recv.at[r], qk_s.at[j], qk_r.at[j], partner)

    half_heads = heads // 2

    def mine(i):
        return emb * half_heads + i

    def theirs(i):
        return (1 - emb) * half_heads + i

    def mix_rows(j):
        return pl.ds(pl.multiple_of(j * HEAD, 32), HEAD)

    def mix_copy(j):
        at = mix_ref.at[mix_rows(j)]
        return send(at, at, mx_s.at[j], mx_r.at[j], partner)

    def rot_copy(j):
        at = rot_ref.at[step(j, GROUP)]
        return send(at, at, rt_s.at[j], rt_r.at[j], partner)

    gu_cols = ff // GU_PIECES

    def gu_copy(c, q, k):
        at = (pl.ds(c * rows, rows), pl.ds(pl.multiple_of(k * ff + q * gu_cols, gu_cols), gu_cols))
        n = (c * GU_PIECES + q) * 2 + k
        return send(gu_send.at[at], gu_recv.at[at], gu_s.at[n], gu_r.at[n], partner)

    gm_rows = gm_send.shape[0] // 2

    def gm_copy(c, hf):
        at = (step(hf, gm_rows), pl.ds(c * rows, rows))
        return send(gm_send.at[at], gm_recv.at[at], gm_s.at[2 * c + hf], gm_r.at[2 * c + hf], partner)

    own = pl.ds(pl.multiple_of(core * half_width, half_width), half_width)
    other = pl.ds(pl.multiple_of((1 - core) * half_width, half_width), half_width)

    def p1_copy(i, c):
        r = pl.ds(c * rows, rows)
        k = i * CHUNKS + c
        return send(part_ref.at[SLOT[i], r, other], sib_ref.at[SLOT[i], r], p1_s.at[k], p1_r.at[k], sibling)

    def p2_copy(i, c):
        r = pl.ds(c * rows, rows)
        k = i * CHUNKS + c
        return send(half_ref.at[SLOT[i], r], far_ref.at[SLOT[i], r], p2_s.at[k], p2_r.at[k], across)

    def p3_copy(i, c):
        r = pl.ds(c * rows, rows)
        k = i * CHUNKS + c
        return send(full_ref.at[SLOT[i], r, own], full_ref.at[SLOT[i], r, own], p3_s.at[k], p3_r.at[k], sibling)

    def stage2(i, c):
        r = pl.ds(c * rows, rows)
        p1_copy(i, c).wait_recv()
        half_ref[SLOT[i], r, :] = add_bf(part_ref[SLOT[i], r, own], sib_ref[SLOT[i], r, :])
        p2_copy(i, c).start()

    def stage3(i, c):
        r = pl.ds(c * rows, rows)
        p2_copy(i, c).wait_recv()
        full_ref[SLOT[i], r, own] = add_bf(half_ref[SLOT[i], r, :], far_ref[SLOT[i], r, :])
        p3_copy(i, c).start()

    def stage4(i, c):
        p3_copy(i, c).wait_recv()

    def stat_put(k, col, n):
        flat = jnp.broadcast_to(col, (n, 128)).T[0:8, :]
        stat_send[k, :, 0:n] = flat
        stat_copy(k).start()

    def stat_get(k, n):
        stat_copy(k).wait_recv()
        total = stat_send[k, 0:1, 0:n] + stat_recv[k, 0:1, 0:n]
        return jnp.broadcast_to(total, (128, n)).T[:, 0:1]

    me = emb * 4 + hid

    def dots_copy(k, n):
        at = dots_ref.at[k, me]
        return send(at, at, dots_s.at[7 * k + n], dots_r.at[8 * k + me], others[n])

    def dots_put(k, col):
        dots_ref[k, me] = jnp.broadcast_to(col, (rows, 128)).T[0:8, :]
        for n in range(7):
            dots_copy(k, n).start()

    def dots_get(k):
        for n in range(7):
            src = lax.rem(emb + (n + 1) // 4, 2) * 4 + lax.rem(hid + n + 1, 4)
            at = dots_ref.at[k, src]
            send(at, at, dots_s.at[7 * k + n], dots_r.at[8 * k + src], others[n]).wait_recv()
        total = dots_ref[k, 0, 0:1, :]
        for n in range(1, 8):
            total = total + dots_ref[k, n, 0:1, :]
        return jnp.broadcast_to(total, (128, rows)).T[:, 0:1]

    place = pos_in[...].reshape(1, tokens).astype(F32)
    pair_i = lax.broadcasted_iota(jnp.int32, (HALF, 1), 0).astype(F32)
    angles = jnp.exp(pair_i * (-2.0 * math.log(ROPE_BASE) / HEAD)) * place
    cos_ref[...] = jnp.cos(angles)
    sin_ref[...] = jnp.sin(angles)
    g1_ref[...] = g1_in[...].reshape(1, width)
    g2_ref[...] = g2_in[...].reshape(1, width)
    loads[0].wait()
    x32 = x_ref[...].astype(F32)
    sq1 = jnp.sum(x32 * x32, axis=-1, keepdims=True)
    for copy in loads[3:]:
        copy.start()
    for slot in range(2):
        raw_load(slot, slot).start()

    def ga_body(k, carry):
        cols = step(k, ga_cols)
        ga_send[:, cols] = dot_nt(dy_ref[...], wdown_ref[cols, :]).astype(BF)
        return carry

    loads[1].wait()
    loads[2].wait()
    lax.fori_loop(0, 4, ga_body, 0)
    pl.semaphore_wait(barrier, 7)
    stat_put(0, sq1, tokens)
    ga_copy(0).start()
    lax.fori_loop(4, 8, ga_body, 0)
    inv1 = lax.rsqrt(stat_get(0, tokens) / full_width + EPSILON)
    inv1_ref[...] = inv1
    r1_ref[...] = (x_ref[...].astype(F32) * inv1 * g1_ref[...]).astype(BF)
    stores = [store(r1_ref, r1_hbm, 0)]

    loads[3].wait()

    def qkv_product(j):
        r = step(j, GROUP)
        qkv_send[r, :] = dot_nt(wqkv_ref[r, :], r1_ref[...]).astype(BF)

    def qkv_theirs(i, carry):
        qkv_product(theirs(i))
        qkv_copy(theirs(i)).start()
        return carry

    def qkv_mine(i, carry):
        qkv_product(mine(i))
        return carry

    lax.fori_loop(0, half_heads, qkv_theirs, 0)
    lax.fori_loop(0, half_heads, qkv_mine, 0)

    row_i = lax.broadcasted_iota(jnp.int32, (256, 256), 0)
    col_i = lax.broadcasted_iota(jnp.int32, (256, 256), 1)
    perm = (col_i == (row_i % 8) * 32 + row_i // 8).astype(F32).astype(BF)
    blocks = raw_rows // 512

    def raw_body(i, carry):
        slot = lax.rem(i, 2)
        raw_load(i, slot).wait()

        def block_body(b, inner):
            for u in range(4):
                base = pl.multiple_of(b * 2048 + u * 512, 512)
                pair = jnp.concatenate([raw_ref[slot, pl.ds(base, 256), :], raw_ref[slot, pl.ds(base + 256, 256), :]], axis=1)
                out = dot_nn(perm, pair)
                d = pl.ds(pl.multiple_of(i * (raw_rows // 32) + b * 64 + u * 16, 16), 16)
                for t in range(16):
                    for k, dst in ((0, wg_ref), (1, wu_ref)):
                        r = (2 * t + k) * 8
                        both = jnp.concatenate([out[r:r + 8, 0:128], out[r:r + 8, 128:256]], axis=0)
                        dst[d, t * 128:(t + 1) * 128] = both.astype(BF)
            return inner

        lax.fori_loop(0, blocks // 4, block_body, 0)

        @pl.when(i + 2 < raw_steps)
        def _():
            raw_load(i + 2, slot).start()
        return carry

    part_one, part_two = raw_steps // 2, raw_steps - raw_steps // 3
    lax.fori_loop(0, part_one, raw_body, 0)

    scale = HEAD ** -0.5
    causal = (lax.broadcasted_iota(jnp.int32, (tokens, tokens), 0) <= lax.broadcasted_iota(jnp.int32, (tokens, tokens), 1))

    def rope(v, cos_t, sin_t):
        v = v.astype(F32)
        one, two = v[0:HALF], v[HALF:HEAD]
        return jnp.concatenate([one * cos_t - two * sin_t, two * cos_t + one * sin_t], axis=0).astype(BF)

    def unrope(v, cos_t, sin_t):
        v = v.astype(F32)
        one, two = v[0:HALF], v[HALF:HEAD]
        return jnp.concatenate([one * cos_t + two * sin_t, two * cos_t - one * sin_t], axis=0).astype(BF)

    last = half_heads - 1

    def head_rows(j):
        base = pl.multiple_of(j * GROUP, 32)
        return tuple(pl.ds(base + n * HEAD, HEAD) for n in range(3))

    def probabilities(j, q, k):
        scores = jnp.where(causal, dot_tn(k, q) * scale, -1e30)
        weight = jnp.exp(scores - jnp.max(scores, axis=0, keepdims=True))
        prob = weight / jnp.sum(weight, axis=0, keepdims=True)
        late_ref[j] = prob[:, rows:]
        early_ref[j] = prob[0:rows, 0:rows]
        return prob

    def attn_body(i, carry):
        j = mine(i)

        @pl.when(i == last)
        def _():
            qkv_copy(theirs(i)).wait_send()
            ga_copy(1).start()
        qkv_copy(j).wait_recv()
        r_q, r_k, r_v = head_rows(j)
        cos_t, sin_t = cos_ref[...], sin_ref[...]
        q = rope(add_bf(qkv_send[r_q, :], qkv_recv[r_q, :]), cos_t, sin_t)
        k = rope(add_bf(qkv_send[r_k, :], qkv_recv[r_k, :]), cos_t, sin_t)
        v = add_bf(qkv_send[r_v, :], qkv_recv[r_v, :])
        rot_ref[r_q, :] = q
        rot_ref[r_k, :] = k
        rot_ref[r_v, :] = v
        prob = probabilities(j, q, k)
        mix_ref[mix_rows(j), :] = dot_nn(v, prob.astype(BF)).astype(BF)
        mix_copy(j).start()
        return carry

    lax.fori_loop(0, half_heads, attn_body, 0)
    for n in range(2, 6):
        ga_copy(n).start()
    lax.fori_loop(part_one, part_two, raw_body, 0)
    for i in range(half_heads):
        mix_copy(theirs(i)).wait_recv()
    stores.append(store(mix_ref, mix_hbm, 1))

    loads[4].wait()
    order = tuple(reversed(range(CHUNKS)))
    for c in order:
        r = pl.ds(c * rows, rows)
        part_ref[SLOT[AR_OUT], r, :] = dot_tn(mix_ref[:, c * rows:(c + 1) * rows], wout_ref[...]).astype(BF)
        p1_copy(AR_OUT, c).start()
    def gu_start(c, q):
        for k in range(2):
            gu_copy(c, q, k).start()

    def hidden_fwd(c):
        r = pl.ds(c * rows, rows)
        stage4(AR_OUT, c)
        h = add_bf(x_ref[r, :], full_ref[SLOT[AR_OUT], r, :])
        h_ref[r, :] = h
        h32 = h.astype(F32)
        stat_put(1 + c, jnp.sum(h32 * h32, axis=-1, keepdims=True), rows)

    def gate_up(c, at_once):
        r = pl.ds(c * rows, rows)
        inv2 = lax.rsqrt(stat_get(1 + c, rows) / full_width + EPSILON)
        inv2_ref[r, :] = inv2
        r2_ref[r, :] = (h_ref[r, :].astype(F32) * inv2 * g2_ref[...]).astype(BF)

        def gu_body(q, carry):
            for k, w_ref in ((0, wg_ref), (1, wu_ref)):
                dst = pl.ds(pl.multiple_of(k * ff + q * gu_cols, gu_cols), gu_cols)
                gu_send[r, dst] = dot_nn(r2_ref[r, :], w_ref[:, step(q, gu_cols)]).astype(BF)

            @pl.when(q < at_once)
            def _():
                gu_start(c, q)
            return carry

        lax.fori_loop(0, GU_PIECES, gu_body, 0)

    stage2(AR_OUT, LATE)
    lax.fori_loop(part_two, raw_steps, raw_body, 0)
    p2_copy(AR_OUT, LATE).wait_send()
    stage2(AR_OUT, EARLY)
    stage3(AR_OUT, LATE)
    hidden_fwd(LATE)
    for k in range(6, 8):
        ga_copy(k).start()
    gate_up(LATE, 2)
    stage3(AR_OUT, EARLY)
    hidden_fwd(EARLY)
    gu_start(LATE, 2)
    gu_start(LATE, 3)
    gate_up(EARLY, 0)
    tile = 512
    stores.append(store(r2_ref, r2_hbm, 2))

    for k in range(8):
        ga_copy(k).wait_recv()
    for c in order:
        p1_copy(AR_OUT, c).wait_send()
        p3_copy(AR_OUT, c).wait_send()
    p2_copy(AR_OUT, EARLY).wait_send()

    def mlp_pieces(c, lo, hi, then_at=None):
        r = pl.ds(c * rows, rows)
        if lo == 0:
            cot_ref[...] = jnp.zeros_like(cot_ref)

        def piece(q, carry):
            gu_copy(c, q, 0).wait_recv()
            gu_copy(c, q, 1).wait_recv()
            if then_at is not None:
                @pl.when(q == then_at)
                def _():
                    gu_start(EARLY, 0)
            for n in range(gu_cols // 256):
                cg = pl.ds(pl.multiple_of(q * gu_cols + n * 256, 256), 256)
                cu = pl.ds(pl.multiple_of(ff + q * gu_cols + n * 256, 256), 256)
                gate = add_bf(gu_send[r, cg], gu_recv[r, cg]).astype(F32)
                up = add_bf(gu_send[r, cu], gu_recv[r, cu]).astype(F32)
                ga = add_bf(ga_send[r, cg], ga_recv[r, cg]).astype(F32)
                sig = 1.0 / (1.0 + jnp.exp(-gate))
                silu = gate * sig
                act_ref[r, cg] = (silu * up).astype(BF)
                dgu_ref[r, cg] = (ga * up * (sig * (1.0 + gate * (1.0 - sig)))).astype(BF)
                dgu_ref[r, cu] = (ga * silu).astype(BF)
            at_g = step(q, gu_cols)
            at_u = pl.ds(pl.multiple_of(ff + q * gu_cols, gu_cols), gu_cols)
            for n in range(width // tile):
                w = slice(n * tile, (n + 1) * tile)
                cot_ref[:, w] += dot_nt(dgu_ref[r, at_g], wg_ref[w, at_g]) + dot_nt(dgu_ref[r, at_u], wu_ref[w, at_g])
            return carry

        lax.fori_loop(lo, hi, piece, 0)

    def mlp_end(c):
        r = pl.ds(c * rows, rows)
        part_ref[SLOT[AR_R2], r, :] = cot_ref[...].astype(BF)
        p1_copy(AR_R2, c).start()
        unit = h_ref[r, :].astype(F32) * inv2_ref[r, :]
        dots_put(c, jnp.sum(cot_ref[...] * g2_ref[...] * unit, axis=-1, keepdims=True))

    def down_chunk(c):
        r = pl.ds(c * rows, rows)

        def down_body(n, carry):
            w = step(n, tile)
            part_ref[SLOT[AR_Y], r, w] = dot_nn(act_ref[r, :], wdown_ref[:, w]).astype(BF)
            return carry

        lax.fori_loop(0, width // tile, down_body, 0)
        p1_copy(AR_Y, c).start()

    dg1_ref[...] = jnp.zeros_like(dg1_ref)
    dg2_ref[...] = jnp.zeros_like(dg2_ref)

    def hidden_back(c, then=lambda: None):
        r = pl.ds(c * rows, rows)
        dots = dots_get(c)
        stage4(AR_R2, c)
        inv2 = inv2_ref[r, :]
        unit = h_ref[r, :].astype(F32) * inv2
        gin = full_ref[SLOT[AR_R2], r, :].astype(F32)
        norm = inv2 * (gin * g2_ref[...] - unit * (dots / full_width))
        dh_ref[r, :] = (dy_ref[r, :].astype(F32) + norm).astype(BF)
        gm_send[:, c * rows:(c + 1) * rows] = dot_nt(wout_ref[...], dh_ref[r, :]).astype(BF)
        for hf in range(2):
            gm_copy(c, hf).start()
        then()
        dg2_ref[...] += jnp.sum(gin * unit, axis=0, keepdims=True)

    def y_chunk(c):
        r = pl.ds(c * rows, rows)
        stage4(AR_Y, c)
        h_ref[r, :] = add_bf(h_ref[r, :], full_ref[SLOT[AR_Y], r, :])

    def scores_back(v, da, prob):
        dp = dot_tn(v, da).astype(BF).astype(F32)
        weighted = prob * dp
        return ((weighted - prob * jnp.sum(weighted, axis=0, keepdims=True)) * scale).astype(BF)

    def late_head(j):
        r_q, r_k, r_v = head_rows(j)
        r_a = mix_rows(j)
        cos_t, sin_t = cos_ref[:, rows:], sin_ref[:, rows:]
        da = add_bf(gm_send[r_a, rows:], gm_recv[r_a, rows:])
        prob = late_ref[j]
        k = rot_ref[r_k, :]
        ds = scores_back(rot_ref[r_v, :], da, prob)
        dv = dot_nt(da, prob.astype(BF))
        dk = dot_nt(rot_ref[r_q, rows:], ds)
        dqkv_ref[r_q, rows:] = unrope(dot_nn(k, ds).astype(BF), cos_t, sin_t)
        dqkv_ref[r_k, rows:] = unrope(dk[:, rows:].astype(BF), cos_t, sin_t)
        dqkv_ref[r_v, rows:] = dv[:, rows:].astype(BF)
        kv_part[0, r_a, :] = dk[:, 0:rows]
        kv_part[1, r_a, :] = dv[:, 0:rows]

    def late_mine(i, carry):
        late_head(mine(i))
        return carry

    def late_theirs(i, carry):
        j = theirs(i)
        rot_copy(j).wait_recv()
        r_q, r_k, _ = head_rows(j)
        probabilities(j, rot_ref[r_q, :], rot_ref[r_k, :])
        late_head(j)
        return carry

    def early_body(j, carry):
        r_q, r_k, r_v = head_rows(j)
        r_a = mix_rows(j)
        cos_t, sin_t = cos_ref[:, 0:rows], sin_ref[:, 0:rows]
        da = add_bf(gm_send[r_a, 0:rows], gm_recv[r_a, 0:rows])
        prob = early_ref[j]
        ds = scores_back(rot_ref[r_v, 0:rows], da, prob)
        dv = kv_part[1, r_a, :] + dot_nt(da, prob.astype(BF))
        dk = kv_part[0, r_a, :] + dot_nt(rot_ref[r_q, 0:rows], ds)
        dqkv_ref[r_q, 0:rows] = unrope(dot_nn(rot_ref[r_k, 0:rows], ds).astype(BF), cos_t, sin_t)
        dqkv_ref[r_k, 0:rows] = unrope(dk.astype(BF), cos_t, sin_t)
        dqkv_ref[r_v, 0:rows] = dv.astype(BF)
        return carry

    def input_cot(c):
        r = pl.ds(c * rows, rows)
        cot = dot_tn(dqkv_ref[:, c * rows:(c + 1) * rows], wqkv_ref[...])
        part_ref[SLOT[AR_R1], r, :] = cot.astype(BF)
        p1_copy(AR_R1, c).start()
        unit = x_ref[r, :].astype(F32) * inv1_ref[r, :]
        dots_put(CHUNKS + c, jnp.sum(cot * g1_ref[...] * unit, axis=-1, keepdims=True))

    def input_back(c):
        r = pl.ds(c * rows, rows)
        dots = dots_get(CHUNKS + c)
        stage4(AR_R1, c)
        inv1 = inv1_ref[r, :]
        unit = x_ref[r, :].astype(F32) * inv1
        gin = full_ref[SLOT[AR_R1], r, :].astype(F32)
        norm = inv1 * (gin * g1_ref[...] - unit * (dots / full_width))
        dx_ref[r, :] = (dh_ref[r, :].astype(F32) + norm).astype(BF)
        stores.append(store(dx_ref.at[r], dx_hbm.at[r], 8 + c))
        dg1_ref[...] += jnp.sum(gin * unit, axis=0, keepdims=True)

    def rest_of_gate_up():
        gu_start(EARLY, 2)
        gu_start(EARLY, 3)
        for i in range(2):
            rot_copy(mine(i)).start()

    mlp_pieces(LATE, 0, GU_PIECES, then_at=2)
    mlp_end(LATE)
    gu_start(EARLY, 1)
    stage2(AR_R2, LATE)
    down_chunk(LATE)
    stage3(AR_R2, LATE)
    stage2(AR_Y, LATE)
    hidden_back(LATE, rest_of_gate_up)
    mlp_pieces(EARLY, 0, 2)
    stage3(AR_Y, LATE)
    gm_copy(LATE, emb).wait_recv()
    lax.fori_loop(0, half_heads, late_mine, 0)
    y_chunk(LATE)
    mlp_pieces(EARLY, 2, GU_PIECES)
    mlp_end(EARLY)
    for i in range(2, half_heads):
        rot_copy(mine(i)).start()
    stores.append(store(dgu_ref, dgu_hbm, 3))
    stores.append(store(act_ref, act_hbm, 4))
    stage2(AR_R2, EARLY)
    down_chunk(EARLY)
    gm_copy(LATE, 1 - emb).wait_recv()
    lax.fori_loop(0, 2, late_theirs, 0)
    stage3(AR_R2, EARLY)
    hidden_back(EARLY)
    stores.append(store(dh_ref, dh_hbm, 5))
    stage2(AR_Y, EARLY)
    lax.fori_loop(2, half_heads, late_theirs, 0)
    input_cot(LATE)
    gm_copy(EARLY, 0).wait_recv()
    stage2(AR_R1, LATE)
    lax.fori_loop(0, half_heads, early_body, 0)
    gm_copy(EARLY, 1).wait_recv()
    lax.fori_loop(half_heads, heads, early_body, 0)
    input_cot(EARLY)
    stores.append(store(dqkv_ref, dqkv_hbm, 7))
    stage3(AR_R1, LATE)
    stage2(AR_R1, EARLY)
    stage3(AR_Y, EARLY)
    input_back(LATE)
    y_chunk(EARLY)
    stores.append(store(h_ref, y_hbm, 6))
    stage3(AR_R1, EARLY)
    input_back(EARLY)

    for k in range(3):
        stat_copy(k).wait_send()
    for k in range(2 * CHUNKS):
        for n in range(7):
            dots_copy(k, n).wait_send()
    for k in range(8):
        ga_copy(k).wait_send()
    for i in range(half_heads):
        if i < last:
            qkv_copy(theirs(i)).wait_send()
        mix_copy(mine(i)).wait_send()
        rot_copy(mine(i)).wait_send()
    for c in range(CHUNKS):
        for q in range(GU_PIECES):
            for k in range(2):
                gu_copy(c, q, k).wait_send()
        for hf in range(2):
            gm_copy(c, hf).wait_send()
        for i in range(1, 4):
            p1_copy(i, c).wait_send()
            p2_copy(i, c).wait_send()
            p3_copy(i, c).wait_send()
    for copy in stores:
        copy.wait()


def run_layer(x_in, positions, gain_one, gain_two, w_qkv, w_out, w_gu, w_down, grad_out):
    tokens, width = x_in.shape
    ff = w_down.shape[0]
    chans = w_qkv.shape[0]
    mix = w_out.shape[0]
    heads = mix // HEAD
    rows = tokens // CHUNKS
    act = lambda n, dtype=BF: jax.ShapeDtypeStruct((tokens, n), dtype)
    any_spec = pl.BlockSpec(memory_space=pl.ANY)
    vmem_spec = pl.BlockSpec(memory_space=pltpu.VMEM)
    raw_rows = 128 * 32
    scratch = [
        pltpu.VMEM((tokens, width), BF), pltpu.VMEM((tokens, width), BF),
        pltpu.VMEM((chans, width), BF), pltpu.VMEM((mix, width), BF),
        pltpu.VMEM((width, ff), BF), pltpu.VMEM((width, ff), BF), pltpu.VMEM((ff, width), BF),
        pltpu.VMEM((2, raw_rows, 128), BF),
        pltpu.VMEM((1, width), F32), pltpu.VMEM((1, width), F32), pltpu.VMEM((HALF, tokens), F32), pltpu.VMEM((HALF, tokens), F32),
        pltpu.VMEM((tokens, width), BF), pltpu.VMEM((tokens, width), BF), pltpu.VMEM((tokens, width), BF), pltpu.VMEM((tokens, width), BF),
        pltpu.VMEM((tokens, ff), BF), pltpu.VMEM((tokens, 2 * ff), BF),
        pltpu.VMEM((chans, tokens), BF), pltpu.VMEM((heads, tokens, rows), F32), pltpu.VMEM((heads, rows, rows), F32), pltpu.VMEM((mix, tokens), BF), pltpu.VMEM((chans, tokens), BF),
        pltpu.VMEM((tokens, width), BF),
        pltpu.VMEM((2, mix, rows), F32), pltpu.VMEM((rows, width), F32), pltpu.VMEM((2 * CHUNKS, 8, 8, rows), F32),
        pltpu.VMEM((tokens, 1), F32), pltpu.VMEM((tokens, 1), F32),
        pltpu.VMEM((tokens, ff), BF), pltpu.VMEM((tokens, ff), BF),
        pltpu.VMEM((chans, tokens), BF), pltpu.VMEM((chans, tokens), BF),
        pltpu.VMEM((tokens, 2 * ff), BF), pltpu.VMEM((tokens, 2 * ff), BF),
        pltpu.VMEM((mix, tokens), BF), pltpu.VMEM((mix, tokens), BF),
        pltpu.VMEM((3, 8, tokens), F32), pltpu.VMEM((3, 8, tokens), F32),
        pltpu.VMEM((3, tokens, width), BF), pltpu.VMEM((3, tokens, width // 2), BF), pltpu.VMEM((3, tokens, width // 2), BF),
        pltpu.VMEM((3, tokens, width // 2), BF), pltpu.VMEM((3, tokens, width), BF),
        pltpu.SemaphoreType.DMA((5,)), pltpu.SemaphoreType.DMA((2,)), pltpu.SemaphoreType.DMA((8 + CHUNKS,)),
    ]
    for n in (3, 8, heads, 2 * GU_PIECES * CHUNKS, 2 * CHUNKS, 4 * CHUNKS, 4 * CHUNKS, 4 * CHUNKS):
        scratch += [pltpu.SemaphoreType.DMA((n,)), pltpu.SemaphoreType.DMA((n,))]
    for n in (7 * 2 * CHUNKS, 8 * 2 * CHUNKS, heads, heads, heads, heads):
        scratch += [pltpu.SemaphoreType.DMA((n,))]
    vec = jax.ShapeDtypeStruct((1, width), F32)
    return pl.pallas_call(
        layer_kernel,
        name="layer",
        out_shape=(act(width), act(width), vec, vec, act(width), jax.ShapeDtypeStruct((chans, tokens), BF),
                   jax.ShapeDtypeStruct((mix, tokens), BF), act(width), act(width), act(2 * ff), act(ff)),
        in_specs=[any_spec, any_spec, vmem_spec, vmem_spec, vmem_spec, any_spec, any_spec, any_spec, any_spec],
        out_specs=(any_spec, any_spec, vmem_spec, vmem_spec) + (any_spec,) * 7,
        scratch_shapes=scratch,
        compiler_params=pltpu.CompilerParams(collective_id=0, has_side_effects=True, vmem_limit_bytes=67000000),
    )(x_in, grad_out, gain_one, gain_two, positions, w_qkv, w_out, w_gu, w_down)


def grads_kernel(act_hbm, dy_hbm, r2_hbm, dgu_hbm, mix_hbm, dh_hbm, dqkv_hbm, r1_hbm, y_in, dx_in, dg1_in, dg2_in,
                 down_out, gu_out, wout_out, qkv_out, y_out, dx_out, dg1_out, dg2_out,
                 act_ref, dy_ref, r2_ref, dgu_ref, mix_ref, dh_ref, dqkv_ref, r1_ref, y_ref, dx_ref, rows_ref, inter_ref,
                 load_sem, rows_sem, inter_sem, end_sem):
    block = rows_ref.shape[1]
    pad = inter_ref.shape[1] // GU_BLOCK
    ff = dgu_ref.shape[1] // 2
    pairs = [(dqkv_hbm, dqkv_ref), (r1_hbm, r1_ref), (r2_hbm, r2_ref), (dgu_hbm, dgu_ref), (mix_hbm, mix_ref), (dh_hbm, dh_ref),
             (act_hbm, act_ref), (dy_hbm, dy_ref), (y_in, y_ref), (dx_in, dx_ref)]
    loads = [pltpu.make_async_copy(src, dst, load_sem.at[n]) for n, (src, dst) in enumerate(pairs)]
    for copy in loads[:2]:
        copy.start()
    dg1_out[...] = dg1_in[...].reshape(dg1_out.shape)
    dg2_out[...] = dg2_in[...].reshape(dg2_out.shape)

    slots = rows_ref.shape[0]

    def rows_copy(out, index, slot):
        return pltpu.make_async_copy(rows_ref.at[slot], out.at[step(index, block)], rows_sem.at[slot])

    def product(out, lhs_of, rhs_ref, first):
        def body(i, carry):
            slot = lax.rem(i + first, slots)

            @pl.when(i + first >= slots)
            def _():
                rows_copy(out, 0, slot).wait()
            rows_ref[slot] = lhs_of(i, rhs_ref)
            rows_copy(out, i, slot).start()
            return carry
        count = out.shape[0] // block
        lax.fori_loop(0, count, body, 0)
        return first + count

    def plain_rows(ref):
        return lambda i, rhs_ref: dot_nn(ref[step(i, block), :], rhs_ref[...])

    loads[0].wait()
    loads[1].wait()
    for copy in loads[2:]:
        copy.start()
    sent = product(qkv_out, plain_rows(dqkv_ref), r1_ref, 0)

    loads[2].wait()
    loads[3].wait()

    def inter_copy(index, slot):
        return pltpu.make_async_copy(inter_ref.at[slot].reshape(GU_BLOCK, pad, 128).at[:, 0:32, :],
                                     gu_out.at[step(index, GU_BLOCK)], inter_sem.at[slot])

    gu_steps = gu_out.shape[0] // GU_BLOCK

    def gu_body(i, carry):
        slot = lax.rem(i, slots)

        @pl.when(i >= slots)
        def _():
            inter_copy(0, slot).wait()
        lhs = r2_ref[:, step(i, GU_BLOCK)].T
        for k in range(2):
            for n in range(ff // 512):
                val = dot_nn(lhs, dgu_ref[:, k * ff + n * 512:k * ff + (n + 1) * 512])
                for t in range(4):
                    row = 2 * (4 * n + t) + k
                    inter_ref[slot, pl.ds(row, GU_BLOCK, stride=pad), :] = val[:, t * 128:(t + 1) * 128]
        inter_copy(i, slot).start()
        return carry

    lax.fori_loop(0, gu_steps, gu_body, 0)

    loads[4].wait()
    loads[5].wait()
    sent = product(wout_out, plain_rows(mix_ref), dh_ref, sent)
    loads[6].wait()
    loads[7].wait()
    sent = product(down_out, lambda i, rhs_ref: dot_tn(act_ref[:, step(i, block)], rhs_ref[...]), dy_ref, sent)
    loads[8].wait()
    loads[9].wait()
    ends = [pltpu.make_async_copy(y_ref, y_out, end_sem.at[0]), pltpu.make_async_copy(dx_ref, dx_out, end_sem.at[1])]
    for copy in ends:
        copy.start()
    for slot in range(slots):
        rows_copy(down_out, 0, slot).wait()
        inter_copy(0, slot).wait()
    for copy in ends:
        copy.wait()


GU_BLOCK = 128


def weight_grads(act, grad_out, r2, dgu, mix, dh, dqkv, r1, y, dx, dg1, dg2):
    tokens, width = r2.shape
    ff = act.shape[1]
    any_spec = pl.BlockSpec(memory_space=pl.ANY)
    vmem_spec = pl.BlockSpec(memory_space=pltpu.VMEM)
    out = lambda *shape: jax.ShapeDtypeStruct(shape, F32)
    like = lambda a: jax.ShapeDtypeStruct(a.shape, a.dtype)
    arrays = (act, grad_out, r2, dgu, mix, dh, dqkv, r1, y, dx)
    return pl.pallas_call(
        grads_kernel,
        name="weight_grads",
        in_specs=[any_spec] * 10 + [vmem_spec] * 2,
        out_specs=[any_spec] * 6 + [vmem_spec] * 2,
        out_shape=[out(ff, width), out(width, 32, 128), out(mix.shape[0], width), out(dqkv.shape[0], width), like(y), like(dx), out(width), out(width)],
        scratch_shapes=[pltpu.VMEM(a.shape, a.dtype) for a in arrays] + [
            pltpu.VMEM((4, 256, width), F32), pltpu.VMEM((4, GU_BLOCK * 40, 128), F32),
            pltpu.SemaphoreType.DMA((10,)), pltpu.SemaphoreType.DMA((4,)), pltpu.SemaphoreType.DMA((4,)), pltpu.SemaphoreType.DMA((2,))],
        compiler_params=pltpu.CompilerParams(vmem_limit_bytes=56 << 20),
    )(*arrays, dg1, dg2)


def solution(mesh):
    def per_device(x_in, positions, gain_one, gain_two, w_qkv, w_out, w_gu, w_down, grad_out):
        width, groups, chans = w_qkv.shape
        ff = w_down.shape[0]
        qkv_rows = w_qkv.transpose(1, 2, 0).reshape(groups * chans, width)
        gu_rows = w_gu.reshape(width, 2, ff // 128, 128).transpose(0, 2, 1, 3).reshape(width * 2 * (ff // 128), 128)
        y, dx, dg1, dg2, r1, dqkv, mix, dh, r2, dgu, act = run_layer(
            x_in, positions, gain_one, gain_two, qkv_rows, w_out, gu_rows, w_down, grad_out)
        d_down, d_gu, d_out, d_qkv, y, dx, dg1, dg2 = weight_grads(act, grad_out, r2, dgu, mix, dh, dqkv, r1, y, dx, dg1, dg2)
        d_gu = d_gu.reshape(width, ff // 128, 2, 128).transpose(0, 2, 1, 3).reshape(width, 2, ff)
        d_qkv = d_qkv.reshape(groups, chans, width).transpose(2, 0, 1)
        return y, dx, dg1, dg2, d_qkv, d_out, d_gu, d_down

    act_spec = P('dp', 'embed')
    in_specs = (act_spec, P('dp'), P('embed'), P('embed'), P('embed', 'heads', None), P('heads', 'embed'), P('embed', None, 'heads'), P('heads', 'embed'), act_spec)
    out_specs = (act_spec, act_spec, P(('dp', 'embed')), P(('dp', 'embed')), P(('dp', 'embed'), 'heads', None), P(('dp', 'heads'), 'embed'), P(('dp', 'embed'), None, 'heads'), P(('dp', 'heads'), 'embed'))
    return jax.shard_map(per_device, mesh=mesh, in_specs=in_specs, out_specs=out_specs, check_vma=False)
```

```python
import math

import jax
import jax.numpy as jnp
from jax import lax
from jax.experimental import pallas as pl
from jax.experimental.pallas import tpu as pltpu
from jax.sharding import PartitionSpec as P

EPSILON = 1e-5
ROPE_BASE = 10000.0
HEAD = 96
HALF = HEAD // 2
GROUP = 3 * HEAD
CHUNKS = 2
MESH = pl.DeviceIdType.MESH
BF = jnp.bfloat16
F32 = jnp.float32

AR_OUT, AR_R2, AR_Y, AR_R1 = range(4)
SLOT = (0, 1, 2, 0)
GU_PIECES = 4
EARLY, LATE = 0, 1


def dot_nn(lhs, rhs):
    return lax.dot_general(lhs, rhs, (((1,), (0,)), ((), ())), preferred_element_type=F32)


def dot_nt(lhs, rhs):
    return lax.dot_general(lhs, rhs, (((1,), (1,)), ((), ())), preferred_element_type=F32)


def dot_tn(lhs, rhs):
    return lax.dot_general(lhs, rhs, (((0,), (0,)), ((), ())), preferred_element_type=F32)


def add_bf(one, two):
    return (one.astype(F32) + two.astype(F32)).astype(BF)


def step(index, size):
    return pl.ds(pl.multiple_of(index * size, size), size)


def layer_kernel(x_hbm, dy_hbm, g1_in, g2_in, pos_in, wqkv_hbm, wout_hbm, wgu_hbm, wdown_hbm,
                 y_hbm, dx_hbm, dg1_hbm, dg2_hbm, r1_hbm, dqkv_hbm, mix_hbm, dh_hbm, r2_hbm, dgu_hbm, act_hbm,
                 x_ref, dy_ref, wqkv_ref, wout_ref, wg_ref, wu_ref, wdown_ref, raw_ref,
                 g1_ref, g2_ref, cos_ref, sin_ref, r1_ref, r2_ref, h_ref, dh_ref, act_ref, dgu_ref, rot_ref, late_ref, early_ref, mix_ref, dqkv_ref, dx_ref,
                 kv_part, cot_ref, dots_ref, dg1_ref, dg2_ref,
                 inv1_ref, inv2_ref,
                 ga_send, ga_recv, qkv_send, qkv_recv, gu_send, gu_recv, gm_send, gm_recv, stat_send, stat_recv,
                 part_ref, sib_ref, half_ref, far_ref, full_ref,
                 load_sem, raw_sem, store_sem,
                 st_s, st_r, ga_s, ga_r, qk_s, qk_r, gu_s, gu_r, gm_s, gm_r, p1_s, p1_r, p2_s, p2_r, p3_s, p3_r, dots_s, dots_r, mx_s, mx_r, rt_s, rt_r):
    tokens, width = x_ref.shape
    full_width = 2 * width
    ff = wdown_ref.shape[0]
    heads = wqkv_ref.shape[0] // GROUP
    half_width = width // 2
    rows = tokens // CHUNKS
    emb = lax.axis_index("embed")
    hid = lax.axis_index("heads")
    core = lax.rem(hid, 2)
    sibling = {"heads": hid + 1 - 2 * core}
    across = {"heads": lax.rem(hid + 2, 4)}
    partner = {"embed": 1 - emb}

    barrier = pltpu.get_barrier_semaphore()
    others = [{"embed": lax.rem(emb + n // 4, 2), "heads": lax.rem(hid + n, 4)} for n in range(1, 8)]
    for peer in others:
        pl.semaphore_signal(barrier, inc=1, device_id=peer, device_id_type=MESH)

    def load(src, dst, sem):
        return pltpu.make_async_copy(src, dst, load_sem.at[sem])

    loads = [load(x_hbm, x_ref, 0), load(dy_hbm, dy_ref, 1), load(wdown_hbm, wdown_ref, 2),
             load(wqkv_hbm, wqkv_ref, 3), load(wout_hbm, wout_ref, 4)]
    for copy in loads[:3]:
        copy.start()

    raw_rows = raw_ref.shape[1]
    raw_steps = wgu_hbm.shape[0] // raw_rows

    def raw_load(index, slot):
        return pltpu.make_async_copy(wgu_hbm.at[step(index, raw_rows)], raw_ref.at[slot], raw_sem.at[slot])

    def store(src, dst, sem):
        copy = pltpu.make_async_copy(src, dst, store_sem.at[sem])
        copy.start()
        return copy

    def send(src, dst, s_sem, r_sem, peer):
        return pltpu.make_async_remote_copy(src_ref=src, dst_ref=dst, send_sem=s_sem, recv_sem=r_sem,
                                            device_id=peer, device_id_type=MESH)

    def stat_copy(k):
        return send(stat_send.at[k], stat_recv.at[k], st_s.at[k], st_r.at[k], partner)

    ga_cols = ff // 8

    def ga_copy(k):
        cols = step(k, ga_cols)
        return send(ga_send.at[:, cols], ga_recv.at[:, cols], ga_s.at[k], ga_r.at[k], partner)

    def qkv_copy(j):
        r = step(j, GROUP)
        return send(qkv_send.at[r], qkv_recv.at[r], qk_s.at[j], qk_r.at[j], partner)

    half_heads = heads // 2

    def mine(i):
        return emb * half_heads + i

    def theirs(i):
        return (1 - emb) * half_heads + i

    def mix_rows(j):
        return pl.ds(pl.multiple_of(j * HEAD, 32), HEAD)

    def mix_copy(j):
        at = mix_ref.at[mix_rows(j)]
        return send(at, at, mx_s.at[j], mx_r.at[j], partner)

    def rot_copy(j):
        at = rot_ref.at[step(j, GROUP)]
        return send(at, at, rt_s.at[j], rt_r.at[j], partner)

    gu_cols = ff // GU_PIECES

    def gu_copy(c, q, k):
        at = (pl.ds(c * rows, rows), pl.ds(pl.multiple_of(k * ff + q * gu_cols, gu_cols), gu_cols))
        n = (c * GU_PIECES + q) * 2 + k
        return send(gu_send.at[at], gu_recv.at[at], gu_s.at[n], gu_r.at[n], partner)

    gm_rows = gm_send.shape[0] // 2

    def gm_copy(c, hf):
        at = (step(hf, gm_rows), pl.ds(c * rows, rows))
        return send(gm_send.at[at], gm_recv.at[at], gm_s.at[2 * c + hf], gm_r.at[2 * c + hf], partner)

    own = pl.ds(pl.multiple_of(core * half_width, half_width), half_width)
    other = pl.ds(pl.multiple_of((1 - core) * half_width, half_width), half_width)

    def p1_copy(i, c):
        r = pl.ds(c * rows, rows)
        k = i * CHUNKS + c
        return send(part_ref.at[SLOT[i], r, other], sib_ref.at[SLOT[i], r], p1_s.at[k], p1_r.at[k], sibling)

    def p2_copy(i, c):
        r = pl.ds(c * rows, rows)
        k = i * CHUNKS + c
        return send(half_ref.at[SLOT[i], r], far_ref.at[SLOT[i], r], p2_s.at[k], p2_r.at[k], across)

    def p3_copy(i, c):
        r = pl.ds(c * rows, rows)
        k = i * CHUNKS + c
        return send(full_ref.at[SLOT[i], r, own], full_ref.at[SLOT[i], r, own], p3_s.at[k], p3_r.at[k], sibling)

    def stage2(i, c):
        r = pl.ds(c * rows, rows)
        p1_copy(i, c).wait_recv()
        half_ref[SLOT[i], r, :] = add_bf(part_ref[SLOT[i], r, own], sib_ref[SLOT[i], r, :])
        p2_copy(i, c).start()

    def stage3(i, c):
        r = pl.ds(c * rows, rows)
        p2_copy(i, c).wait_recv()
        full_ref[SLOT[i], r, own] = add_bf(half_ref[SLOT[i], r, :], far_ref[SLOT[i], r, :])
        p3_copy(i, c).start()

    def stage4(i, c):
        p3_copy(i, c).wait_recv()

    def stat_put(k, col, n):
        flat = jnp.broadcast_to(col, (n, 128)).T[0:8, :]
        stat_send[k, :, 0:n] = flat
        stat_copy(k).start()

    def stat_get(k, n):
        stat_copy(k).wait_recv()
        total = stat_send[k, 0:1, 0:n] + stat_recv[k, 0:1, 0:n]
        return jnp.broadcast_to(total, (128, n)).T[:, 0:1]

    me = emb * 4 + hid

    def dots_copy(k, n):
        at = dots_ref.at[k, me]
        return send(at, at, dots_s.at[7 * k + n], dots_r.at[8 * k + me], others[n])

    def dots_put(k, col):
        dots_ref[k, me] = jnp.broadcast_to(col, (rows, 128)).T[0:8, :]
        for n in range(7):
            dots_copy(k, n).start()

    def dots_get(k):
        for n in range(7):
            src = lax.rem(emb + (n + 1) // 4, 2) * 4 + lax.rem(hid + n + 1, 4)
            at = dots_ref.at[k, src]
            send(at, at, dots_s.at[7 * k + n], dots_r.at[8 * k + src], others[n]).wait_recv()
        total = dots_ref[k, 0, 0:1, :]
        for n in range(1, 8):
            total = total + dots_ref[k, n, 0:1, :]
        return jnp.broadcast_to(total, (128, rows)).T[:, 0:1]

    place = pos_in[...].reshape(1, tokens).astype(F32)
    pair_i = lax.broadcasted_iota(jnp.int32, (HALF, 1), 0).astype(F32)
    angles = jnp.exp(pair_i * (-2.0 * math.log(ROPE_BASE) / HEAD)) * place
    cos_ref[...] = jnp.cos(angles)
    sin_ref[...] = jnp.sin(angles)
    g1_ref[...] = g1_in[...].reshape(1, width)
    g2_ref[...] = g2_in[...].reshape(1, width)
    loads[0].wait()
    x32 = x_ref[...].astype(F32)
    sq1 = jnp.sum(x32 * x32, axis=-1, keepdims=True)
    for copy in loads[3:]:
        copy.start()
    for slot in range(2):
        raw_load(slot, slot).start()

    def ga_body(k, carry):
        cols = step(k, ga_cols)
        ga_send[:, cols] = dot_nt(dy_ref[...], wdown_ref[cols, :]).astype(BF)
        return carry

    loads[1].wait()
    loads[2].wait()
    lax.fori_loop(0, 4, ga_body, 0)
    pl.semaphore_wait(barrier, 7)
    stat_put(0, sq1, tokens)
    ga_copy(0).start()
    lax.fori_loop(4, 8, ga_body, 0)
    inv1 = lax.rsqrt(stat_get(0, tokens) / full_width + EPSILON)
    inv1_ref[...] = inv1
    r1_ref[...] = (x_ref[...].astype(F32) * inv1 * g1_ref[...]).astype(BF)
    stores = [store(r1_ref, r1_hbm, 0)]

    loads[3].wait()

    def qkv_product(j):
        r = step(j, GROUP)
        qkv_send[r, :] = dot_nt(wqkv_ref[r, :], r1_ref[...]).astype(BF)

    def qkv_theirs(i, carry):
        qkv_product(theirs(i))
        qkv_copy(theirs(i)).start()
        return carry

    def qkv_mine(i, carry):
        qkv_product(mine(i))
        return carry

    lax.fori_loop(0, half_heads, qkv_theirs, 0)
    lax.fori_loop(0, half_heads, qkv_mine, 0)

    row_i = lax.broadcasted_iota(jnp.int32, (256, 256), 0)
    col_i = lax.broadcasted_iota(jnp.int32, (256, 256), 1)
    perm = (col_i == (row_i % 8) * 32 + row_i // 8).astype(F32).astype(BF)
    blocks = raw_rows // 512

    def raw_body(i, carry):
        slot = lax.rem(i, 2)
        raw_load(i, slot).wait()

        def block_body(b, inner):
            for u in range(4):
                base = pl.multiple_of(b * 2048 + u * 512, 512)
                pair = jnp.concatenate([raw_ref[slot, pl.ds(base, 256), :], raw_ref[slot, pl.ds(base + 256, 256), :]], axis=1)
                out = dot_nn(perm, pair)
                d = pl.ds(pl.multiple_of(i * (raw_rows // 32) + b * 64 + u * 16, 16), 16)
                for t in range(16):
                    for k, dst in ((0, wg_ref), (1, wu_ref)):
                        r = (2 * t + k) * 8
                        both = jnp.concatenate([out[r:r + 8, 0:128], out[r:r + 8, 128:256]], axis=0)
                        dst[d, t * 128:(t + 1) * 128] = both.astype(BF)
            return inner

        lax.fori_loop(0, blocks // 4, block_body, 0)

        @pl.when(i + 2 < raw_steps)
        def _():
            raw_load(i + 2, slot).start()
        return carry

    part_one, part_two = raw_steps // 2, raw_steps - raw_steps // 3
    lax.fori_loop(0, part_one, raw_body, 0)

    scale = HEAD ** -0.5
    causal = (lax.broadcasted_iota(jnp.int32, (tokens, tokens), 0) <= lax.broadcasted_iota(jnp.int32, (tokens, tokens), 1))

    def rope(v, cos_t, sin_t):
        v = v.astype(F32)
        one, two = v[0:HALF], v[HALF:HEAD]
        return jnp.concatenate([one * cos_t - two * sin_t, two * cos_t + one * sin_t], axis=0).astype(BF)

    def unrope(v, cos_t, sin_t):
        v = v.astype(F32)
        one, two = v[0:HALF], v[HALF:HEAD]
        return jnp.concatenate([one * cos_t + two * sin_t, two * cos_t - one * sin_t], axis=0).astype(BF)

    last = half_heads - 1

    def head_rows(j):
        base = pl.multiple_of(j * GROUP, 32)
        return tuple(pl.ds(base + n * HEAD, HEAD) for n in range(3))

    def probabilities(j, q, k):
        scores = jnp.where(causal, dot_tn(k, q) * scale, -1e30)
        weight = jnp.exp(scores - jnp.max(scores, axis=0, keepdims=True))
        prob = weight / jnp.sum(weight, axis=0, keepdims=True)
        late_ref[j] = prob[:, rows:]
        early_ref[j] = prob[0:rows, 0:rows]
        return prob

    def attn_body(i, carry):
        j = mine(i)

        @pl.when(i == last)
        def _():
            qkv_copy(theirs(i)).wait_send()
            ga_copy(1).start()
        qkv_copy(j).wait_recv()
        r_q, r_k, r_v = head_rows(j)
        cos_t, sin_t = cos_ref[...], sin_ref[...]
        q = rope(add_bf(qkv_send[r_q, :], qkv_recv[r_q, :]), cos_t, sin_t)
        k = rope(add_bf(qkv_send[r_k, :], qkv_recv[r_k, :]), cos_t, sin_t)
        v = add_bf(qkv_send[r_v, :], qkv_recv[r_v, :])
        rot_ref[r_q, :] = q
        rot_ref[r_k, :] = k
        rot_ref[r_v, :] = v
        prob = probabilities(j, q, k)
        mix_ref[mix_rows(j), :] = dot_nn(v, prob.astype(BF)).astype(BF)
        mix_copy(j).start()
        return carry

    lax.fori_loop(0, half_heads, attn_body, 0)
    for n in range(2, 6):
        ga_copy(n).start()
    lax.fori_loop(part_one, part_two, raw_body, 0)
    for i in range(half_heads):
        mix_copy(theirs(i)).wait_recv()
    stores.append(store(mix_ref, mix_hbm, 1))

    loads[4].wait()
    order = tuple(reversed(range(CHUNKS)))
    for c in order:
        r = pl.ds(c * rows, rows)
        part_ref[SLOT[AR_OUT], r, :] = dot_tn(mix_ref[:, c * rows:(c + 1) * rows], wout_ref[...]).astype(BF)
        p1_copy(AR_OUT, c).start()
    def gu_start(c, q):
        for k in range(2):
            gu_copy(c, q, k).start()

    def hidden_fwd(c):
        r = pl.ds(c * rows, rows)
        stage4(AR_OUT, c)
        h = add_bf(x_ref[r, :], full_ref[SLOT[AR_OUT], r, :])
        h_ref[r, :] = h
        h32 = h.astype(F32)
        stat_put(1 + c, jnp.sum(h32 * h32, axis=-1, keepdims=True), rows)

    def gate_up(c, at_once):
        r = pl.ds(c * rows, rows)
        inv2 = lax.rsqrt(stat_get(1 + c, rows) / full_width + EPSILON)
        inv2_ref[r, :] = inv2
        r2_ref[r, :] = (h_ref[r, :].astype(F32) * inv2 * g2_ref[...]).astype(BF)

        def gu_body(q, carry):
            for k, w_ref in ((0, wg_ref), (1, wu_ref)):
                dst = pl.ds(pl.multiple_of(k * ff + q * gu_cols, gu_cols), gu_cols)
                gu_send[r, dst] = dot_nn(r2_ref[r, :], w_ref[:, step(q, gu_cols)]).astype(BF)

            @pl.when(q < at_once)
            def _():
                gu_start(c, q)
            return carry

        lax.fori_loop(0, GU_PIECES, gu_body, 0)

    stage2(AR_OUT, LATE)
    lax.fori_loop(part_two, raw_steps, raw_body, 0)
    p2_copy(AR_OUT, LATE).wait_send()
    stage2(AR_OUT, EARLY)
    stage3(AR_OUT, LATE)
    hidden_fwd(LATE)
    for k in range(6, 8):
        ga_copy(k).start()
    gate_up(LATE, 2)
    stage3(AR_OUT, EARLY)
    hidden_fwd(EARLY)
    gu_start(LATE, 2)
    gu_start(LATE, 3)
    gate_up(EARLY, 0)
    tile = 512
    stores.append(store(r2_ref, r2_hbm, 2))

    for k in range(8):
        ga_copy(k).wait_recv()
    for c in order:
        p1_copy(AR_OUT, c).wait_send()
        p3_copy(AR_OUT, c).wait_send()
    p2_copy(AR_OUT, EARLY).wait_send()

    def mlp_pieces(c, lo, hi):
        r = pl.ds(c * rows, rows)
        if lo == 0:
            cot_ref[...] = jnp.zeros_like(cot_ref)

        def piece(q, carry):
            if c == EARLY:
                @pl.when(q == GU_PIECES - 1)
                def _():
                    for k in range(2):
                        gu_copy(c, q, k).wait_send()
                    for i in range(2):
                        rot_copy(mine(i)).start()
            gu_copy(c, q, 0).wait_recv()
            gu_copy(c, q, 1).wait_recv()
            if c == LATE:
                @pl.when(q == 2)
                def _():
                    gu_start(EARLY, 0)
            for n in range(gu_cols // 256):
                cg = pl.ds(pl.multiple_of(q * gu_cols + n * 256, 256), 256)
                cu = pl.ds(pl.multiple_of(ff + q * gu_cols + n * 256, 256), 256)
                gate = add_bf(gu_send[r, cg], gu_recv[r, cg]).astype(F32)
                up = add_bf(gu_send[r, cu], gu_recv[r, cu]).astype(F32)
                ga = add_bf(ga_send[r, cg], ga_recv[r, cg]).astype(F32)
                sig = 1.0 / (1.0 + jnp.exp(-gate))
                silu = gate * sig
                act_ref[r, cg] = (silu * up).astype(BF)
                dgu_ref[r, cg] = (ga * up * (sig * (1.0 + gate * (1.0 - sig)))).astype(BF)
                dgu_ref[r, cu] = (ga * silu).astype(BF)
            at_g = step(q, gu_cols)
            at_u = pl.ds(pl.multiple_of(ff + q * gu_cols, gu_cols), gu_cols)
            for n in range(width // tile):
                w = slice(n * tile, (n + 1) * tile)
                cot_ref[:, w] += dot_nt(dgu_ref[r, at_g], wg_ref[w, at_g]) + dot_nt(dgu_ref[r, at_u], wu_ref[w, at_g])
            return carry

        lax.fori_loop(lo, hi, piece, 0)

    def mlp_end(c):
        r = pl.ds(c * rows, rows)
        part_ref[SLOT[AR_R2], r, :] = cot_ref[...].astype(BF)
        p1_copy(AR_R2, c).start()
        unit = h_ref[r, :].astype(F32) * inv2_ref[r, :]
        dots_put(c, jnp.sum(cot_ref[...] * g2_ref[...] * unit, axis=-1, keepdims=True))

    def down_chunk(c):
        r = pl.ds(c * rows, rows)

        def down_body(n, carry):
            w = step(n, tile)
            part_ref[SLOT[AR_Y], r, w] = dot_nn(act_ref[r, :], wdown_ref[:, w]).astype(BF)
            return carry

        lax.fori_loop(0, width // tile, down_body, 0)
        p1_copy(AR_Y, c).start()

    dg1_ref[...] = jnp.zeros_like(dg1_ref)
    dg2_ref[...] = jnp.zeros_like(dg2_ref)

    def hidden_back(c, then=lambda: None):
        r = pl.ds(c * rows, rows)
        dots = dots_get(c)
        stage4(AR_R2, c)
        inv2 = inv2_ref[r, :]
        unit = h_ref[r, :].astype(F32) * inv2
        gin = full_ref[SLOT[AR_R2], r, :].astype(F32)
        norm = inv2 * (gin * g2_ref[...] - unit * (dots / full_width))
        dh_ref[r, :] = (dy_ref[r, :].astype(F32) + norm).astype(BF)
        gm_send[:, c * rows:(c + 1) * rows] = dot_nt(wout_ref[...], dh_ref[r, :]).astype(BF)
        for hf in range(2):
            gm_copy(c, hf).start()
        then()
        dg2_ref[...] += jnp.sum(gin * unit, axis=0, keepdims=True)

    def y_chunk(c):
        r = pl.ds(c * rows, rows)
        stage4(AR_Y, c)
        h_ref[r, :] = add_bf(h_ref[r, :], full_ref[SLOT[AR_Y], r, :])

    def scores_back(v, da, prob):
        dp = dot_tn(v, da).astype(BF).astype(F32)
        weighted = prob * dp
        return ((weighted - prob * jnp.sum(weighted, axis=0, keepdims=True)) * scale).astype(BF)

    def write(stored):
        for ref, at, value in stored:
            ref[at] = value

    def late_heads(js):
        stored = []
        cos_t, sin_t = cos_ref[:, rows:], sin_ref[:, rows:]
        late, early = slice(rows, None), slice(0, rows)
        for j in js:
            r_q, r_k, r_v = head_rows(j)
            r_a = mix_rows(j)
            da = add_bf(gm_send[r_a, late], gm_recv[r_a, late])
            prob = late_ref[j]
            k = rot_ref[r_k, :]
            ds = scores_back(rot_ref[r_v, :], da, prob)
            dv = dot_nt(da, prob.astype(BF))
            dk = dot_nt(rot_ref[r_q, late], ds)
            stored += [(dqkv_ref, (r_q, late), unrope(dot_nn(k, ds).astype(BF), cos_t, sin_t)),
                       (dqkv_ref, (r_k, late), unrope(dk[:, late].astype(BF), cos_t, sin_t)),
                       (dqkv_ref, (r_v, late), dv[:, late].astype(BF)),
                       (kv_part, (0, r_a), dk[:, early]), (kv_part, (1, r_a), dv[:, early])]
        write(stored)

    def late_mine(i, carry):
        late_heads((mine(2 * i), mine(2 * i + 1)))
        return carry

    def late_theirs(i, carry):
        j = theirs(i)
        rot_copy(j).wait_recv()
        r_q, r_k, _ = head_rows(j)
        probabilities(j, rot_ref[r_q, :], rot_ref[r_k, :])
        late_heads((j,))
        return carry

    def early_body(i, carry):
        stored = []
        early = slice(0, rows)
        cos_t, sin_t = cos_ref[:, early], sin_ref[:, early]
        for j in (2 * i, 2 * i + 1):
            r_q, r_k, r_v = head_rows(j)
            r_a = mix_rows(j)
            da = add_bf(gm_send[r_a, early], gm_recv[r_a, early])
            prob = early_ref[j]
            ds = scores_back(rot_ref[r_v, early], da, prob)
            dv = kv_part[1, r_a, :] + dot_nt(da, prob.astype(BF))
            dk = kv_part[0, r_a, :] + dot_nt(rot_ref[r_q, early], ds)
            stored += [(dqkv_ref, (r_q, early), unrope(dot_nn(rot_ref[r_k, early], ds).astype(BF), cos_t, sin_t)),
                       (dqkv_ref, (r_k, early), unrope(dk.astype(BF), cos_t, sin_t)),
                       (dqkv_ref, (r_v, early), dv.astype(BF))]
        write(stored)
        return carry

    half_chans = half_heads * GROUP

    def cot_product(c, lo, hi):
        return dot_tn(dqkv_ref[lo:hi, c * rows:(c + 1) * rows], wqkv_ref[lo:hi, :])

    def input_cot(c):
        r = pl.ds(c * rows, rows)
        cot = cot_product(c, half_chans, None) + (cot_ref[...] if c == EARLY else cot_product(c, 0, half_chans))
        part_ref[SLOT[AR_R1], r, :] = cot.astype(BF)
        p1_copy(AR_R1, c).start()
        unit = x_ref[r, :].astype(F32) * inv1_ref[r, :]
        dots_put(CHUNKS + c, jnp.sum(cot * g1_ref[...] * unit, axis=-1, keepdims=True))

    def input_back(c):
        r = pl.ds(c * rows, rows)
        dots = dots_get(CHUNKS + c)
        stage4(AR_R1, c)
        inv1 = inv1_ref[r, :]
        unit = x_ref[r, :].astype(F32) * inv1
        gin = full_ref[SLOT[AR_R1], r, :].astype(F32)
        norm = inv1 * (gin * g1_ref[...] - unit * (dots / full_width))
        dx_ref[r, :] = (dh_ref[r, :].astype(F32) + norm).astype(BF)
        stores.append(store(dx_ref.at[r], dx_hbm.at[r], 8 + c))
        dg1_ref[...] += jnp.sum(gin * unit, axis=0, keepdims=True)

    def rest_of_gate_up():
        gu_start(EARLY, 2)
        gu_start(EARLY, 3)

    mlp_pieces(LATE, 0, GU_PIECES)
    mlp_end(LATE)
    gu_start(EARLY, 1)
    stage2(AR_R2, LATE)
    down_chunk(LATE)
    stage3(AR_R2, LATE)
    stage2(AR_Y, LATE)
    hidden_back(LATE, rest_of_gate_up)
    mlp_pieces(EARLY, 0, 2)
    stage3(AR_Y, LATE)
    gm_copy(LATE, emb).wait_recv()
    lax.fori_loop(0, half_heads // 2, late_mine, 0)
    y_chunk(LATE)
    mlp_pieces(EARLY, 2, GU_PIECES)
    mlp_end(EARLY)
    for i in range(2, half_heads):
        rot_copy(mine(i)).start()
    stores.append(store(dgu_ref, dgu_hbm, 3))
    stores.append(store(act_ref, act_hbm, 4))
    stage2(AR_R2, EARLY)
    down_chunk(EARLY)
    gm_copy(LATE, 1 - emb).wait_recv()
    lax.fori_loop(0, 2, late_theirs, 0)
    stage3(AR_R2, EARLY)
    hidden_back(EARLY)
    stores.append(store(dh_ref, dh_hbm, 5))
    stores.append(store(dg2_ref, dg2_hbm, 6))
    stage2(AR_Y, EARLY)
    lax.fori_loop(2, half_heads, late_theirs, 0)
    input_cot(LATE)
    gm_copy(EARLY, 0).wait_recv()
    stage2(AR_R1, LATE)
    lax.fori_loop(0, half_heads // 2, early_body, 0)
    cot_ref[...] = cot_product(EARLY, 0, half_chans)
    gm_copy(EARLY, 1).wait_recv()
    lax.fori_loop(half_heads // 2, half_heads, early_body, 0)
    input_cot(EARLY)
    stores.append(store(dqkv_ref, dqkv_hbm, 7))
    stage2(AR_R1, EARLY)
    stage3(AR_R1, LATE)
    stage3(AR_Y, EARLY)
    input_back(LATE)
    y_chunk(EARLY)
    stores.append(store(h_ref, y_hbm, 10))
    stage3(AR_R1, EARLY)
    input_back(EARLY)
    stores.append(store(dg1_ref, dg1_hbm, 11))

    for k in range(3):
        stat_copy(k).wait_send()
    for k in range(2 * CHUNKS):
        for n in range(7):
            dots_copy(k, n).wait_send()
    for k in range(8):
        ga_copy(k).wait_send()
    for i in range(half_heads):
        if i < last:
            qkv_copy(theirs(i)).wait_send()
        mix_copy(mine(i)).wait_send()
        rot_copy(mine(i)).wait_send()
    for c in range(CHUNKS):
        for q in range(GU_PIECES - (c == EARLY)):
            for k in range(2):
                gu_copy(c, q, k).wait_send()
        for hf in range(2):
            gm_copy(c, hf).wait_send()
        for i in range(1, 4):
            p1_copy(i, c).wait_send()
            p2_copy(i, c).wait_send()
            p3_copy(i, c).wait_send()
    for copy in stores:
        copy.wait()


def run_layer(x_in, positions, gain_one, gain_two, w_qkv, w_out, w_gu, w_down, grad_out):
    tokens, width = x_in.shape
    ff = w_down.shape[0]
    chans = w_qkv.shape[0]
    mix = w_out.shape[0]
    heads = mix // HEAD
    rows = tokens // CHUNKS
    act = lambda n, dtype=BF: jax.ShapeDtypeStruct((tokens, n), dtype)
    any_spec = pl.BlockSpec(memory_space=pl.ANY)
    vmem_spec = pl.BlockSpec(memory_space=pltpu.VMEM)
    raw_rows = 128 * 32
    scratch = [
        pltpu.VMEM((tokens, width), BF), pltpu.VMEM((tokens, width), BF),
        pltpu.VMEM((chans, width), BF), pltpu.VMEM((mix, width), BF),
        pltpu.VMEM((width, ff), BF), pltpu.VMEM((width, ff), BF), pltpu.VMEM((ff, width), BF),
        pltpu.VMEM((2, raw_rows, 128), BF),
        pltpu.VMEM((1, width), F32), pltpu.VMEM((1, width), F32), pltpu.VMEM((HALF, tokens), F32), pltpu.VMEM((HALF, tokens), F32),
        pltpu.VMEM((tokens, width), BF), pltpu.VMEM((tokens, width), BF), pltpu.VMEM((tokens, width), BF), pltpu.VMEM((tokens, width), BF),
        pltpu.VMEM((tokens, ff), BF), pltpu.VMEM((tokens, 2 * ff), BF),
        pltpu.VMEM((chans, tokens), BF), pltpu.VMEM((heads, tokens, rows), F32), pltpu.VMEM((heads, rows, rows), F32), pltpu.VMEM((mix, tokens), BF), pltpu.VMEM((chans, tokens), BF),
        pltpu.VMEM((tokens, width), BF),
        pltpu.VMEM((2, mix, rows), F32), pltpu.VMEM((rows, width), F32), pltpu.VMEM((2 * CHUNKS, 8, 8, rows), F32), pltpu.VMEM((1, width), F32), pltpu.VMEM((1, width), F32),
        pltpu.VMEM((tokens, 1), F32), pltpu.VMEM((tokens, 1), F32),
        pltpu.VMEM((tokens, ff), BF), pltpu.VMEM((tokens, ff), BF),
        pltpu.VMEM((chans, tokens), BF), pltpu.VMEM((chans, tokens), BF),
        pltpu.VMEM((tokens, 2 * ff), BF), pltpu.VMEM((tokens, 2 * ff), BF),
        pltpu.VMEM((mix, tokens), BF), pltpu.VMEM((mix, tokens), BF),
        pltpu.VMEM((3, 8, tokens), F32), pltpu.VMEM((3, 8, tokens), F32),
        pltpu.VMEM((3, tokens, width), BF), pltpu.VMEM((3, tokens, width // 2), BF), pltpu.VMEM((3, tokens, width // 2), BF),
        pltpu.VMEM((3, tokens, width // 2), BF), pltpu.VMEM((3, tokens, width), BF),
        pltpu.SemaphoreType.DMA((5,)), pltpu.SemaphoreType.DMA((2,)), pltpu.SemaphoreType.DMA((10 + CHUNKS,)),
    ]
    for n in (3, 8, heads, 2 * GU_PIECES * CHUNKS, 2 * CHUNKS, 4 * CHUNKS, 4 * CHUNKS, 4 * CHUNKS):
        scratch += [pltpu.SemaphoreType.DMA((n,)), pltpu.SemaphoreType.DMA((n,))]
    for n in (7 * 2 * CHUNKS, 8 * 2 * CHUNKS, heads, heads, heads, heads):
        scratch += [pltpu.SemaphoreType.DMA((n,))]
    vec = jax.ShapeDtypeStruct((1, width), F32)
    return pl.pallas_call(
        layer_kernel,
        name="layer",
        out_shape=(act(width), act(width), vec, vec, act(width), jax.ShapeDtypeStruct((chans, tokens), BF),
                   jax.ShapeDtypeStruct((mix, tokens), BF), act(width), act(width), act(2 * ff), act(ff)),
        in_specs=[any_spec, any_spec, vmem_spec, vmem_spec, vmem_spec, any_spec, any_spec, any_spec, any_spec],
        out_specs=(any_spec,) * 11,
        scratch_shapes=scratch,
        compiler_params=pltpu.CompilerParams(collective_id=0, has_side_effects=True, vmem_limit_bytes=67000000),
    )(x_in, grad_out, gain_one, gain_two, positions, w_qkv, w_out, w_gu, w_down)


def grads_kernel(act_hbm, dy_hbm, r2_hbm, dgu_hbm, mix_hbm, dh_hbm, dqkv_hbm, r1_hbm, y_in, dx_in, dg1_in, dg2_in,
                 down_out, gu_out, wout_out, qkv_out, y_out, dx_out, dg1_out, dg2_out,
                 act_ref, dy_ref, r2_ref, dgu_ref, mix_ref, dh_ref, dqkv_ref, r1_ref, y_ref, dx_ref, rows_ref, inter_ref,
                 load_sem, rows_sem, inter_sem, end_sem):
    block = rows_ref.shape[1]
    pad = inter_ref.shape[1] // GU_BLOCK
    ff = dgu_ref.shape[1] // 2
    pairs = [(dqkv_hbm, dqkv_ref), (r1_hbm, r1_ref), (r2_hbm, r2_ref), (dgu_hbm, dgu_ref), (mix_hbm, mix_ref), (dh_hbm, dh_ref),
             (act_hbm, act_ref), (dy_hbm, dy_ref), (y_in, y_ref), (dx_in, dx_ref)]
    loads = [pltpu.make_async_copy(src, dst, load_sem.at[n]) for n, (src, dst) in enumerate(pairs)]
    for copy in loads[:2]:
        copy.start()
    dg1_out[...] = dg1_in[...].reshape(dg1_out.shape)
    dg2_out[...] = dg2_in[...].reshape(dg2_out.shape)

    slots = rows_ref.shape[0]

    def rows_copy(out, index, slot):
        return pltpu.make_async_copy(rows_ref.at[slot], out.at[step(index, block)], rows_sem.at[slot])

    def product(out, lhs_of, rhs_ref, first):
        def body(i, carry):
            slot = lax.rem(i + first, slots)

            @pl.when(i + first >= slots)
            def _():
                rows_copy(out, 0, slot).wait()
            rows_ref[slot] = lhs_of(i, rhs_ref)
            rows_copy(out, i, slot).start()
            return carry
        count = out.shape[0] // block
        lax.fori_loop(0, count, body, 0)
        return first + count

    def plain_rows(ref):
        return lambda i, rhs_ref: dot_nn(ref[step(i, block), :], rhs_ref[...])

    loads[0].wait()
    loads[1].wait()
    for copy in loads[2:]:
        copy.start()
    sent = product(qkv_out, plain_rows(dqkv_ref), r1_ref, 0)

    loads[2].wait()
    loads[3].wait()

    def inter_copy(index, slot):
        return pltpu.make_async_copy(inter_ref.at[slot].reshape(GU_BLOCK, pad, 128).at[:, 0:32, :],
                                     gu_out.at[step(index, GU_BLOCK)], inter_sem.at[slot])

    gu_steps = gu_out.shape[0] // GU_BLOCK

    def gu_body(i, carry):
        slot = lax.rem(i, slots)

        @pl.when(i >= slots)
        def _():
            inter_copy(0, slot).wait()
        lhs = r2_ref[:, step(i, GU_BLOCK)].T
        for k in range(2):
            for n in range(ff // 512):
                val = dot_nn(lhs, dgu_ref[:, k * ff + n * 512:k * ff + (n + 1) * 512])
                for t in range(4):
                    row = 2 * (4 * n + t) + k
                    inter_ref[slot, pl.ds(row, GU_BLOCK, stride=pad), :] = val[:, t * 128:(t + 1) * 128]
        inter_copy(i, slot).start()
        return carry

    lax.fori_loop(0, gu_steps, gu_body, 0)

    loads[4].wait()
    loads[5].wait()
    sent = product(wout_out, plain_rows(mix_ref), dh_ref, sent)
    loads[6].wait()
    loads[7].wait()
    sent = product(down_out, lambda i, rhs_ref: dot_tn(act_ref[:, step(i, block)], rhs_ref[...]), dy_ref, sent)
    loads[8].wait()
    loads[9].wait()
    ends = [pltpu.make_async_copy(y_ref, y_out, end_sem.at[0]), pltpu.make_async_copy(dx_ref, dx_out, end_sem.at[1])]
    for copy in ends:
        copy.start()
    for slot in range(slots):
        rows_copy(down_out, 0, slot).wait()
        inter_copy(0, slot).wait()
    for copy in ends:
        copy.wait()


GU_BLOCK = 128


def weight_grads(act, grad_out, r2, dgu, mix, dh, dqkv, r1, y, dx, dg1, dg2):
    tokens, width = r2.shape
    ff = act.shape[1]
    any_spec = pl.BlockSpec(memory_space=pl.ANY)
    vmem_spec = pl.BlockSpec(memory_space=pltpu.VMEM)
    out = lambda *shape: jax.ShapeDtypeStruct(shape, F32)
    like = lambda a: jax.ShapeDtypeStruct(a.shape, a.dtype)
    arrays = (act, grad_out, r2, dgu, mix, dh, dqkv, r1, y, dx)
    return pl.pallas_call(
        grads_kernel,
        name="weight_grads",
        in_specs=[any_spec] * 10 + [vmem_spec] * 2,
        out_specs=[any_spec] * 6 + [vmem_spec] * 2,
        out_shape=[out(ff, width), out(width, 32, 128), out(mix.shape[0], width), out(dqkv.shape[0], width), like(y), like(dx), out(width), out(width)],
        scratch_shapes=[pltpu.VMEM(a.shape, a.dtype) for a in arrays] + [
            pltpu.VMEM((4, 256, width), F32), pltpu.VMEM((4, GU_BLOCK * 40, 128), F32),
            pltpu.SemaphoreType.DMA((10,)), pltpu.SemaphoreType.DMA((4,)), pltpu.SemaphoreType.DMA((4,)), pltpu.SemaphoreType.DMA((2,))],
        compiler_params=pltpu.CompilerParams(vmem_limit_bytes=56 << 20),
    )(*arrays, dg1, dg2)


def solution(mesh):
    def per_device(x_in, positions, gain_one, gain_two, w_qkv, w_out, w_gu, w_down, grad_out):
        width, groups, chans = w_qkv.shape
        ff = w_down.shape[0]
        qkv_rows = w_qkv.transpose(1, 2, 0).reshape(groups * chans, width)
        gu_rows = w_gu.reshape(width, 2, ff // 128, 128).transpose(0, 2, 1, 3).reshape(width * 2 * (ff // 128), 128)
        y, dx, dg1, dg2, r1, dqkv, mix, dh, r2, dgu, act = run_layer(
            x_in, positions, gain_one, gain_two, qkv_rows, w_out, gu_rows, w_down, grad_out)
        d_down, d_gu, d_out, d_qkv, y, dx, dg1, dg2 = weight_grads(act, grad_out, r2, dgu, mix, dh, dqkv, r1, y, dx, dg1, dg2)
        d_gu = d_gu.reshape(width, ff // 128, 2, 128).transpose(0, 2, 1, 3).reshape(width, 2, ff)
        d_qkv = d_qkv.reshape(groups, chans, width).transpose(2, 0, 1)
        return y, dx, dg1, dg2, d_qkv, d_out, d_gu, d_down

    act_spec = P('dp', 'embed')
    in_specs = (act_spec, P('dp'), P('embed'), P('embed'), P('embed', 'heads', None), P('heads', 'embed'), P('embed', None, 'heads'), P('heads', 'embed'), act_spec)
    out_specs = (act_spec, act_spec, P(('dp', 'embed')), P(('dp', 'embed')), P(('dp', 'embed'), 'heads', None), P(('dp', 'heads'), 'embed'), P(('dp', 'embed'), None, 'heads'), P(('dp', 'heads'), 'embed'))
    return jax.shard_map(per_device, mesh=mesh, in_specs=in_specs, out_specs=out_specs, check_vma=False)
```

```python
import math

import jax
import jax.numpy as jnp
from jax import lax
from jax.experimental import pallas as pl
from jax.experimental.pallas import tpu as pltpu
from jax.sharding import PartitionSpec as P

EPSILON = 1e-5
ROPE_BASE = 10000.0
HEAD = 96
HALF = HEAD // 2
GROUP = 3 * HEAD
CHUNKS = 2
MESH = pl.DeviceIdType.MESH
BF = jnp.bfloat16
F32 = jnp.float32

AR_OUT, AR_R2, AR_Y, AR_R1 = range(4)
SLOT = (0, 1, 2, 0)
GU_PIECES = 4
EARLY, LATE = 0, 1


def dot_nn(lhs, rhs):
    return lax.dot_general(lhs, rhs, (((1,), (0,)), ((), ())), preferred_element_type=F32)


def dot_nt(lhs, rhs):
    return lax.dot_general(lhs, rhs, (((1,), (1,)), ((), ())), preferred_element_type=F32)


def dot_tn(lhs, rhs):
    return lax.dot_general(lhs, rhs, (((0,), (0,)), ((), ())), preferred_element_type=F32)


def add_bf(one, two):
    return (one.astype(F32) + two.astype(F32)).astype(BF)


def step(index, size):
    return pl.ds(pl.multiple_of(index * size, size), size)


def layer_kernel(x_hbm, dy_hbm, g1_in, g2_in, pos_in, wqkv_hbm, wout_hbm, wgu_hbm, wdown_hbm,
                 y_hbm, dx_hbm, dg1_hbm, dg2_hbm, r1_hbm, dqkv_hbm, mix_hbm, dh_hbm, r2_hbm, dgu_hbm, act_hbm,
                 x_ref, dy_ref, wqkv_ref, wout_ref, wg_ref, wu_ref, wdown_ref, raw_ref,
                 g1_ref, g2_ref, cos_ref, sin_ref, r1_ref, r2_ref, h_ref, dh_ref, act_ref, dgu_ref, rot_ref, late_ref, early_ref, mix_ref, dqkv_ref, dx_ref,
                 kv_part, cot_ref, dots_ref, dg1_ref, dg2_ref,
                 inv1_ref, inv2_ref,
                 ga_send, ga_recv, qkv_send, qkv_recv, gu_send, gu_recv, gm_send, gm_recv, stat_send, stat_recv,
                 part_ref, sib_ref, half_ref, far_ref, full_ref,
                 load_sem, raw_sem, store_sem,
                 st_s, st_r, ga_s, ga_r, qk_s, qk_r, gu_s, gu_r, gm_s, gm_r, p1_s, p1_r, p2_s, p2_r, p3_s, p3_r, dots_s, dots_r, mx_s, mx_r, rt_s, rt_r):
    tokens, width = x_ref.shape
    full_width = 2 * width
    ff = wdown_ref.shape[0]
    heads = wqkv_ref.shape[0] // GROUP
    half_width = width // 2
    rows = tokens // CHUNKS
    emb = lax.axis_index("embed")
    hid = lax.axis_index("heads")
    core = lax.rem(hid, 2)
    sibling = {"heads": hid + 1 - 2 * core}
    across = {"heads": lax.rem(hid + 2, 4)}
    partner = {"embed": 1 - emb}

    barrier = pltpu.get_barrier_semaphore()
    others = [{"embed": lax.rem(emb + n // 4, 2), "heads": lax.rem(hid + n, 4)} for n in range(1, 8)]
    for peer in others:
        pl.semaphore_signal(barrier, inc=1, device_id=peer, device_id_type=MESH)

    def load(src, dst, sem):
        return pltpu.make_async_copy(src, dst, load_sem.at[sem])

    loads = [load(x_hbm, x_ref, 0), load(dy_hbm, dy_ref, 1), load(wdown_hbm, wdown_ref, 2),
             load(wqkv_hbm, wqkv_ref, 3), load(wout_hbm, wout_ref, 4)]
    for copy in loads[:3]:
        copy.start()

    raw_rows = raw_ref.shape[1]
    raw_steps = wgu_hbm.shape[0] // raw_rows

    def raw_load(index, slot):
        return pltpu.make_async_copy(wgu_hbm.at[step(index, raw_rows)], raw_ref.at[slot], raw_sem.at[slot])

    def store(src, dst, sem):
        copy = pltpu.make_async_copy(src, dst, store_sem.at[sem])
        copy.start()
        return copy

    def send(src, dst, s_sem, r_sem, peer):
        return pltpu.make_async_remote_copy(src_ref=src, dst_ref=dst, send_sem=s_sem, recv_sem=r_sem,
                                            device_id=peer, device_id_type=MESH)

    def stat_copy(k):
        return send(stat_send.at[k], stat_recv.at[k], st_s.at[k], st_r.at[k], partner)

    ga_cols = ff // 8

    def ga_copy(k):
        cols = step(k, ga_cols)
        return send(ga_send.at[:, cols], ga_recv.at[:, cols], ga_s.at[0], ga_r.at[0], partner)

    ga_all = send(ga_send, ga_recv, ga_s.at[0], ga_r.at[0], partner)

    def qkv_copy(i, j):
        r = step(j, GROUP)
        return send(qkv_send.at[r], qkv_recv.at[r], qk_s.at[0], qk_r.at[i], partner)

    half_heads = heads // 2
    half_chans = half_heads * GROUP

    def mine(i):
        return emb * half_heads + i

    def theirs(i):
        return (1 - emb) * half_heads + i

    def mix_rows(j):
        return pl.ds(pl.multiple_of(j * HEAD, 32), HEAD)

    def mix_copy(j):
        at = mix_ref.at[mix_rows(j)]
        return send(at, at, mx_s.at[0], mx_r.at[0], partner)

    def mix_all(which):
        at = mix_ref.at[step(which, half_heads * HEAD)]
        return send(at, at, mx_s.at[0], mx_r.at[0], partner)

    def rot_copy(i, j):
        at = rot_ref.at[step(j, GROUP)]
        return send(at, at, rt_s.at[0], rt_r.at[i], partner)

    gu_cols = ff // GU_PIECES

    def gu_copy(c, q, k):
        at = (pl.ds(c * rows, rows), pl.ds(pl.multiple_of(k * ff + q * gu_cols, gu_cols), gu_cols))
        return send(gu_send.at[at], gu_recv.at[at], gu_s.at[c], gu_r.at[c * GU_PIECES + q], partner)

    def gu_pair(c, q):
        at = (pl.ds(c * rows, rows), pl.ds(0, 2 * gu_cols))
        return send(gu_send.at[at], gu_recv.at[at], gu_s.at[c], gu_r.at[c * GU_PIECES + q], partner)

    def gu_sent(c):
        at = pl.ds(c * rows, rows)
        send(gu_send.at[at], gu_recv.at[at], gu_s.at[c], gu_r.at[0], partner).wait_send()

    gm_rows = gm_send.shape[0] // 2

    def gm_copy(c, hf):
        at = (step(hf, gm_rows), pl.ds(c * rows, rows))
        return send(gm_send.at[at], gm_recv.at[at], gm_s.at[c], gm_r.at[2 * c + hf], partner)

    own = pl.ds(pl.multiple_of(core * half_width, half_width), half_width)
    other = pl.ds(pl.multiple_of((1 - core) * half_width, half_width), half_width)

    def p1_copy(i, c):
        r = pl.ds(c * rows, rows)
        k = i * CHUNKS + c
        return send(part_ref.at[SLOT[i], r, other], sib_ref.at[SLOT[i], r], p1_s.at[i], p1_r.at[k], sibling)

    def p2_copy(i, c):
        r = pl.ds(c * rows, rows)
        k = i * CHUNKS + c
        return send(half_ref.at[SLOT[i], r], far_ref.at[SLOT[i], r], p2_s.at[k], p2_r.at[k], across)

    def p3_copy(i, c):
        r = pl.ds(c * rows, rows)
        k = i * CHUNKS + c
        return send(full_ref.at[SLOT[i], r, own], full_ref.at[SLOT[i], r, own], p3_s.at[i], p3_r.at[k], sibling)

    def p1_p3_sent(i):
        n = SLOT[i]
        send(part_ref.at[n, :, other], sib_ref.at[n], p1_s.at[i], p1_r.at[0], sibling).wait_send()
        send(full_ref.at[n, :, own], full_ref.at[n, :, own], p3_s.at[i], p3_r.at[0], sibling).wait_send()

    def stage2(i, c):
        r = pl.ds(c * rows, rows)
        p1_copy(i, c).wait_recv()
        half_ref[SLOT[i], r, :] = add_bf(part_ref[SLOT[i], r, own], sib_ref[SLOT[i], r, :])
        p2_copy(i, c).start()

    def stage3(i, c):
        r = pl.ds(c * rows, rows)
        p2_copy(i, c).wait_recv()
        full_ref[SLOT[i], r, own] = add_bf(half_ref[SLOT[i], r, :], far_ref[SLOT[i], r, :])
        p3_copy(i, c).start()

    def stage4(i, c):
        p3_copy(i, c).wait_recv()

    def stat_put(k, col, n):
        flat = jnp.broadcast_to(col, (n, 128)).T[0:8, :]
        stat_send[k, :, 0:n] = flat
        stat_copy(k).start()

    def stat_get(k, n):
        stat_copy(k).wait_recv()
        total = stat_send[k, 0:1, 0:n] + stat_recv[k, 0:1, 0:n]
        return jnp.broadcast_to(total, (128, n)).T[:, 0:1]

    me = emb * 4 + hid

    def dots_copy(k, n):
        at = dots_ref.at[k, me]
        return send(at, at, dots_s.at[k], dots_r.at[k], others[n])

    def dots_all(k):
        at = dots_ref.at[k, pl.ds(0, 7)]
        return send(at, at, dots_s.at[k], dots_r.at[k], partner)

    def dots_put(k, col):
        dots_ref[k, me] = jnp.broadcast_to(col, (rows, 128)).T[0:8, :]
        for n in range(7):
            dots_copy(k, n).start()

    def dots_get(k):
        dots_all(k).wait_recv()
        total = dots_ref[k, 0, 0:1, :]
        for n in range(1, 8):
            total = total + dots_ref[k, n, 0:1, :]
        return jnp.broadcast_to(total, (128, rows)).T[:, 0:1]

    place = pos_in[...].reshape(1, tokens).astype(F32)
    pair_i = lax.broadcasted_iota(jnp.int32, (HALF, 1), 0).astype(F32)
    angles = jnp.exp(pair_i * (-2.0 * math.log(ROPE_BASE) / HEAD)) * place
    cos_ref[...] = jnp.cos(angles)
    sin_ref[...] = jnp.sin(angles)
    g1_ref[...] = g1_in[...].reshape(1, width)
    g2_ref[...] = g2_in[...].reshape(1, width)
    loads[0].wait()
    x32 = x_ref[...].astype(F32)
    sq1 = jnp.sum(x32 * x32, axis=-1, keepdims=True)
    for copy in loads[3:]:
        copy.start()
    for slot in range(2):
        raw_load(slot, slot).start()

    def ga_body(k, carry):
        cols = step(k, ga_cols)
        ga_send[:, cols] = dot_nt(dy_ref[...], wdown_ref[cols, :]).astype(BF)
        return carry

    loads[1].wait()
    loads[2].wait()
    lax.fori_loop(0, 4, ga_body, 0)
    pl.semaphore_wait(barrier, 7)
    stat_put(0, sq1, tokens)
    ga_copy(0).start()
    lax.fori_loop(4, 8, ga_body, 0)
    inv1 = lax.rsqrt(stat_get(0, tokens) / full_width + EPSILON)
    inv1_ref[...] = inv1
    r1_ref[...] = (x_ref[...].astype(F32) * inv1 * g1_ref[...]).astype(BF)
    stores = [store(r1_ref, r1_hbm, 0)]

    loads[3].wait()

    def qkv_product(j):
        r = step(j, GROUP)
        qkv_send[r, :] = dot_nt(wqkv_ref[r, :], r1_ref[...]).astype(BF)

    def qkv_theirs(i, carry):
        qkv_product(theirs(i))
        qkv_copy(i, theirs(i)).start()
        return carry

    def qkv_mine(i, carry):
        qkv_product(mine(i))
        return carry

    lax.fori_loop(0, half_heads, qkv_theirs, 0)
    lax.fori_loop(0, half_heads, qkv_mine, 0)

    row_i = lax.broadcasted_iota(jnp.int32, (256, 256), 0)
    col_i = lax.broadcasted_iota(jnp.int32, (256, 256), 1)
    perm = (col_i == (row_i % 8) * 32 + row_i // 8).astype(F32).astype(BF)
    blocks = raw_rows // 512

    def raw_body(i, carry):
        slot = lax.rem(i, 2)
        raw_load(i, slot).wait()

        def block_body(b, inner):
            for u in range(4):
                base = pl.multiple_of(b * 2048 + u * 512, 512)
                pair = jnp.concatenate([raw_ref[slot, pl.ds(base, 256), :], raw_ref[slot, pl.ds(base + 256, 256), :]], axis=1)
                out = dot_nn(perm, pair)
                d = pl.ds(pl.multiple_of(i * (raw_rows // 32) + b * 64 + u * 16, 16), 16)
                for t in range(16):
                    for k, dst in ((0, wg_ref), (1, wu_ref)):
                        r = (2 * t + k) * 8
                        both = jnp.concatenate([out[r:r + 8, 0:128], out[r:r + 8, 128:256]], axis=0)
                        dst[d, t * 128:(t + 1) * 128] = both.astype(BF)
            return inner

        lax.fori_loop(0, blocks // 4, block_body, 0)

        @pl.when(i + 2 < raw_steps)
        def _():
            raw_load(i + 2, slot).start()
        return carry

    part_one, part_two = raw_steps // 2, raw_steps - raw_steps // 3
    lax.fori_loop(0, part_one, raw_body, 0)

    scale = HEAD ** -0.5
    causal = (lax.broadcasted_iota(jnp.int32, (tokens, tokens), 0) <= lax.broadcasted_iota(jnp.int32, (tokens, tokens), 1))

    def rope(v, cos_t, sin_t):
        v = v.astype(F32)
        one, two = v[0:HALF], v[HALF:HEAD]
        return jnp.concatenate([one * cos_t - two * sin_t, two * cos_t + one * sin_t], axis=0).astype(BF)

    def unrope(v, cos_t, sin_t):
        v = v.astype(F32)
        one, two = v[0:HALF], v[HALF:HEAD]
        return jnp.concatenate([one * cos_t + two * sin_t, two * cos_t - one * sin_t], axis=0).astype(BF)

    last = half_heads - 1

    def head_rows(j):
        base = pl.multiple_of(j * GROUP, 32)
        return tuple(pl.ds(base + n * HEAD, HEAD) for n in range(3))

    def probabilities(j, q, k):
        scores = jnp.where(causal, dot_tn(k, q) * scale, -1e30)
        weight = jnp.exp(scores - jnp.max(scores, axis=0, keepdims=True))
        prob = weight / jnp.sum(weight, axis=0, keepdims=True)
        late_ref[j] = prob[:, rows:]
        early_ref[j] = prob[0:rows, 0:rows]
        return prob

    def attn_body(i, carry):
        j = mine(i)

        @pl.when(i == last)
        def _():
            r = step(1 - emb, half_chans)
            send(qkv_send.at[r], qkv_recv.at[r], qk_s.at[0], qk_r.at[0], partner).wait_send()
            ga_copy(1).start()
        qkv_copy(i, j).wait_recv()
        r_q, r_k, r_v = head_rows(j)
        cos_t, sin_t = cos_ref[...], sin_ref[...]
        q = rope(add_bf(qkv_send[r_q, :], qkv_recv[r_q, :]), cos_t, sin_t)
        k = rope(add_bf(qkv_send[r_k, :], qkv_recv[r_k, :]), cos_t, sin_t)
        v = add_bf(qkv_send[r_v, :], qkv_recv[r_v, :])
        rot_ref[r_q, :] = q
        rot_ref[r_k, :] = k
        rot_ref[r_v, :] = v
        prob = probabilities(j, q, k)
        mix_ref[mix_rows(j), :] = dot_nn(v, prob.astype(BF)).astype(BF)
        mix_copy(j).start()
        return carry

    lax.fori_loop(0, half_heads, attn_body, 0)
    for n in range(2, 6):
        ga_copy(n).start()
    lax.fori_loop(part_one, part_two, raw_body, 0)
    mix_all(1 - emb).wait_recv()
    stores.append(store(mix_ref, mix_hbm, 1))

    loads[4].wait()
    order = tuple(reversed(range(CHUNKS)))
    for c in order:
        r = pl.ds(c * rows, rows)
        part_ref[SLOT[AR_OUT], r, :] = dot_tn(mix_ref[:, c * rows:(c + 1) * rows], wout_ref[...]).astype(BF)
        p1_copy(AR_OUT, c).start()
    def gu_start(c, q):
        for k in range(2):
            gu_copy(c, q, k).start()

    def hidden_fwd(c):
        r = pl.ds(c * rows, rows)
        stage4(AR_OUT, c)
        h = add_bf(x_ref[r, :], full_ref[SLOT[AR_OUT], r, :])
        h_ref[r, :] = h
        h32 = h.astype(F32)
        stat_put(1 + c, jnp.sum(h32 * h32, axis=-1, keepdims=True), rows)

    def gate_up(c, at_once):
        r = pl.ds(c * rows, rows)
        inv2 = lax.rsqrt(stat_get(1 + c, rows) / full_width + EPSILON)
        inv2_ref[r, :] = inv2
        r2_ref[r, :] = (h_ref[r, :].astype(F32) * inv2 * g2_ref[...]).astype(BF)

        def gu_body(q, carry):
            for k, w_ref in ((0, wg_ref), (1, wu_ref)):
                dst = pl.ds(pl.multiple_of(k * ff + q * gu_cols, gu_cols), gu_cols)
                gu_send[r, dst] = dot_nn(r2_ref[r, :], w_ref[:, step(q, gu_cols)]).astype(BF)

            @pl.when(q < at_once)
            def _():
                gu_start(c, q)
            return carry

        lax.fori_loop(0, GU_PIECES, gu_body, 0)

    stage2(AR_OUT, LATE)
    lax.fori_loop(part_two, raw_steps, raw_body, 0)
    p2_copy(AR_OUT, LATE).wait_send()
    stage2(AR_OUT, EARLY)
    stage3(AR_OUT, LATE)
    hidden_fwd(LATE)
    for k in range(6, 8):
        ga_copy(k).start()
    gate_up(LATE, 2)
    stage3(AR_OUT, EARLY)
    hidden_fwd(EARLY)
    gu_start(LATE, 2)
    gu_start(LATE, 3)
    gate_up(EARLY, 0)
    tile = 512
    stores.append(store(r2_ref, r2_hbm, 2))

    ga_all.wait_recv()
    p1_p3_sent(AR_OUT)
    p2_copy(AR_OUT, EARLY).wait_send()

    def mlp_pieces(c, lo, hi):
        r = pl.ds(c * rows, rows)
        if lo == 0:
            cot_ref[...] = jnp.zeros_like(cot_ref)

        def piece(q, carry):
            if c == EARLY:
                @pl.when(q == GU_PIECES - 1)
                def _():
                    gu_sent(EARLY)
                    for i in range(2):
                        rot_copy(i, mine(i)).start()
            gu_pair(c, q).wait_recv()
            if c == LATE:
                @pl.when(q == 2)
                def _():
                    gu_start(EARLY, 0)
            for n in range(gu_cols // 256):
                cg = pl.ds(pl.multiple_of(q * gu_cols + n * 256, 256), 256)
                cu = pl.ds(pl.multiple_of(ff + q * gu_cols + n * 256, 256), 256)
                gate = add_bf(gu_send[r, cg], gu_recv[r, cg]).astype(F32)
                up = add_bf(gu_send[r, cu], gu_recv[r, cu]).astype(F32)
                ga = add_bf(ga_send[r, cg], ga_recv[r, cg]).astype(F32)
                sig = 1.0 / (1.0 + jnp.exp(-gate))
                silu = gate * sig
                act_ref[r, cg] = (silu * up).astype(BF)
                dgu_ref[r, cg] = (ga * up * (sig * (1.0 + gate * (1.0 - sig)))).astype(BF)
                dgu_ref[r, cu] = (ga * silu).astype(BF)
            at_g = step(q, gu_cols)
            at_u = pl.ds(pl.multiple_of(ff + q * gu_cols, gu_cols), gu_cols)
            for n in range(width // tile):
                w = slice(n * tile, (n + 1) * tile)
                cot_ref[:, w] += dot_nt(dgu_ref[r, at_g], wg_ref[w, at_g]) + dot_nt(dgu_ref[r, at_u], wu_ref[w, at_g])
            return carry

        lax.fori_loop(lo, hi, piece, 0)

    def mlp_end(c):
        r = pl.ds(c * rows, rows)
        part_ref[SLOT[AR_R2], r, :] = cot_ref[...].astype(BF)
        p1_copy(AR_R2, c).start()
        unit = h_ref[r, :].astype(F32) * inv2_ref[r, :]
        dots_put(c, jnp.sum(cot_ref[...] * g2_ref[...] * unit, axis=-1, keepdims=True))

    def down_chunk(c):
        r = pl.ds(c * rows, rows)

        def down_body(n, carry):
            w = step(n, tile)
            part_ref[SLOT[AR_Y], r, w] = dot_nn(act_ref[r, :], wdown_ref[:, w]).astype(BF)
            return carry

        lax.fori_loop(0, width // tile, down_body, 0)
        p1_copy(AR_Y, c).start()

    dg1_ref[...] = jnp.zeros_like(dg1_ref)
    dg2_ref[...] = jnp.zeros_like(dg2_ref)

    def hidden_back(c, then=lambda: None):
        r = pl.ds(c * rows, rows)
        dots = dots_get(c)
        stage4(AR_R2, c)
        inv2 = inv2_ref[r, :]
        unit = h_ref[r, :].astype(F32) * inv2
        gin = full_ref[SLOT[AR_R2], r, :].astype(F32)
        norm = inv2 * (gin * g2_ref[...] - unit * (dots / full_width))
        dh_ref[r, :] = (dy_ref[r, :].astype(F32) + norm).astype(BF)
        gm_send[:, c * rows:(c + 1) * rows] = dot_nt(wout_ref[...], dh_ref[r, :]).astype(BF)
        for hf in range(2):
            gm_copy(c, hf).start()
        then()
        dg2_ref[...] += jnp.sum(gin * unit, axis=0, keepdims=True)

    def y_chunk(c):
        r = pl.ds(c * rows, rows)
        stage4(AR_Y, c)
        h_ref[r, :] = add_bf(h_ref[r, :], full_ref[SLOT[AR_Y], r, :])

    def scores_back(v, da, prob):
        dp = dot_tn(v, da).astype(BF).astype(F32)
        weighted = prob * dp
        return ((weighted - prob * jnp.sum(weighted, axis=0, keepdims=True)) * scale).astype(BF)

    def write(stored):
        for ref, at, value in stored:
            ref[at] = value

    def late_heads(js):
        stored = []
        cos_t, sin_t = cos_ref[:, rows:], sin_ref[:, rows:]
        late, early = slice(rows, None), slice(0, rows)
        for j in js:
            r_q, r_k, r_v = head_rows(j)
            r_a = mix_rows(j)
            da = add_bf(gm_send[r_a, late], gm_recv[r_a, late])
            prob = late_ref[j]
            k = rot_ref[r_k, :]
            ds = scores_back(rot_ref[r_v, :], da, prob)
            dv = dot_nt(da, prob.astype(BF))
            dk = dot_nt(rot_ref[r_q, late], ds)
            stored += [(dqkv_ref, (r_q, late), unrope(dot_nn(k, ds).astype(BF), cos_t, sin_t)),
                       (dqkv_ref, (r_k, late), unrope(dk[:, late].astype(BF), cos_t, sin_t)),
                       (dqkv_ref, (r_v, late), dv[:, late].astype(BF)),
                       (kv_part, (0, r_a), dk[:, early]), (kv_part, (1, r_a), dv[:, early])]
        write(stored)

    def late_mine(i, carry):
        late_heads((mine(2 * i), mine(2 * i + 1)))
        return carry

    def late_theirs(i, carry):
        j = theirs(i)
        rot_copy(i, j).wait_recv()
        r_q, r_k, _ = head_rows(j)
        probabilities(j, rot_ref[r_q, :], rot_ref[r_k, :])
        late_heads((j,))
        return carry

    def early_body(i, carry):
        stored = []
        early = slice(0, rows)
        cos_t, sin_t = cos_ref[:, early], sin_ref[:, early]
        for j in (2 * i, 2 * i + 1):
            r_q, r_k, r_v = head_rows(j)
            r_a = mix_rows(j)
            da = add_bf(gm_send[r_a, early], gm_recv[r_a, early])
            prob = early_ref[j]
            ds = scores_back(rot_ref[r_v, early], da, prob)
            dv = kv_part[1, r_a, :] + dot_nt(da, prob.astype(BF))
            dk = kv_part[0, r_a, :] + dot_nt(rot_ref[r_q, early], ds)
            stored += [(dqkv_ref, (r_q, early), unrope(dot_nn(rot_ref[r_k, early], ds).astype(BF), cos_t, sin_t)),
                       (dqkv_ref, (r_k, early), unrope(dk.astype(BF), cos_t, sin_t)),
                       (dqkv_ref, (r_v, early), dv.astype(BF))]
        write(stored)
        return carry

    def cot_product(c, lo, hi):
        return dot_tn(dqkv_ref[lo:hi, c * rows:(c + 1) * rows], wqkv_ref[lo:hi, :])

    def input_cot(c):
        r = pl.ds(c * rows, rows)
        cot = cot_product(c, half_chans, None) + (cot_ref[...] if c == EARLY else cot_product(c, 0, half_chans))
        part_ref[SLOT[AR_R1], r, :] = cot.astype(BF)
        p1_copy(AR_R1, c).start()
        unit = x_ref[r, :].astype(F32) * inv1_ref[r, :]
        dots_put(CHUNKS + c, jnp.sum(cot * g1_ref[...] * unit, axis=-1, keepdims=True))

    def input_back(c):
        r = pl.ds(c * rows, rows)
        dots = dots_get(CHUNKS + c)
        stage4(AR_R1, c)
        inv1 = inv1_ref[r, :]
        unit = x_ref[r, :].astype(F32) * inv1
        gin = full_ref[SLOT[AR_R1], r, :].astype(F32)
        norm = inv1 * (gin * g1_ref[...] - unit * (dots / full_width))
        dx_ref[r, :] = (dh_ref[r, :].astype(F32) + norm).astype(BF)
        stores.append(store(dx_ref.at[r], dx_hbm.at[r], 8 + c))
        dg1_ref[...] += jnp.sum(gin * unit, axis=0, keepdims=True)

    def rest_of_gate_up():
        gu_start(EARLY, 2)
        gu_start(EARLY, 3)

    mlp_pieces(LATE, 0, GU_PIECES)
    mlp_end(LATE)
    gu_start(EARLY, 1)
    stage2(AR_R2, LATE)
    down_chunk(LATE)
    stage3(AR_R2, LATE)
    stage2(AR_Y, LATE)
    hidden_back(LATE, rest_of_gate_up)
    mlp_pieces(EARLY, 0, 2)
    stage3(AR_Y, LATE)
    gm_copy(LATE, emb).wait_recv()
    lax.fori_loop(0, half_heads // 2, late_mine, 0)
    y_chunk(LATE)
    mlp_pieces(EARLY, 2, GU_PIECES)
    mlp_end(EARLY)
    for i in range(2, half_heads):
        rot_copy(i, mine(i)).start()
    stores.append(store(dgu_ref, dgu_hbm, 3))
    stores.append(store(act_ref, act_hbm, 4))
    stage2(AR_R2, EARLY)
    down_chunk(EARLY)
    gm_copy(LATE, 1 - emb).wait_recv()
    lax.fori_loop(0, 2, late_theirs, 0)
    stage3(AR_R2, EARLY)
    hidden_back(EARLY)
    stores.append(store(dh_ref, dh_hbm, 5))
    stores.append(store(dg2_ref, dg2_hbm, 6))
    stage2(AR_Y, EARLY)
    lax.fori_loop(2, half_heads, late_theirs, 0)
    input_cot(LATE)
    gm_copy(EARLY, 0).wait_recv()
    stage2(AR_R1, LATE)
    lax.fori_loop(0, half_heads // 2, early_body, 0)
    cot_ref[...] = cot_product(EARLY, 0, half_chans)
    gm_copy(EARLY, 1).wait_recv()
    lax.fori_loop(half_heads // 2, half_heads, early_body, 0)
    input_cot(EARLY)
    stores.append(store(dqkv_ref, dqkv_hbm, 7))
    stage2(AR_R1, EARLY)
    stage3(AR_R1, LATE)
    stage3(AR_Y, EARLY)
    input_back(LATE)
    y_chunk(EARLY)
    stores.append(store(h_ref, y_hbm, 10))
    stage3(AR_R1, EARLY)
    input_back(EARLY)
    stores.append(store(dg1_ref, dg1_hbm, 11))

    for k in range(3):
        stat_copy(k).wait_send()
    for k in range(2 * CHUNKS):
        dots_all(k).wait_send()
    ga_all.wait_send()
    mix_all(emb).wait_send()
    at = rot_ref.at[step(emb, half_chans)]
    send(at, at, rt_s.at[0], rt_r.at[0], partner).wait_send()
    for c in range(CHUNKS):
        at = (slice(None), pl.ds(c * rows, rows))
        send(gm_send.at[at], gm_recv.at[at], gm_s.at[c], gm_r.at[0], partner).wait_send()
        for i in (AR_R2, AR_Y, AR_R1):
            p2_copy(i, c).wait_send()
    gu_sent(LATE)
    for i in (AR_R2, AR_Y, AR_R1):
        p1_p3_sent(i)
    for copy in stores:
        copy.wait()


def run_layer(x_in, positions, gain_one, gain_two, w_qkv, w_out, w_gu, w_down, grad_out):
    tokens, width = x_in.shape
    ff = w_down.shape[0]
    chans = w_qkv.shape[0]
    mix = w_out.shape[0]
    heads = mix // HEAD
    rows = tokens // CHUNKS
    act = lambda n, dtype=BF: jax.ShapeDtypeStruct((tokens, n), dtype)
    any_spec = pl.BlockSpec(memory_space=pl.ANY)
    vmem_spec = pl.BlockSpec(memory_space=pltpu.VMEM)
    raw_rows = 128 * 32
    scratch = [
        pltpu.VMEM((tokens, width), BF), pltpu.VMEM((tokens, width), BF),
        pltpu.VMEM((chans, width), BF), pltpu.VMEM((mix, width), BF),
        pltpu.VMEM((width, ff), BF), pltpu.VMEM((width, ff), BF), pltpu.VMEM((ff, width), BF),
        pltpu.VMEM((2, raw_rows, 128), BF),
        pltpu.VMEM((1, width), F32), pltpu.VMEM((1, width), F32), pltpu.VMEM((HALF, tokens), F32), pltpu.VMEM((HALF, tokens), F32),
        pltpu.VMEM((tokens, width), BF), pltpu.VMEM((tokens, width), BF), pltpu.VMEM((tokens, width), BF), pltpu.VMEM((tokens, width), BF),
        pltpu.VMEM((tokens, ff), BF), pltpu.VMEM((tokens, 2 * ff), BF),
        pltpu.VMEM((chans, tokens), BF), pltpu.VMEM((heads, tokens, rows), F32), pltpu.VMEM((heads, rows, rows), F32), pltpu.VMEM((mix, tokens), BF), pltpu.VMEM((chans, tokens), BF),
        pltpu.VMEM((tokens, width), BF),
        pltpu.VMEM((2, mix, rows), F32), pltpu.VMEM((rows, width), F32), pltpu.VMEM((2 * CHUNKS, 8, 8, rows), F32), pltpu.VMEM((1, width), F32), pltpu.VMEM((1, width), F32),
        pltpu.VMEM((tokens, 1), F32), pltpu.VMEM((tokens, 1), F32),
        pltpu.VMEM((tokens, ff), BF), pltpu.VMEM((tokens, ff), BF),
        pltpu.VMEM((chans, tokens), BF), pltpu.VMEM((chans, tokens), BF),
        pltpu.VMEM((tokens, 2 * ff), BF), pltpu.VMEM((tokens, 2 * ff), BF),
        pltpu.VMEM((mix, tokens), BF), pltpu.VMEM((mix, tokens), BF),
        pltpu.VMEM((3, 8, tokens), F32), pltpu.VMEM((3, 8, tokens), F32),
        pltpu.VMEM((3, tokens, width), BF), pltpu.VMEM((3, tokens, width // 2), BF), pltpu.VMEM((3, tokens, width // 2), BF),
        pltpu.VMEM((3, tokens, width // 2), BF), pltpu.VMEM((3, tokens, width), BF),
        pltpu.SemaphoreType.DMA((5,)), pltpu.SemaphoreType.DMA((2,)), pltpu.SemaphoreType.DMA((10 + CHUNKS,)),
    ]
    half_heads = heads // 2
    for n in (3, 3, 1, 1, 1, half_heads, CHUNKS, GU_PIECES * CHUNKS, CHUNKS, 2 * CHUNKS, 4, 4 * CHUNKS, 4 * CHUNKS, 4 * CHUNKS, 4, 4 * CHUNKS,
              2 * CHUNKS, 2 * CHUNKS, 1, 1, 1, half_heads):
        scratch += [pltpu.SemaphoreType.DMA((n,))]
    vec = jax.ShapeDtypeStruct((1, width), F32)
    return pl.pallas_call(
        layer_kernel,
        name="layer",
        out_shape=(act(width), act(width), vec, vec, act(width), jax.ShapeDtypeStruct((chans, tokens), BF),
                   jax.ShapeDtypeStruct((mix, tokens), BF), act(width), act(width), act(2 * ff), act(ff)),
        in_specs=[any_spec, any_spec, vmem_spec, vmem_spec, vmem_spec, any_spec, any_spec, any_spec, any_spec],
        out_specs=(any_spec,) * 11,
        scratch_shapes=scratch,
        compiler_params=pltpu.CompilerParams(collective_id=0, has_side_effects=True, vmem_limit_bytes=67000000),
    )(x_in, grad_out, gain_one, gain_two, positions, w_qkv, w_out, w_gu, w_down)


def grads_kernel(act_hbm, dy_hbm, r2_hbm, dgu_hbm, mix_hbm, dh_hbm, dqkv_hbm, r1_hbm, y_in, dx_in, dg1_in, dg2_in,
                 down_out, gu_out, wout_out, qkv_out, y_out, dx_out, dg1_out, dg2_out,
                 act_ref, dy_ref, r2_ref, dgu_ref, mix_ref, dh_ref, dqkv_ref, r1_ref, y_ref, dx_ref, rows_ref, inter_ref,
                 load_sem, rows_sem, inter_sem, end_sem):
    block = rows_ref.shape[1]
    pad = inter_ref.shape[1] // GU_BLOCK
    ff = dgu_ref.shape[1] // 2
    pairs = [(dqkv_hbm, dqkv_ref), (r1_hbm, r1_ref), (r2_hbm, r2_ref), (dgu_hbm, dgu_ref), (mix_hbm, mix_ref), (dh_hbm, dh_ref),
             (act_hbm, act_ref), (dy_hbm, dy_ref), (y_in, y_ref), (dx_in, dx_ref)]
    loads = [pltpu.make_async_copy(src, dst, load_sem.at[n]) for n, (src, dst) in enumerate(pairs)]
    for copy in loads[:2]:
        copy.start()
    dg1_out[...] = dg1_in[...].reshape(dg1_out.shape)
    dg2_out[...] = dg2_in[...].reshape(dg2_out.shape)

    slots, inter_slots = rows_ref.shape[0], inter_ref.shape[0]

    def rows_copy(out, index, slot):
        return pltpu.make_async_copy(rows_ref.at[slot], out.at[step(index, block)], rows_sem.at[slot])

    def product(out, lhs_of, rhs_ref, first):
        def body(i, carry):
            slot = lax.rem(i + first, slots)

            @pl.when(i + first >= slots)
            def _():
                rows_copy(out, 0, slot).wait()
            rows_ref[slot] = lhs_of(i, rhs_ref)
            rows_copy(out, i, slot).start()
            return carry
        count = out.shape[0] // block
        lax.fori_loop(0, count, body, 0)
        return first + count

    def plain_rows(ref):
        return lambda i, rhs_ref: dot_nn(ref[step(i, block), :], rhs_ref[...])

    loads[0].wait()
    loads[1].wait()
    for copy in loads[2:]:
        copy.start()
    sent = product(qkv_out, plain_rows(dqkv_ref), r1_ref, 0)

    loads[2].wait()
    loads[3].wait()

    def inter_copy(index, slot):
        return pltpu.make_async_copy(inter_ref.at[slot].reshape(GU_BLOCK, pad, 128).at[:, 0:32, :],
                                     gu_out.at[step(index, GU_BLOCK)], inter_sem.at[slot])

    gu_steps = gu_out.shape[0] // GU_BLOCK

    def gu_body(i, carry):
        slot = lax.rem(i, inter_slots)

        @pl.when(i >= inter_slots)
        def _():
            inter_copy(0, slot).wait()
        lhs = r2_ref[:, step(i, GU_BLOCK)].T
        for k in range(2):
            for n in range(ff // 512):
                val = dot_nn(lhs, dgu_ref[:, k * ff + n * 512:k * ff + (n + 1) * 512])
                for t in range(4):
                    row = 2 * (4 * n + t) + k
                    inter_ref[slot, pl.ds(row, GU_BLOCK, stride=pad), :] = val[:, t * 128:(t + 1) * 128]
        inter_copy(i, slot).start()
        return carry

    lax.fori_loop(0, gu_steps, gu_body, 0)

    loads[4].wait()
    loads[5].wait()
    sent = product(wout_out, plain_rows(mix_ref), dh_ref, sent)
    loads[6].wait()
    loads[7].wait()
    sent = product(down_out, lambda i, rhs_ref: dot_tn(act_ref[:, step(i, block)], rhs_ref[...]), dy_ref, sent)
    loads[8].wait()
    loads[9].wait()
    ends = [pltpu.make_async_copy(y_ref, y_out, end_sem.at[0]), pltpu.make_async_copy(dx_ref, dx_out, end_sem.at[1])]
    for copy in ends:
        copy.start()
    for slot in range(slots):
        rows_copy(down_out, 0, slot).wait()
    for slot in range(inter_slots):
        inter_copy(0, slot).wait()
    for copy in ends:
        copy.wait()


GU_BLOCK = 128


def weight_grads(act, grad_out, r2, dgu, mix, dh, dqkv, r1, y, dx, dg1, dg2):
    tokens, width = r2.shape
    ff = act.shape[1]
    any_spec = pl.BlockSpec(memory_space=pl.ANY)
    vmem_spec = pl.BlockSpec(memory_space=pltpu.VMEM)
    out = lambda *shape: jax.ShapeDtypeStruct(shape, F32)
    like = lambda a: jax.ShapeDtypeStruct(a.shape, a.dtype)
    arrays = (act, grad_out, r2, dgu, mix, dh, dqkv, r1, y, dx)
    return pl.pallas_call(
        grads_kernel,
        name="weight_grads",
        in_specs=[any_spec] * 10 + [vmem_spec] * 2,
        out_specs=[any_spec] * 6 + [vmem_spec] * 2,
        out_shape=[out(ff, width), out(width, 32, 128), out(mix.shape[0], width), out(dqkv.shape[0], width), like(y), like(dx), out(width), out(width)],
        scratch_shapes=[pltpu.VMEM(a.shape, a.dtype) for a in arrays] + [
            pltpu.VMEM((8, 256, width), F32), pltpu.VMEM((6, GU_BLOCK * 40, 128), F32),
            pltpu.SemaphoreType.DMA((10,)), pltpu.SemaphoreType.DMA((8,)), pltpu.SemaphoreType.DMA((6,)), pltpu.SemaphoreType.DMA((2,))],
        compiler_params=pltpu.CompilerParams(vmem_limit_bytes=56 << 20),
    )(*arrays, dg1, dg2)


def solution(mesh):
    def per_device(x_in, positions, gain_one, gain_two, w_qkv, w_out, w_gu, w_down, grad_out):
        width, groups, chans = w_qkv.shape
        ff = w_down.shape[0]
        qkv_rows = w_qkv.transpose(1, 2, 0).reshape(groups * chans, width)
        gu_rows = w_gu.reshape(width, 2, ff // 128, 128).transpose(0, 2, 1, 3).reshape(width * 2 * (ff // 128), 128)
        y, dx, dg1, dg2, r1, dqkv, mix, dh, r2, dgu, act = run_layer(
            x_in, positions, gain_one, gain_two, qkv_rows, w_out, gu_rows, w_down, grad_out)
        d_down, d_gu, d_out, d_qkv, y, dx, dg1, dg2 = weight_grads(act, grad_out, r2, dgu, mix, dh, dqkv, r1, y, dx, dg1, dg2)
        d_gu = d_gu.reshape(width, ff // 128, 2, 128).transpose(0, 2, 1, 3).reshape(width, 2, ff)
        d_qkv = d_qkv.reshape(groups, chans, width).transpose(2, 0, 1)
        return y, dx, dg1, dg2, d_qkv, d_out, d_gu, d_down

    act_spec = P('dp', 'embed')
    in_specs = (act_spec, P('dp'), P('embed'), P('embed'), P('embed', 'heads', None), P('heads', 'embed'), P('embed', None, 'heads'), P('heads', 'embed'), act_spec)
    out_specs = (act_spec, act_spec, P(('dp', 'embed')), P(('dp', 'embed')), P(('dp', 'embed'), 'heads', None), P(('dp', 'heads'), 'embed'), P(('dp', 'embed'), None, 'heads'), P(('dp', 'heads'), 'embed'))
    return jax.shard_map(per_device, mesh=mesh, in_specs=in_specs, out_specs=out_specs, check_vma=False)
```

```python
import math

import jax
import jax.numpy as jnp
from jax import lax
from jax.experimental import pallas as pl
from jax.experimental.pallas import tpu as pltpu
from jax.sharding import PartitionSpec as P

EPSILON = 1e-5
ROPE_BASE = 10000.0
HEAD = 96
HALF = HEAD // 2
GROUP = 3 * HEAD
CHUNKS = 2
MESH = pl.DeviceIdType.MESH
BF = jnp.bfloat16
F32 = jnp.float32

AR_OUT, AR_R2, AR_Y, AR_R1 = range(4)
SLOT = (0, 1, 2, 0)
GU_PIECES = 4
EARLY, LATE = 0, 1


def dot_nn(lhs, rhs):
    return lax.dot_general(lhs, rhs, (((1,), (0,)), ((), ())), preferred_element_type=F32)


def dot_nt(lhs, rhs):
    return lax.dot_general(lhs, rhs, (((1,), (1,)), ((), ())), preferred_element_type=F32)


def dot_tn(lhs, rhs):
    return lax.dot_general(lhs, rhs, (((0,), (0,)), ((), ())), preferred_element_type=F32)


def add_bf(one, two):
    return (one.astype(F32) + two.astype(F32)).astype(BF)


def step(index, size):
    return pl.ds(pl.multiple_of(index * size, size), size)


def layer_kernel(x_hbm, dy_hbm, g1_in, g2_in, pos_in, wqkv_hbm, wout_hbm, wgu_hbm, wdown_hbm,
                 y_hbm, dx_hbm, dg1_hbm, dg2_hbm, r1_hbm, dqkv_hbm, mix_hbm, dh_hbm, r2_hbm, dgu_hbm, act_hbm,
                 x_ref, dy_ref, wqkv_ref, wout_ref, wg_ref, wu_ref, wdown_ref, raw_ref,
                 g1_ref, g2_ref, cos_ref, sin_ref, r1_ref, r2_ref, h_ref, dh_ref, act_ref, dgu_ref, rot_ref, late_ref, early_ref, mix_ref, dqkv_ref, dx_ref,
                 kv_part, cot_ref, dots_ref, dg1_ref, dg2_ref,
                 inv1_ref, inv2_ref,
                 ga_send, ga_recv, qkv_send, qkv_recv, gu_send, gu_recv, gm_send, gm_recv, stat_send, stat_recv,
                 part_ref, sib_ref, half_ref, far_ref, full_ref,
                 load_sem, raw_sem, store_sem,
                 st_s, st_r, ga_s, ga_r, qk_s, qk_r, gu_s, gu_r, gm_s, gm_r, p1_s, p1_r, p2_s, p2_r, p3_s, p3_r, dots_s, dots_r, mx_s, mx_r, rt_s, rt_r):
    tokens, width = x_ref.shape
    full_width = 2 * width
    ff = wdown_ref.shape[0]
    heads = wqkv_ref.shape[0] // GROUP
    half_width = width // 2
    rows = tokens // CHUNKS
    emb = lax.axis_index("embed")
    hid = lax.axis_index("heads")
    core = lax.rem(hid, 2)
    sibling = {"heads": hid + 1 - 2 * core}
    across = {"heads": lax.rem(hid + 2, 4)}
    partner = {"embed": 1 - emb}

    barrier = pltpu.get_barrier_semaphore()
    others = [{"embed": lax.rem(emb + n // 4, 2), "heads": lax.rem(hid + n, 4)} for n in range(1, 8)]
    for peer in others:
        pl.semaphore_signal(barrier, inc=1, device_id=peer, device_id_type=MESH)

    def load(src, dst, sem):
        return pltpu.make_async_copy(src, dst, load_sem.at[sem])

    first, rest = pl.ds(0, ff // 8), pl.ds(ff // 8, ff - ff // 8)
    loads = [load(x_hbm, x_ref, 0), load(dy_hbm, dy_ref, 1), load(wdown_hbm.at[first], wdown_ref.at[first], 2),
             load(wqkv_hbm, wqkv_ref, 3), load(wout_hbm, wout_ref, 4), load(wdown_hbm.at[rest], wdown_ref.at[rest], 5)]
    for copy in loads[:4]:
        copy.start()

    raw_rows = raw_ref.shape[1]
    raw_steps = wgu_hbm.shape[0] // raw_rows

    def raw_load(index, slot):
        return pltpu.make_async_copy(wgu_hbm.at[step(index, raw_rows)], raw_ref.at[slot], raw_sem.at[slot])

    def store(src, dst, sem):
        copy = pltpu.make_async_copy(src, dst, store_sem.at[sem])
        copy.start()
        return copy

    def send(src, dst, s_sem, r_sem, peer):
        return pltpu.make_async_remote_copy(src_ref=src, dst_ref=dst, send_sem=s_sem, recv_sem=r_sem,
                                            device_id=peer, device_id_type=MESH)

    def stat_copy(k):
        return send(stat_send.at[k], stat_recv.at[k], st_s.at[k], st_r.at[k], partner)

    ga_cols = ff // 8

    def ga_copy(k):
        cols = step(k, ga_cols)
        return send(ga_send.at[:, cols], ga_recv.at[:, cols], ga_s.at[0], ga_r.at[0], partner)

    ga_all = send(ga_send, ga_recv, ga_s.at[0], ga_r.at[0], partner)

    def qkv_copy(i, j):
        r = step(j, GROUP)
        return send(qkv_send.at[r], qkv_recv.at[r], qk_s.at[0], qk_r.at[i], partner)

    half_heads = heads // 2
    half_chans = half_heads * GROUP

    def mine(i):
        return emb * half_heads + i

    def theirs(i):
        return (1 - emb) * half_heads + i

    def mix_rows(j):
        return pl.ds(pl.multiple_of(j * HEAD, 32), HEAD)

    def mix_copy(j):
        at = mix_ref.at[mix_rows(j)]
        return send(at, at, mx_s.at[0], mx_r.at[0], partner)

    def mix_all(which):
        at = mix_ref.at[step(which, half_heads * HEAD)]
        return send(at, at, mx_s.at[0], mx_r.at[0], partner)

    def rot_copy(i, j):
        at = rot_ref.at[step(j, GROUP)]
        return send(at, at, rt_s.at[0], rt_r.at[i], partner)

    gu_cols = ff // GU_PIECES

    def gu_copy(c, q, k):
        at = (pl.ds(c * rows, rows), pl.ds(pl.multiple_of(k * ff + q * gu_cols, gu_cols), gu_cols))
        return send(gu_send.at[at], gu_recv.at[at], gu_s.at[c], gu_r.at[c * GU_PIECES + q], partner)

    def gu_pair(c, q):
        at = (pl.ds(c * rows, rows), pl.ds(0, 2 * gu_cols))
        return send(gu_send.at[at], gu_recv.at[at], gu_s.at[c], gu_r.at[c * GU_PIECES + q], partner)

    def gu_sent(c):
        at = pl.ds(c * rows, rows)
        send(gu_send.at[at], gu_recv.at[at], gu_s.at[c], gu_r.at[0], partner).wait_send()

    gm_rows = gm_send.shape[0] // 2

    def gm_copy(c, hf):
        at = (step(hf, gm_rows), pl.ds(c * rows, rows))
        return send(gm_send.at[at], gm_recv.at[at], gm_s.at[c], gm_r.at[2 * c + hf], partner)

    own = pl.ds(pl.multiple_of(core * half_width, half_width), half_width)
    other = pl.ds(pl.multiple_of((1 - core) * half_width, half_width), half_width)

    def p1_copy(i, c):
        r = pl.ds(c * rows, rows)
        k = i * CHUNKS + c
        return send(part_ref.at[SLOT[i], r, other], sib_ref.at[SLOT[i], r], p1_s.at[i], p1_r.at[k], sibling)

    def p2_copy(i, c):
        r = pl.ds(c * rows, rows)
        k = i * CHUNKS + c
        return send(half_ref.at[SLOT[i], r], far_ref.at[SLOT[i], r], p2_s.at[k], p2_r.at[k], across)

    def p3_copy(i, c):
        r = pl.ds(c * rows, rows)
        k = i * CHUNKS + c
        return send(full_ref.at[SLOT[i], r, own], full_ref.at[SLOT[i], r, own], p3_s.at[i], p3_r.at[k], sibling)

    def p1_p3_sent(i):
        n = SLOT[i]
        send(part_ref.at[n, :, other], sib_ref.at[n], p1_s.at[i], p1_r.at[0], sibling).wait_send()
        send(full_ref.at[n, :, own], full_ref.at[n, :, own], p3_s.at[i], p3_r.at[0], sibling).wait_send()

    def stage2(i, c):
        r = pl.ds(c * rows, rows)
        p1_copy(i, c).wait_recv()
        half_ref[SLOT[i], r, :] = add_bf(part_ref[SLOT[i], r, own], sib_ref[SLOT[i], r, :])
        p2_copy(i, c).start()

    def stage3(i, c):
        r = pl.ds(c * rows, rows)
        p2_copy(i, c).wait_recv()
        full_ref[SLOT[i], r, own] = add_bf(half_ref[SLOT[i], r, :], far_ref[SLOT[i], r, :])
        p3_copy(i, c).start()

    def stage4(i, c):
        p3_copy(i, c).wait_recv()

    def stat_put(k, col, n):
        flat = jnp.broadcast_to(col, (n, 128)).T[0:8, :]
        stat_send[k, :, 0:n] = flat
        stat_copy(k).start()

    def stat_get(k, n):
        stat_copy(k).wait_recv()
        total = stat_send[k, 0:1, 0:n] + stat_recv[k, 0:1, 0:n]
        return jnp.broadcast_to(total, (128, n)).T[:, 0:1]

    me = emb * 4 + hid

    def dots_copy(k, n):
        at = dots_ref.at[k, me]
        return send(at, at, dots_s.at[k], dots_r.at[k], others[n])

    def dots_all(k):
        at = dots_ref.at[k, pl.ds(0, 7)]
        return send(at, at, dots_s.at[k], dots_r.at[k], partner)

    def dots_put(k, col):
        dots_ref[k, me] = jnp.broadcast_to(col, (rows, 128)).T[0:8, :]
        for n in range(7):
            dots_copy(k, n).start()

    def dots_get(k):
        dots_all(k).wait_recv()
        total = dots_ref[k, 0, 0:1, :]
        for n in range(1, 8):
            total = total + dots_ref[k, n, 0:1, :]
        return jnp.broadcast_to(total, (128, rows)).T[:, 0:1]

    def ga_body(k, carry):
        cols = step(k, ga_cols)
        ga_send[:, cols] = dot_nt(dy_ref[...], wdown_ref[cols, :]).astype(BF)
        return carry

    loads[0].wait()
    x32 = x_ref[...].astype(F32)
    sq1 = jnp.sum(x32 * x32, axis=-1, keepdims=True)
    loads[1].wait()
    loads[2].wait()
    ga_body(0, 0)
    pl.semaphore_wait(barrier, 7)
    stat_put(0, sq1, tokens)
    ga_copy(0).start()
    for copy in loads[4:]:
        copy.start()
    for slot in range(2):
        raw_load(slot, slot).start()
    g1_ref[...] = g1_in[...].reshape(1, width)
    g2_ref[...] = g2_in[...].reshape(1, width)
    place = pos_in[...].reshape(1, tokens).astype(F32)
    pair_i = lax.broadcasted_iota(jnp.int32, (HALF, 1), 0).astype(F32)
    angles = jnp.exp(pair_i * (-2.0 * math.log(ROPE_BASE) / HEAD)) * place
    cos_ref[...] = jnp.cos(angles)
    sin_ref[...] = jnp.sin(angles)
    inv1 = lax.rsqrt(stat_get(0, tokens) / full_width + EPSILON)
    inv1_ref[...] = inv1
    r1_ref[...] = (x_ref[...].astype(F32) * inv1 * g1_ref[...]).astype(BF)
    stores = [store(r1_ref, r1_hbm, 0)]

    loads[3].wait()

    def qkv_product(j):
        r = step(j, GROUP)
        qkv_send[r, :] = dot_nt(wqkv_ref[r, :], r1_ref[...]).astype(BF)

    def qkv_theirs(i, carry):
        qkv_product(theirs(i))
        qkv_copy(i, theirs(i)).start()
        return carry

    def qkv_mine(i, carry):
        qkv_product(mine(i))
        return carry

    lax.fori_loop(0, half_heads, qkv_theirs, 0)
    lax.fori_loop(0, half_heads, qkv_mine, 0)
    loads[5].wait()
    lax.fori_loop(1, 8, ga_body, 0)

    row_i = lax.broadcasted_iota(jnp.int32, (256, 256), 0)
    col_i = lax.broadcasted_iota(jnp.int32, (256, 256), 1)
    perm = (col_i == (row_i % 8) * 32 + row_i // 8).astype(F32).astype(BF)
    blocks = raw_rows // 512

    def raw_body(i, carry):
        slot = lax.rem(i, 2)
        raw_load(i, slot).wait()

        def block_body(b, inner):
            for u in range(4):
                base = pl.multiple_of(b * 2048 + u * 512, 512)
                pair = jnp.concatenate([raw_ref[slot, pl.ds(base, 256), :], raw_ref[slot, pl.ds(base + 256, 256), :]], axis=1)
                out = dot_nn(perm, pair)
                d = pl.ds(pl.multiple_of(i * (raw_rows // 32) + b * 64 + u * 16, 16), 16)
                for t in range(16):
                    for k, dst in ((0, wg_ref), (1, wu_ref)):
                        r = (2 * t + k) * 8
                        both = jnp.concatenate([out[r:r + 8, 0:128], out[r:r + 8, 128:256]], axis=0)
                        dst[d, t * 128:(t + 1) * 128] = both.astype(BF)
            return inner

        lax.fori_loop(0, blocks // 4, block_body, 0)

        @pl.when(i + 2 < raw_steps)
        def _():
            raw_load(i + 2, slot).start()
        return carry

    part_one, part_two = raw_steps // 2, raw_steps - raw_steps // 3
    lax.fori_loop(0, part_one, raw_body, 0)

    scale = HEAD ** -0.5
    causal = (lax.broadcasted_iota(jnp.int32, (tokens, tokens), 0) <= lax.broadcasted_iota(jnp.int32, (tokens, tokens), 1))

    def rope(v, cos_t, sin_t):
        v = v.astype(F32)
        one, two = v[0:HALF], v[HALF:HEAD]
        return jnp.concatenate([one * cos_t - two * sin_t, two * cos_t + one * sin_t], axis=0).astype(BF)

    def unrope(v, cos_t, sin_t):
        v = v.astype(F32)
        one, two = v[0:HALF], v[HALF:HEAD]
        return jnp.concatenate([one * cos_t + two * sin_t, two * cos_t - one * sin_t], axis=0).astype(BF)

    last = half_heads - 1

    def head_rows(j):
        base = pl.multiple_of(j * GROUP, 32)
        return tuple(pl.ds(base + n * HEAD, HEAD) for n in range(3))

    def probabilities(j, q, k):
        scores = jnp.where(causal, dot_tn(k, q) * scale, -1e30)
        weight = jnp.exp(scores - jnp.max(scores, axis=0, keepdims=True))
        prob = weight / jnp.sum(weight, axis=0, keepdims=True)
        late_ref[j] = prob[:, rows:]
        early_ref[j] = prob[0:rows, 0:rows]
        return prob

    def attn_body(i, carry):
        j = mine(i)

        @pl.when(i == last)
        def _():
            r = step(1 - emb, half_chans)
            send(qkv_send.at[r], qkv_recv.at[r], qk_s.at[0], qk_r.at[0], partner).wait_send()
            ga_copy(1).start()
        qkv_copy(i, j).wait_recv()
        r_q, r_k, r_v = head_rows(j)
        cos_t, sin_t = cos_ref[...], sin_ref[...]
        q = rope(add_bf(qkv_send[r_q, :], qkv_recv[r_q, :]), cos_t, sin_t)
        k = rope(add_bf(qkv_send[r_k, :], qkv_recv[r_k, :]), cos_t, sin_t)
        v = add_bf(qkv_send[r_v, :], qkv_recv[r_v, :])
        rot_ref[r_q, :] = q
        rot_ref[r_k, :] = k
        rot_ref[r_v, :] = v
        prob = probabilities(j, q, k)
        mix_ref[mix_rows(j), :] = dot_nn(v, prob.astype(BF)).astype(BF)
        mix_copy(j).start()
        return carry

    lax.fori_loop(0, half_heads, attn_body, 0)
    for n in range(2, 6):
        ga_copy(n).start()
    lax.fori_loop(part_one, part_two, raw_body, 0)
    mix_all(1 - emb).wait_recv()
    stores.append(store(mix_ref, mix_hbm, 1))

    loads[4].wait()
    order = tuple(reversed(range(CHUNKS)))
    for c in order:
        r = pl.ds(c * rows, rows)
        part_ref[SLOT[AR_OUT], r, :] = dot_tn(mix_ref[:, c * rows:(c + 1) * rows], wout_ref[...]).astype(BF)
        p1_copy(AR_OUT, c).start()
    def gu_start(c, q):
        for k in range(2):
            gu_copy(c, q, k).start()

    def hidden_fwd(c):
        r = pl.ds(c * rows, rows)
        stage4(AR_OUT, c)
        h = add_bf(x_ref[r, :], full_ref[SLOT[AR_OUT], r, :])
        h_ref[r, :] = h
        h32 = h.astype(F32)
        stat_put(1 + c, jnp.sum(h32 * h32, axis=-1, keepdims=True), rows)

    def gate_up(c, at_once):
        r = pl.ds(c * rows, rows)
        inv2 = lax.rsqrt(stat_get(1 + c, rows) / full_width + EPSILON)
        inv2_ref[r, :] = inv2
        r2_ref[r, :] = (h_ref[r, :].astype(F32) * inv2 * g2_ref[...]).astype(BF)

        def gu_body(q, carry):
            for k, w_ref in ((0, wg_ref), (1, wu_ref)):
                dst = pl.ds(pl.multiple_of(k * ff + q * gu_cols, gu_cols), gu_cols)
                gu_send[r, dst] = dot_nn(r2_ref[r, :], w_ref[:, step(q, gu_cols)]).astype(BF)

            @pl.when(q < at_once)
            def _():
                gu_start(c, q)
            return carry

        lax.fori_loop(0, GU_PIECES, gu_body, 0)

    stage2(AR_OUT, LATE)
    lax.fori_loop(part_two, raw_steps, raw_body, 0)
    p2_copy(AR_OUT, LATE).wait_send()
    stage2(AR_OUT, EARLY)
    stage3(AR_OUT, LATE)
    hidden_fwd(LATE)
    for k in range(6, 8):
        ga_copy(k).start()
    gate_up(LATE, 2)
    stage3(AR_OUT, EARLY)
    hidden_fwd(EARLY)
    gu_start(LATE, 2)
    gu_start(LATE, 3)
    gate_up(EARLY, 0)
    tile = 512
    stores.append(store(r2_ref, r2_hbm, 2))

    ga_all.wait_recv()
    p1_p3_sent(AR_OUT)
    p2_copy(AR_OUT, EARLY).wait_send()

    def mlp_pieces(c, lo, hi):
        r = pl.ds(c * rows, rows)
        if lo == 0:
            cot_ref[...] = jnp.zeros_like(cot_ref)

        def piece(q, carry):
            if c == EARLY:
                @pl.when(q == GU_PIECES - 1)
                def _():
                    gu_sent(EARLY)
                    for i in range(2):
                        rot_copy(i, mine(i)).start()
            gu_pair(c, q).wait_recv()
            if c == LATE:
                @pl.when(q == 2)
                def _():
                    gu_start(EARLY, 0)
            for n in range(gu_cols // 256):
                cg = pl.ds(pl.multiple_of(q * gu_cols + n * 256, 256), 256)
                cu = pl.ds(pl.multiple_of(ff + q * gu_cols + n * 256, 256), 256)
                gate = add_bf(gu_send[r, cg], gu_recv[r, cg]).astype(F32)
                up = add_bf(gu_send[r, cu], gu_recv[r, cu]).astype(F32)
                ga = add_bf(ga_send[r, cg], ga_recv[r, cg]).astype(F32)
                sig = 1.0 / (1.0 + jnp.exp(-gate))
                silu = gate * sig
                act_ref[r, cg] = (silu * up).astype(BF)
                dgu_ref[r, cg] = (ga * up * (sig * (1.0 + gate * (1.0 - sig)))).astype(BF)
                dgu_ref[r, cu] = (ga * silu).astype(BF)
            at_g = step(q, gu_cols)
            at_u = pl.ds(pl.multiple_of(ff + q * gu_cols, gu_cols), gu_cols)
            for n in range(width // tile):
                w = slice(n * tile, (n + 1) * tile)
                cot_ref[:, w] += dot_nt(dgu_ref[r, at_g], wg_ref[w, at_g]) + dot_nt(dgu_ref[r, at_u], wu_ref[w, at_g])
            return carry

        lax.fori_loop(lo, hi, piece, 0)

    def mlp_end(c):
        r = pl.ds(c * rows, rows)
        part_ref[SLOT[AR_R2], r, :] = cot_ref[...].astype(BF)
        p1_copy(AR_R2, c).start()
        unit = h_ref[r, :].astype(F32) * inv2_ref[r, :]
        dots_put(c, jnp.sum(cot_ref[...] * g2_ref[...] * unit, axis=-1, keepdims=True))

    def down_chunk(c):
        r = pl.ds(c * rows, rows)

        def down_body(n, carry):
            w = step(n, tile)
            part_ref[SLOT[AR_Y], r, w] = dot_nn(act_ref[r, :], wdown_ref[:, w]).astype(BF)
            return carry

        lax.fori_loop(0, width // tile, down_body, 0)
        p1_copy(AR_Y, c).start()

    dg1_ref[...] = jnp.zeros_like(dg1_ref)
    dg2_ref[...] = jnp.zeros_like(dg2_ref)

    def hidden_back(c, then=lambda: None):
        r = pl.ds(c * rows, rows)
        dots = dots_get(c)
        stage4(AR_R2, c)
        inv2 = inv2_ref[r, :]
        unit = h_ref[r, :].astype(F32) * inv2
        gin = full_ref[SLOT[AR_R2], r, :].astype(F32)
        norm = inv2 * (gin * g2_ref[...] - unit * (dots / full_width))
        dh_ref[r, :] = (dy_ref[r, :].astype(F32) + norm).astype(BF)
        gm_send[:, c * rows:(c + 1) * rows] = dot_nt(wout_ref[...], dh_ref[r, :]).astype(BF)
        for hf in range(2):
            gm_copy(c, hf).start()
        then()
        dg2_ref[...] += jnp.sum(gin * unit, axis=0, keepdims=True)

    def y_chunk(c):
        r = pl.ds(c * rows, rows)
        stage4(AR_Y, c)
        h_ref[r, :] = add_bf(h_ref[r, :], full_ref[SLOT[AR_Y], r, :])

    def scores_back(v, da, prob):
        dp = dot_tn(v, da).astype(BF).astype(F32)
        weighted = prob * dp
        return ((weighted - prob * jnp.sum(weighted, axis=0, keepdims=True)) * scale).astype(BF)

    def write(stored):
        for ref, at, value in stored:
            ref[at] = value

    def late_heads(js):
        stored = []
        cos_t, sin_t = cos_ref[:, rows:], sin_ref[:, rows:]
        late, early = slice(rows, None), slice(0, rows)
        for j in js:
            r_q, r_k, r_v = head_rows(j)
            r_a = mix_rows(j)
            da = add_bf(gm_send[r_a, late], gm_recv[r_a, late])
            prob = late_ref[j]
            k = rot_ref[r_k, :]
            ds = scores_back(rot_ref[r_v, :], da, prob)
            dv = dot_nt(da, prob.astype(BF))
            dk = dot_nt(rot_ref[r_q, late], ds)
            stored += [(dqkv_ref, (r_q, late), unrope(dot_nn(k, ds).astype(BF), cos_t, sin_t)),
                       (dqkv_ref, (r_k, late), unrope(dk[:, late].astype(BF), cos_t, sin_t)),
                       (dqkv_ref, (r_v, late), dv[:, late].astype(BF)),
                       (kv_part, (0, r_a), dk[:, early]), (kv_part, (1, r_a), dv[:, early])]
        write(stored)

    def late_mine(i, carry):
        late_heads((mine(2 * i), mine(2 * i + 1)))
        return carry

    def late_theirs(i, carry):
        j = theirs(i)
        rot_copy(i, j).wait_recv()
        r_q, r_k, _ = head_rows(j)
        probabilities(j, rot_ref[r_q, :], rot_ref[r_k, :])
        late_heads((j,))
        return carry

    def early_body(i, carry):
        stored = []
        early = slice(0, rows)
        cos_t, sin_t = cos_ref[:, early], sin_ref[:, early]
        for j in (2 * i, 2 * i + 1):
            r_q, r_k, r_v = head_rows(j)
            r_a = mix_rows(j)
            da = add_bf(gm_send[r_a, early], gm_recv[r_a, early])
            prob = early_ref[j]
            ds = scores_back(rot_ref[r_v, early], da, prob)
            dv = kv_part[1, r_a, :] + dot_nt(da, prob.astype(BF))
            dk = kv_part[0, r_a, :] + dot_nt(rot_ref[r_q, early], ds)
            stored += [(dqkv_ref, (r_q, early), unrope(dot_nn(rot_ref[r_k, early], ds).astype(BF), cos_t, sin_t)),
                       (dqkv_ref, (r_k, early), unrope(dk.astype(BF), cos_t, sin_t)),
                       (dqkv_ref, (r_v, early), dv.astype(BF))]
        write(stored)
        return carry

    def cot_product(c, lo, hi):
        return dot_tn(dqkv_ref[lo:hi, c * rows:(c + 1) * rows], wqkv_ref[lo:hi, :])

    def input_cot(c):
        r = pl.ds(c * rows, rows)
        cot = cot_product(c, half_chans, None) + (cot_ref[...] if c == EARLY else cot_product(c, 0, half_chans))
        part_ref[SLOT[AR_R1], r, :] = cot.astype(BF)
        p1_copy(AR_R1, c).start()
        unit = x_ref[r, :].astype(F32) * inv1_ref[r, :]
        dots_put(CHUNKS + c, jnp.sum(cot * g1_ref[...] * unit, axis=-1, keepdims=True))

    def input_back(c):
        r = pl.ds(c * rows, rows)
        dots = dots_get(CHUNKS + c)
        stage4(AR_R1, c)
        inv1 = inv1_ref[r, :]
        unit = x_ref[r, :].astype(F32) * inv1
        gin = full_ref[SLOT[AR_R1], r, :].astype(F32)
        norm = inv1 * (gin * g1_ref[...] - unit * (dots / full_width))
        dx_ref[r, :] = (dh_ref[r, :].astype(F32) + norm).astype(BF)
        stores.append(store(dx_ref.at[r], dx_hbm.at[r], 8 + c))
        dg1_ref[...] += jnp.sum(gin * unit, axis=0, keepdims=True)

    def rest_of_gate_up():
        gu_start(EARLY, 3)

    mlp_pieces(LATE, 0, GU_PIECES)
    mlp_end(LATE)
    gu_start(EARLY, 1)
    stage2(AR_R2, LATE)
    down_chunk(LATE)
    stage3(AR_R2, LATE)
    stage2(AR_Y, LATE)
    gu_start(EARLY, 2)
    hidden_back(LATE, rest_of_gate_up)
    mlp_pieces(EARLY, 0, 2)
    stage3(AR_Y, LATE)
    gm_copy(LATE, emb).wait_recv()
    lax.fori_loop(0, half_heads // 2, late_mine, 0)
    y_chunk(LATE)
    mlp_pieces(EARLY, 2, GU_PIECES)
    mlp_end(EARLY)
    for i in range(2, half_heads):
        rot_copy(i, mine(i)).start()
    stores.append(store(dgu_ref, dgu_hbm, 3))
    stores.append(store(act_ref, act_hbm, 4))
    stage2(AR_R2, EARLY)
    down_chunk(EARLY)
    gm_copy(LATE, 1 - emb).wait_recv()
    lax.fori_loop(0, 2, late_theirs, 0)
    stage3(AR_R2, EARLY)
    stage2(AR_Y, EARLY)
    hidden_back(EARLY)
    stores.append(store(dh_ref, dh_hbm, 5))
    stores.append(store(dg2_ref, dg2_hbm, 6))
    lax.fori_loop(2, half_heads, late_theirs, 0)
    input_cot(LATE)
    gm_copy(EARLY, 0).wait_recv()
    stage2(AR_R1, LATE)
    lax.fori_loop(0, half_heads // 2, early_body, 0)
    cot_ref[...] = cot_product(EARLY, 0, half_chans)
    gm_copy(EARLY, 1).wait_recv()
    lax.fori_loop(half_heads // 2, half_heads, early_body, 0)
    input_cot(EARLY)
    stores.append(store(dqkv_ref, dqkv_hbm, 7))
    stage2(AR_R1, EARLY)
    stage3(AR_R1, LATE)
    stage3(AR_Y, EARLY)
    input_back(LATE)
    y_chunk(EARLY)
    stores.append(store(h_ref, y_hbm, 10))
    stage3(AR_R1, EARLY)
    input_back(EARLY)
    stores.append(store(dg1_ref, dg1_hbm, 11))

    for k in range(3):
        stat_copy(k).wait_send()
    for k in range(2 * CHUNKS):
        dots_all(k).wait_send()
    ga_all.wait_send()
    mix_all(emb).wait_send()
    at = rot_ref.at[step(emb, half_chans)]
    send(at, at, rt_s.at[0], rt_r.at[0], partner).wait_send()
    for c in range(CHUNKS):
        at = (slice(None), pl.ds(c * rows, rows))
        send(gm_send.at[at], gm_recv.at[at], gm_s.at[c], gm_r.at[0], partner).wait_send()
        for i in (AR_R2, AR_Y, AR_R1):
            p2_copy(i, c).wait_send()
    gu_sent(LATE)
    for i in (AR_R2, AR_Y, AR_R1):
        p1_p3_sent(i)
    for copy in stores:
        copy.wait()


def run_layer(x_in, positions, gain_one, gain_two, w_qkv, w_out, w_gu, w_down, grad_out):
    tokens, width = x_in.shape
    ff = w_down.shape[0]
    chans = w_qkv.shape[0]
    mix = w_out.shape[0]
    heads = mix // HEAD
    rows = tokens // CHUNKS
    act = lambda n, dtype=BF: jax.ShapeDtypeStruct((tokens, n), dtype)
    any_spec = pl.BlockSpec(memory_space=pl.ANY)
    vmem_spec = pl.BlockSpec(memory_space=pltpu.VMEM)
    raw_rows = 128 * 32
    scratch = [
        pltpu.VMEM((tokens, width), BF), pltpu.VMEM((tokens, width), BF),
        pltpu.VMEM((chans, width), BF), pltpu.VMEM((mix, width), BF),
        pltpu.VMEM((width, ff), BF), pltpu.VMEM((width, ff), BF), pltpu.VMEM((ff, width), BF),
        pltpu.VMEM((2, raw_rows, 128), BF),
        pltpu.VMEM((1, width), F32), pltpu.VMEM((1, width), F32), pltpu.VMEM((HALF, tokens), F32), pltpu.VMEM((HALF, tokens), F32),
        pltpu.VMEM((tokens, width), BF), pltpu.VMEM((tokens, width), BF), pltpu.VMEM((tokens, width), BF), pltpu.VMEM((tokens, width), BF),
        pltpu.VMEM((tokens, ff), BF), pltpu.VMEM((tokens, 2 * ff), BF),
        pltpu.VMEM((chans, tokens), BF), pltpu.VMEM((heads, tokens, rows), F32), pltpu.VMEM((heads, rows, rows), F32), pltpu.VMEM((mix, tokens), BF), pltpu.VMEM((chans, tokens), BF),
        pltpu.VMEM((tokens, width), BF),
        pltpu.VMEM((2, mix, rows), F32), pltpu.VMEM((rows, width), F32), pltpu.VMEM((2 * CHUNKS, 8, 8, rows), F32), pltpu.VMEM((1, width), F32), pltpu.VMEM((1, width), F32),
        pltpu.VMEM((tokens, 1), F32), pltpu.VMEM((tokens, 1), F32),
        pltpu.VMEM((tokens, ff), BF), pltpu.VMEM((tokens, ff), BF),
        pltpu.VMEM((chans, tokens), BF), pltpu.VMEM((chans, tokens), BF),
        pltpu.VMEM((tokens, 2 * ff), BF), pltpu.VMEM((tokens, 2 * ff), BF),
        pltpu.VMEM((mix, tokens), BF), pltpu.VMEM((mix, tokens), BF),
        pltpu.VMEM((3, 8, tokens), F32), pltpu.VMEM((3, 8, tokens), F32),
        pltpu.VMEM((3, tokens, width), BF), pltpu.VMEM((3, tokens, width // 2), BF), pltpu.VMEM((3, tokens, width // 2), BF),
        pltpu.VMEM((3, tokens, width // 2), BF), pltpu.VMEM((3, tokens, width), BF),
        pltpu.SemaphoreType.DMA((6,)), pltpu.SemaphoreType.DMA((2,)), pltpu.SemaphoreType.DMA((10 + CHUNKS,)),
    ]
    half_heads = heads // 2
    for n in (3, 3, 1, 1, 1, half_heads, CHUNKS, GU_PIECES * CHUNKS, CHUNKS, 2 * CHUNKS, 4, 4 * CHUNKS, 4 * CHUNKS, 4 * CHUNKS, 4, 4 * CHUNKS,
              2 * CHUNKS, 2 * CHUNKS, 1, 1, 1, half_heads):
        scratch += [pltpu.SemaphoreType.DMA((n,))]
    vec = jax.ShapeDtypeStruct((1, width), F32)
    return pl.pallas_call(
        layer_kernel,
        name="layer",
        out_shape=(act(width), act(width), vec, vec, act(width), jax.ShapeDtypeStruct((chans, tokens), BF),
                   jax.ShapeDtypeStruct((mix, tokens), BF), act(width), act(width), act(2 * ff), act(ff)),
        in_specs=[any_spec, any_spec, vmem_spec, vmem_spec, vmem_spec, any_spec, any_spec, any_spec, any_spec],
        out_specs=(any_spec,) * 11,
        scratch_shapes=scratch,
        compiler_params=pltpu.CompilerParams(collective_id=0, has_side_effects=True, vmem_limit_bytes=67000000),
    )(x_in, grad_out, gain_one, gain_two, positions, w_qkv, w_out, w_gu, w_down)


def grads_kernel(act_hbm, dy_hbm, r2_hbm, dgu_hbm, mix_hbm, dh_hbm, dqkv_hbm, r1_hbm, y_in, dx_in, dg1_in, dg2_in,
                 down_out, gu_out, wout_out, qkv_out, y_out, dx_out, dg1_out, dg2_out,
                 act_ref, dy_ref, r2_ref, dgu_ref, mix_ref, dh_ref, dqkv_ref, r1_ref, y_ref, dx_ref, rows_ref, inter_ref,
                 load_sem, rows_sem, inter_sem, end_sem):
    block = rows_ref.shape[1]
    pad = inter_ref.shape[1] // GU_BLOCK
    ff = dgu_ref.shape[1] // 2
    pairs = [(dqkv_hbm, dqkv_ref), (r1_hbm, r1_ref), (r2_hbm, r2_ref), (dgu_hbm, dgu_ref), (mix_hbm, mix_ref), (dh_hbm, dh_ref),
             (act_hbm, act_ref), (dy_hbm, dy_ref), (y_in, y_ref), (dx_in, dx_ref)]
    loads = [pltpu.make_async_copy(src, dst, load_sem.at[n]) for n, (src, dst) in enumerate(pairs)]
    for copy in loads[:2]:
        copy.start()
    dg1_out[...] = dg1_in[...].reshape(dg1_out.shape)
    dg2_out[...] = dg2_in[...].reshape(dg2_out.shape)

    slots, inter_slots = rows_ref.shape[0], inter_ref.shape[0]

    def rows_copy(out, index, slot):
        return pltpu.make_async_copy(rows_ref.at[slot], out.at[step(index, block)], rows_sem.at[slot])

    def product(out, lhs_of, rhs_ref, first):
        def body(i, carry):
            slot = lax.rem(i + first, slots)

            @pl.when(i + first >= slots)
            def _():
                rows_copy(out, 0, slot).wait()
            rows_ref[slot] = lhs_of(i, rhs_ref)
            rows_copy(out, i, slot).start()
            return carry
        count = out.shape[0] // block
        lax.fori_loop(0, count, body, 0)
        return first + count

    def plain_rows(ref):
        return lambda i, rhs_ref: dot_nn(ref[step(i, block), :], rhs_ref[...])

    loads[0].wait()
    loads[1].wait()
    for copy in loads[2:]:
        copy.start()
    sent = product(qkv_out, plain_rows(dqkv_ref), r1_ref, 0)

    loads[2].wait()
    loads[3].wait()

    def inter_copy(index, slot):
        return pltpu.make_async_copy(inter_ref.at[slot].reshape(GU_BLOCK, pad, 128).at[:, 0:32, :],
                                     gu_out.at[step(index, GU_BLOCK)], inter_sem.at[slot])

    gu_steps = gu_out.shape[0] // GU_BLOCK

    def gu_body(i, carry):
        slot = lax.rem(i, inter_slots)

        @pl.when(i >= inter_slots)
        def _():
            inter_copy(0, slot).wait()
        lhs = r2_ref[:, step(i, GU_BLOCK)].T
        for k in range(2):
            for n in range(ff // 512):
                val = dot_nn(lhs, dgu_ref[:, k * ff + n * 512:k * ff + (n + 1) * 512])
                for t in range(4):
                    row = 2 * (4 * n + t) + k
                    inter_ref[slot, pl.ds(row, GU_BLOCK, stride=pad), :] = val[:, t * 128:(t + 1) * 128]
        inter_copy(i, slot).start()
        return carry

    lax.fori_loop(0, gu_steps, gu_body, 0)

    loads[4].wait()
    loads[5].wait()
    sent = product(wout_out, plain_rows(mix_ref), dh_ref, sent)
    loads[6].wait()
    loads[7].wait()
    sent = product(down_out, lambda i, rhs_ref: dot_tn(act_ref[:, step(i, block)], rhs_ref[...]), dy_ref, sent)
    loads[8].wait()
    loads[9].wait()
    ends = [pltpu.make_async_copy(y_ref, y_out, end_sem.at[0]), pltpu.make_async_copy(dx_ref, dx_out, end_sem.at[1])]
    for copy in ends:
        copy.start()
    for slot in range(slots):
        rows_copy(down_out, 0, slot).wait()
    for slot in range(inter_slots):
        inter_copy(0, slot).wait()
    for copy in ends:
        copy.wait()


GU_BLOCK = 128


def weight_grads(act, grad_out, r2, dgu, mix, dh, dqkv, r1, y, dx, dg1, dg2):
    tokens, width = r2.shape
    ff = act.shape[1]
    any_spec = pl.BlockSpec(memory_space=pl.ANY)
    vmem_spec = pl.BlockSpec(memory_space=pltpu.VMEM)
    out = lambda *shape: jax.ShapeDtypeStruct(shape, F32)
    like = lambda a: jax.ShapeDtypeStruct(a.shape, a.dtype)
    arrays = (act, grad_out, r2, dgu, mix, dh, dqkv, r1, y, dx)
    return pl.pallas_call(
        grads_kernel,
        name="weight_grads",
        in_specs=[any_spec] * 10 + [vmem_spec] * 2,
        out_specs=[any_spec] * 6 + [vmem_spec] * 2,
        out_shape=[out(ff, width), out(width, 32, 128), out(mix.shape[0], width), out(dqkv.shape[0], width), like(y), like(dx), out(width), out(width)],
        scratch_shapes=[pltpu.VMEM(a.shape, a.dtype) for a in arrays] + [
            pltpu.VMEM((8, 256, width), F32), pltpu.VMEM((6, GU_BLOCK * 40, 128), F32),
            pltpu.SemaphoreType.DMA((10,)), pltpu.SemaphoreType.DMA((8,)), pltpu.SemaphoreType.DMA((6,)), pltpu.SemaphoreType.DMA((2,))],
        compiler_params=pltpu.CompilerParams(vmem_limit_bytes=56 << 20),
    )(*arrays, dg1, dg2)


def solution(mesh):
    def per_device(x_in, positions, gain_one, gain_two, w_qkv, w_out, w_gu, w_down, grad_out):
        width, groups, chans = w_qkv.shape
        ff = w_down.shape[0]
        qkv_rows = w_qkv.transpose(1, 2, 0).reshape(groups * chans, width)
        gu_rows = w_gu.reshape(width, 2, ff // 128, 128).transpose(0, 2, 1, 3).reshape(width * 2 * (ff // 128), 128)
        y, dx, dg1, dg2, r1, dqkv, mix, dh, r2, dgu, act = run_layer(
            x_in, positions, gain_one, gain_two, qkv_rows, w_out, gu_rows, w_down, grad_out)
        d_down, d_gu, d_out, d_qkv, y, dx, dg1, dg2 = weight_grads(act, grad_out, r2, dgu, mix, dh, dqkv, r1, y, dx, dg1, dg2)
        d_gu = d_gu.reshape(width, ff // 128, 2, 128).transpose(0, 2, 1, 3).reshape(width, 2, ff)
        d_qkv = d_qkv.reshape(groups, chans, width).transpose(2, 0, 1)
        return y, dx, dg1, dg2, d_qkv, d_out, d_gu, d_down

    act_spec = P('dp', 'embed')
    in_specs = (act_spec, P('dp'), P('embed'), P('embed'), P('embed', 'heads', None), P('heads', 'embed'), P('embed', None, 'heads'), P('heads', 'embed'), act_spec)
    out_specs = (act_spec, act_spec, P(('dp', 'embed')), P(('dp', 'embed')), P(('dp', 'embed'), 'heads', None), P(('dp', 'heads'), 'embed'), P(('dp', 'embed'), None, 'heads'), P(('dp', 'heads'), 'embed'))
    return jax.shard_map(per_device, mesh=mesh, in_specs=in_specs, out_specs=out_specs, check_vma=False)
```

```python
import math

import jax
import jax.numpy as jnp
from jax import lax
from jax.experimental import pallas as pl
from jax.experimental.pallas import tpu as pltpu
from jax.sharding import PartitionSpec as P

EPSILON = 1e-5
ROPE_BASE = 10000.0
HEAD = 96
HALF = HEAD // 2
GROUP = 3 * HEAD
CHUNKS = 2
MESH = pl.DeviceIdType.MESH
BF = jnp.bfloat16
F32 = jnp.float32

AR_OUT, AR_R2, AR_Y, AR_R1 = range(4)
SLOT = (0, 1, 2, 0)
GU_PIECES = 4
EARLY, LATE = 0, 1


def dot_nn(lhs, rhs):
    return lax.dot_general(lhs, rhs, (((1,), (0,)), ((), ())), preferred_element_type=F32)


def dot_nt(lhs, rhs):
    return lax.dot_general(lhs, rhs, (((1,), (1,)), ((), ())), preferred_element_type=F32)


def dot_tn(lhs, rhs):
    return lax.dot_general(lhs, rhs, (((0,), (0,)), ((), ())), preferred_element_type=F32)


def add_bf(one, two):
    return (one.astype(F32) + two.astype(F32)).astype(BF)


def step(index, size):
    return pl.ds(pl.multiple_of(index * size, size), size)


def layer_kernel(x_hbm, dy_hbm, g1_in, g2_in, pos_in, wqkv_hbm, wout_hbm, wgu_hbm, wdown_hbm,
                 y_hbm, dx_hbm, dg1_hbm, dg2_hbm, r1_hbm, dqkv_hbm, mix_hbm, dh_hbm, r2_hbm, dgu_hbm, act_hbm,
                 x_ref, dy_ref, wqkv_ref, wout_ref, wg_ref, wu_ref, wdown_ref, raw_ref,
                 g1_ref, g2_ref, cos_ref, sin_ref, r1_ref, r2_ref, h_ref, dh_ref, act_ref, dgu_ref, rot_ref, late_ref, early_ref, mix_ref, dqkv_ref, dx_ref,
                 kv_part, cot_ref, dots_ref, dg1_ref, dg2_ref,
                 inv1_ref, inv2_ref,
                 ga_send, ga_recv, qkv_send, qkv_recv, gu_send, gu_recv, gm_send, gm_recv, stat_send, stat_recv,
                 part_ref, sib_ref, half_ref, far_ref, full_ref,
                 load_sem, raw_sem, store_sem,
                 st_s, st_r, ga_s, ga_r, qk_s, qk_r, gu_s, gu_r, gm_s, gm_r, p1_s, p1_r, p2_s, p2_r, p3_s, p3_r, dots_s, dots_r, mx_s, mx_r, rt_s, rt_r):
    tokens, width = x_ref.shape
    full_width = 2 * width
    ff = wdown_ref.shape[0]
    heads = wqkv_ref.shape[0] // GROUP
    half_width = width // 2
    rows = tokens // CHUNKS
    emb = lax.axis_index("embed")
    hid = lax.axis_index("heads")
    core = lax.rem(hid, 2)
    sibling = {"heads": hid + 1 - 2 * core}
    across = {"heads": lax.rem(hid + 2, 4)}
    partner = {"embed": 1 - emb}

    barrier = pltpu.get_barrier_semaphore()
    others = [{"embed": lax.rem(emb + n // 4, 2), "heads": lax.rem(hid + n, 4)} for n in range(1, 8)]
    for peer in others:
        pl.semaphore_signal(barrier, inc=1, device_id=peer, device_id_type=MESH)

    def load(src, dst, sem):
        return pltpu.make_async_copy(src, dst, load_sem.at[sem])

    first, rest = pl.ds(0, ff // 8), pl.ds(ff // 8, ff - ff // 8)
    loads = [load(x_hbm, x_ref, 0), load(dy_hbm, dy_ref, 1), load(wdown_hbm.at[first], wdown_ref.at[first], 2),
             load(wqkv_hbm, wqkv_ref, 3), load(wout_hbm, wout_ref, 4), load(wdown_hbm.at[rest], wdown_ref.at[rest], 5)]
    for copy in loads[:4]:
        copy.start()

    raw_rows = raw_ref.shape[1]
    raw_steps = wgu_hbm.shape[0] // raw_rows

    def raw_load(index, slot):
        return pltpu.make_async_copy(wgu_hbm.at[step(index, raw_rows)], raw_ref.at[slot], raw_sem.at[slot])

    def store(src, dst, sem):
        copy = pltpu.make_async_copy(src, dst, store_sem.at[sem])
        copy.start()
        return copy

    def send(src, dst, s_sem, r_sem, peer):
        return pltpu.make_async_remote_copy(src_ref=src, dst_ref=dst, send_sem=s_sem, recv_sem=r_sem,
                                            device_id=peer, device_id_type=MESH)

    def stat_copy(k):
        return send(stat_send.at[k], stat_recv.at[k], st_s.at[k], st_r.at[k], partner)

    ga_cols = ff // 8

    def ga_copy(k):
        cols = step(k, ga_cols)
        return send(ga_send.at[:, cols], ga_recv.at[:, cols], ga_s.at[0], ga_r.at[0], partner)

    ga_all = send(ga_send, ga_recv, ga_s.at[0], ga_r.at[0], partner)

    def qkv_copy(i, j):
        r = step(j, GROUP)
        return send(qkv_send.at[r], qkv_recv.at[r], qk_s.at[0], qk_r.at[i], partner)

    half_heads = heads // 2
    half_chans = half_heads * GROUP

    def mine(i):
        return emb * half_heads + i

    def theirs(i):
        return (1 - emb) * half_heads + i

    def mix_rows(j):
        return pl.ds(pl.multiple_of(j * HEAD, 32), HEAD)

    def mix_copy(j):
        at = mix_ref.at[mix_rows(j)]
        return send(at, at, mx_s.at[0], mx_r.at[0], partner)

    def mix_all(which):
        at = mix_ref.at[step(which, half_heads * HEAD)]
        return send(at, at, mx_s.at[0], mx_r.at[0], partner)

    def rot_copy(i, j):
        at = rot_ref.at[step(j, GROUP)]
        return send(at, at, rt_s.at[0], rt_r.at[i], partner)

    gu_cols = ff // GU_PIECES

    def gu_copy(c, q, k):
        at = (pl.ds(c * rows, rows), pl.ds(pl.multiple_of(k * ff + q * gu_cols, gu_cols), gu_cols))
        return send(gu_send.at[at], gu_recv.at[at], gu_s.at[c], gu_r.at[c * GU_PIECES + q], partner)

    def gu_pair(c, q):
        at = (pl.ds(c * rows, rows), pl.ds(0, 2 * gu_cols))
        return send(gu_send.at[at], gu_recv.at[at], gu_s.at[c], gu_r.at[c * GU_PIECES + q], partner)

    def gu_sent(c):
        at = pl.ds(c * rows, rows)
        send(gu_send.at[at], gu_recv.at[at], gu_s.at[c], gu_r.at[0], partner).wait_send()

    gm_rows = gm_send.shape[0] // 2

    def gm_copy(c, hf):
        at = (step(hf, gm_rows), pl.ds(c * rows, rows))
        return send(gm_send.at[at], gm_recv.at[at], gm_s.at[c], gm_r.at[2 * c + hf], partner)

    own = pl.ds(pl.multiple_of(core * half_width, half_width), half_width)
    other = pl.ds(pl.multiple_of((1 - core) * half_width, half_width), half_width)

    def p1_copy(i, c):
        r = pl.ds(c * rows, rows)
        k = i * CHUNKS + c
        return send(part_ref.at[SLOT[i], r, other], sib_ref.at[SLOT[i], r], p1_s.at[i], p1_r.at[k], sibling)

    def p2_copy(i, c):
        r = pl.ds(c * rows, rows)
        k = i * CHUNKS + c
        return send(half_ref.at[SLOT[i], r], far_ref.at[SLOT[i], r], p2_s.at[k], p2_r.at[k], across)

    def p3_copy(i, c):
        r = pl.ds(c * rows, rows)
        k = i * CHUNKS + c
        return send(full_ref.at[SLOT[i], r, own], full_ref.at[SLOT[i], r, own], p3_s.at[i], p3_r.at[k], sibling)

    def p1_p3_sent(i):
        n = SLOT[i]
        send(part_ref.at[n, :, other], sib_ref.at[n], p1_s.at[i], p1_r.at[0], sibling).wait_send()
        send(full_ref.at[n, :, own], full_ref.at[n, :, own], p3_s.at[i], p3_r.at[0], sibling).wait_send()

    def stage2(i, c):
        r = pl.ds(c * rows, rows)
        p1_copy(i, c).wait_recv()
        half_ref[SLOT[i], r, :] = add_bf(part_ref[SLOT[i], r, own], sib_ref[SLOT[i], r, :])
        p2_copy(i, c).start()

    def stage3(i, c):
        r = pl.ds(c * rows, rows)
        p2_copy(i, c).wait_recv()
        full_ref[SLOT[i], r, own] = add_bf(half_ref[SLOT[i], r, :], far_ref[SLOT[i], r, :])
        p3_copy(i, c).start()

    def stage4(i, c):
        p3_copy(i, c).wait_recv()

    def stat_put(k, col, n):
        flat = jnp.broadcast_to(col, (n, 128)).T[0:8, :]
        stat_send[k, :, 0:n] = flat
        stat_copy(k).start()

    def stat_get(k, n):
        stat_copy(k).wait_recv()
        total = stat_send[k, 0:1, 0:n] + stat_recv[k, 0:1, 0:n]
        return jnp.broadcast_to(total, (128, n)).T[:, 0:1]

    me = emb * 4 + hid

    def dots_copy(k, n):
        at = dots_ref.at[k, me]
        return send(at, at, dots_s.at[k], dots_r.at[k], others[n])

    def dots_all(k):
        at = dots_ref.at[k, pl.ds(0, 7)]
        return send(at, at, dots_s.at[k], dots_r.at[k], partner)

    def dots_put(k, col):
        dots_ref[k, me] = jnp.broadcast_to(col, (rows, 128)).T[0:8, :]
        for n in range(7):
            dots_copy(k, n).start()

    def dots_get(k):
        dots_all(k).wait_recv()
        total = dots_ref[k, 0, 0:1, :]
        for n in range(1, 8):
            total = total + dots_ref[k, n, 0:1, :]
        return jnp.broadcast_to(total, (128, rows)).T[:, 0:1]

    def ga_body(k, carry):
        cols = step(k, ga_cols)
        ga_send[:, cols] = dot_nt(dy_ref[...], wdown_ref[cols, :]).astype(BF)
        return carry

    loads[0].wait()
    x32 = x_ref[...].astype(F32)
    sq1 = jnp.sum(x32 * x32, axis=-1, keepdims=True)
    loads[1].wait()
    loads[2].wait()
    ga_body(0, 0)
    pl.semaphore_wait(barrier, 7)
    stat_put(0, sq1, tokens)
    ga_copy(0).start()
    for copy in loads[4:]:
        copy.start()
    for slot in range(2):
        raw_load(slot, slot).start()
    g1_ref[...] = g1_in[...].reshape(1, width)
    g2_ref[...] = g2_in[...].reshape(1, width)
    place = pos_in[...].reshape(1, tokens).astype(F32)
    pair_i = lax.broadcasted_iota(jnp.int32, (HALF, 1), 0).astype(F32)
    angles = jnp.exp(pair_i * (-2.0 * math.log(ROPE_BASE) / HEAD)) * place
    cos_ref[...] = jnp.cos(angles)
    sin_ref[...] = jnp.sin(angles)
    inv1 = lax.rsqrt(stat_get(0, tokens) / full_width + EPSILON)
    inv1_ref[...] = inv1
    r1_ref[...] = (x_ref[...].astype(F32) * inv1 * g1_ref[...]).astype(BF)
    stores = [store(r1_ref, r1_hbm, 0)]

    loads[3].wait()

    def qkv_product(j):
        r = step(j, GROUP)
        qkv_send[r, :] = dot_nt(wqkv_ref[r, :], r1_ref[...]).astype(BF)

    def qkv_theirs(i, carry):
        qkv_product(theirs(i))
        qkv_copy(i, theirs(i)).start()
        return carry

    def qkv_mine(i, carry):
        qkv_product(mine(i))
        return carry

    lax.fori_loop(0, half_heads, qkv_theirs, 0)
    lax.fori_loop(0, half_heads, qkv_mine, 0)
    loads[5].wait()
    lax.fori_loop(1, 8, ga_body, 0)

    row_i = lax.broadcasted_iota(jnp.int32, (256, 256), 0)
    col_i = lax.broadcasted_iota(jnp.int32, (256, 256), 1)
    perm = (col_i == (row_i % 8) * 32 + row_i // 8).astype(F32).astype(BF)
    blocks = raw_rows // 512

    def raw_body(i, carry):
        slot = lax.rem(i, 2)
        raw_load(i, slot).wait()

        def block_body(b, inner):
            for u in range(4):
                base = pl.multiple_of(b * 2048 + u * 512, 512)
                pair = jnp.concatenate([raw_ref[slot, pl.ds(base, 256), :], raw_ref[slot, pl.ds(base + 256, 256), :]], axis=1)
                out = dot_nn(perm, pair)
                d = pl.ds(pl.multiple_of(i * (raw_rows // 32) + b * 64 + u * 16, 16), 16)
                for t in range(16):
                    for k, dst in ((0, wg_ref), (1, wu_ref)):
                        r = (2 * t + k) * 8
                        both = jnp.concatenate([out[r:r + 8, 0:128], out[r:r + 8, 128:256]], axis=0)
                        dst[d, t * 128:(t + 1) * 128] = both.astype(BF)
            return inner

        lax.fori_loop(0, blocks // 4, block_body, 0)

        @pl.when(i + 2 < raw_steps)
        def _():
            raw_load(i + 2, slot).start()
        return carry

    part_one, part_two = raw_steps // 2, raw_steps - raw_steps // 3
    lax.fori_loop(0, part_one, raw_body, 0)

    scale = HEAD ** -0.5
    causal = (lax.broadcasted_iota(jnp.int32, (tokens, tokens), 0) <= lax.broadcasted_iota(jnp.int32, (tokens, tokens), 1))

    def rope(v, cos_t, sin_t):
        v = v.astype(F32)
        one, two = v[0:HALF], v[HALF:HEAD]
        return jnp.concatenate([one * cos_t - two * sin_t, two * cos_t + one * sin_t], axis=0).astype(BF)

    def unrope(v, cos_t, sin_t):
        v = v.astype(F32)
        one, two = v[0:HALF], v[HALF:HEAD]
        return jnp.concatenate([one * cos_t + two * sin_t, two * cos_t - one * sin_t], axis=0).astype(BF)

    last = half_heads - 1

    def head_rows(j):
        base = pl.multiple_of(j * GROUP, 32)
        return tuple(pl.ds(base + n * HEAD, HEAD) for n in range(3))

    def probabilities(j, q, k):
        scores = jnp.where(causal, dot_tn(k, q) * scale, -1e30)
        weight = jnp.exp(scores - jnp.max(scores, axis=0, keepdims=True))
        prob = weight / jnp.sum(weight, axis=0, keepdims=True)
        late_ref[j] = prob[:, rows:]
        early_ref[j] = prob[0:rows, 0:rows]
        return prob

    def attn_body(i, carry):
        j = mine(i)

        @pl.when(i == last)
        def _():
            r = step(1 - emb, half_chans)
            send(qkv_send.at[r], qkv_recv.at[r], qk_s.at[0], qk_r.at[0], partner).wait_send()
            ga_copy(1).start()
        qkv_copy(i, j).wait_recv()
        r_q, r_k, r_v = head_rows(j)
        cos_t, sin_t = cos_ref[...], sin_ref[...]
        q = rope(add_bf(qkv_send[r_q, :], qkv_recv[r_q, :]), cos_t, sin_t)
        k = rope(add_bf(qkv_send[r_k, :], qkv_recv[r_k, :]), cos_t, sin_t)
        v = add_bf(qkv_send[r_v, :], qkv_recv[r_v, :])
        rot_ref[r_q, :] = q
        rot_ref[r_k, :] = k
        rot_ref[r_v, :] = v
        prob = probabilities(j, q, k)
        mix_ref[mix_rows(j), :] = dot_nn(v, prob.astype(BF)).astype(BF)
        mix_copy(j).start()
        return carry

    lax.fori_loop(0, half_heads, attn_body, 0)
    for n in range(2, 6):
        ga_copy(n).start()
    lax.fori_loop(part_one, part_two, raw_body, 0)
    mix_all(1 - emb).wait_recv()
    stores.append(store(mix_ref, mix_hbm, 1))

    loads[4].wait()
    order = tuple(reversed(range(CHUNKS)))
    for c in order:
        r = pl.ds(c * rows, rows)
        part_ref[SLOT[AR_OUT], r, :] = dot_tn(mix_ref[:, c * rows:(c + 1) * rows], wout_ref[...]).astype(BF)
        p1_copy(AR_OUT, c).start()
    def gu_start(c, q):
        for k in range(2):
            gu_copy(c, q, k).start()

    def hidden_fwd(c):
        r = pl.ds(c * rows, rows)
        stage4(AR_OUT, c)
        h = add_bf(x_ref[r, :], full_ref[SLOT[AR_OUT], r, :])
        h_ref[r, :] = h
        h32 = h.astype(F32)
        stat_put(1 + c, jnp.sum(h32 * h32, axis=-1, keepdims=True), rows)

    def gate_up(c, at_once):
        r = pl.ds(c * rows, rows)
        inv2 = lax.rsqrt(stat_get(1 + c, rows) / full_width + EPSILON)
        inv2_ref[r, :] = inv2
        r2_ref[r, :] = (h_ref[r, :].astype(F32) * inv2 * g2_ref[...]).astype(BF)

        def gu_body(q, carry):
            for k, w_ref in ((0, wg_ref), (1, wu_ref)):
                dst = pl.ds(pl.multiple_of(k * ff + q * gu_cols, gu_cols), gu_cols)
                gu_send[r, dst] = dot_nn(r2_ref[r, :], w_ref[:, step(q, gu_cols)]).astype(BF)

            @pl.when(q < at_once)
            def _():
                gu_start(c, q)
            return carry

        lax.fori_loop(0, GU_PIECES, gu_body, 0)

    stage2(AR_OUT, LATE)
    lax.fori_loop(part_two, raw_steps, raw_body, 0)
    p2_copy(AR_OUT, LATE).wait_send()
    stage2(AR_OUT, EARLY)
    stage3(AR_OUT, LATE)
    hidden_fwd(LATE)
    for k in range(6, 8):
        ga_copy(k).start()
    gate_up(LATE, 2)
    stage3(AR_OUT, EARLY)
    hidden_fwd(EARLY)
    gu_start(LATE, 2)
    gu_start(LATE, 3)
    gate_up(EARLY, 0)
    tile = 512
    stores.append(store(r2_ref, r2_hbm, 2))

    ga_all.wait_recv()
    p1_p3_sent(AR_OUT)
    p2_copy(AR_OUT, EARLY).wait_send()

    def mlp_pieces(c, lo, hi):
        r = pl.ds(c * rows, rows)
        if lo == 0:
            cot_ref[...] = jnp.zeros_like(cot_ref)

        def piece(q, carry):
            if c == EARLY:
                @pl.when(q == GU_PIECES - 1)
                def _():
                    gu_sent(EARLY)
                    for i in range(2):
                        rot_copy(i, mine(i)).start()
            gu_pair(c, q).wait_recv()
            if c == LATE:
                @pl.when(q == 2)
                def _():
                    gu_start(EARLY, 0)
            for n in range(gu_cols // 256):
                cg = pl.ds(pl.multiple_of(q * gu_cols + n * 256, 256), 256)
                cu = pl.ds(pl.multiple_of(ff + q * gu_cols + n * 256, 256), 256)
                gate = add_bf(gu_send[r, cg], gu_recv[r, cg]).astype(F32)
                up = add_bf(gu_send[r, cu], gu_recv[r, cu]).astype(F32)
                ga = add_bf(ga_send[r, cg], ga_recv[r, cg]).astype(F32)
                sig = 1.0 / (1.0 + jnp.exp(-gate))
                silu = gate * sig
                act_ref[r, cg] = (silu * up).astype(BF)
                dgu_ref[r, cg] = (ga * up * (sig * (1.0 + gate * (1.0 - sig)))).astype(BF)
                dgu_ref[r, cu] = (ga * silu).astype(BF)
            at_g = step(q, gu_cols)
            at_u = pl.ds(pl.multiple_of(ff + q * gu_cols, gu_cols), gu_cols)
            for n in range(width // tile):
                w = slice(n * tile, (n + 1) * tile)
                cot_ref[:, w] += dot_nt(dgu_ref[r, at_g], wg_ref[w, at_g]) + dot_nt(dgu_ref[r, at_u], wu_ref[w, at_g])
            return carry

        lax.fori_loop(lo, hi, piece, 0)

    def mlp_end(c):
        r = pl.ds(c * rows, rows)
        part_ref[SLOT[AR_R2], r, :] = cot_ref[...].astype(BF)
        p1_copy(AR_R2, c).start()
        unit = h_ref[r, :].astype(F32) * inv2_ref[r, :]
        dots_put(c, jnp.sum(cot_ref[...] * g2_ref[...] * unit, axis=-1, keepdims=True))

    def down_chunk(c):
        r = pl.ds(c * rows, rows)

        def down_body(n, carry):
            w = step(n, tile)
            part_ref[SLOT[AR_Y], r, w] = dot_nn(act_ref[r, :], wdown_ref[:, w]).astype(BF)
            return carry

        lax.fori_loop(0, width // tile, down_body, 0)
        p1_copy(AR_Y, c).start()

    dg1_ref[...] = jnp.zeros_like(dg1_ref)
    dg2_ref[...] = jnp.zeros_like(dg2_ref)

    def hidden_back(c, then=lambda: None):
        r = pl.ds(c * rows, rows)
        dots = dots_get(c)
        stage4(AR_R2, c)
        inv2 = inv2_ref[r, :]
        unit = h_ref[r, :].astype(F32) * inv2
        gin = full_ref[SLOT[AR_R2], r, :].astype(F32)
        norm = inv2 * (gin * g2_ref[...] - unit * (dots / full_width))
        dh_ref[r, :] = (dy_ref[r, :].astype(F32) + norm).astype(BF)
        gm_send[:, c * rows:(c + 1) * rows] = dot_nt(wout_ref[...], dh_ref[r, :]).astype(BF)
        for hf in range(2):
            gm_copy(c, hf).start()
        then()
        dg2_ref[...] += jnp.sum(gin * unit, axis=0, keepdims=True)

    def y_chunk(c):
        r = pl.ds(c * rows, rows)
        stage4(AR_Y, c)
        h_ref[r, :] = add_bf(h_ref[r, :], full_ref[SLOT[AR_Y], r, :])

    def scores_back(v, da, prob):
        dp = dot_tn(v, da).astype(BF).astype(F32)
        weighted = prob * dp
        return ((weighted - prob * jnp.sum(weighted, axis=0, keepdims=True)) * scale).astype(BF)

    def write(stored):
        for ref, at, value in stored:
            ref[at] = value

    def late_heads(js):
        stored = []
        cos_t, sin_t = cos_ref[:, rows:], sin_ref[:, rows:]
        late, early = slice(rows, None), slice(0, rows)
        for j in js:
            r_q, r_k, r_v = head_rows(j)
            r_a = mix_rows(j)
            da = add_bf(gm_send[r_a, late], gm_recv[r_a, late])
            prob = late_ref[j]
            k = rot_ref[r_k, :]
            ds = scores_back(rot_ref[r_v, :], da, prob)
            dv = dot_nt(da, prob.astype(BF))
            dk = dot_nt(rot_ref[r_q, late], ds)
            stored += [(dqkv_ref, (r_q, late), unrope(dot_nn(k, ds).astype(BF), cos_t, sin_t)),
                       (dqkv_ref, (r_k, late), unrope(dk[:, late].astype(BF), cos_t, sin_t)),
                       (dqkv_ref, (r_v, late), dv[:, late].astype(BF)),
                       (kv_part, (0, r_a), dk[:, early]), (kv_part, (1, r_a), dv[:, early])]
        write(stored)

    def late_mine(i, carry):
        late_heads((mine(2 * i), mine(2 * i + 1)))
        return carry

    def late_theirs(i, carry):
        j = theirs(i)
        rot_copy(i, j).wait_recv()
        r_q, r_k, _ = head_rows(j)
        probabilities(j, rot_ref[r_q, :], rot_ref[r_k, :])
        late_heads((j,))
        return carry

    def early_heads(js):
        stored = []
        early = slice(0, rows)
        cos_t, sin_t = cos_ref[:, early], sin_ref[:, early]
        for j in js:
            r_q, r_k, r_v = head_rows(j)
            r_a = mix_rows(j)
            da = add_bf(gm_send[r_a, early], gm_recv[r_a, early])
            prob = early_ref[j]
            ds = scores_back(rot_ref[r_v, early], da, prob)
            dv = kv_part[1, r_a, :] + dot_nt(da, prob.astype(BF))
            dk = kv_part[0, r_a, :] + dot_nt(rot_ref[r_q, early], ds)
            stored += [(dqkv_ref, (r_q, early), unrope(dot_nn(rot_ref[r_k, early], ds).astype(BF), cos_t, sin_t)),
                       (dqkv_ref, (r_k, early), unrope(dk.astype(BF), cos_t, sin_t)),
                       (dqkv_ref, (r_v, early), dv.astype(BF))]
        write(stored)

    def cot_product(c, lo, hi):
        return dot_tn(dqkv_ref[lo:hi, c * rows:(c + 1) * rows], wqkv_ref[lo:hi, :])

    def input_cot(c):
        r = pl.ds(c * rows, rows)
        cot = cot_product(c, half_chans, None) + (cot_ref[...] if c == EARLY else cot_product(c, 0, half_chans))
        part_ref[SLOT[AR_R1], r, :] = cot.astype(BF)
        p1_copy(AR_R1, c).start()
        unit = x_ref[r, :].astype(F32) * inv1_ref[r, :]
        dots_put(CHUNKS + c, jnp.sum(cot * g1_ref[...] * unit, axis=-1, keepdims=True))

    def input_back(c):
        r = pl.ds(c * rows, rows)
        dots = dots_get(CHUNKS + c)
        stage4(AR_R1, c)
        inv1 = inv1_ref[r, :]
        unit = x_ref[r, :].astype(F32) * inv1
        gin = full_ref[SLOT[AR_R1], r, :].astype(F32)
        norm = inv1 * (gin * g1_ref[...] - unit * (dots / full_width))
        dx_ref[r, :] = (dh_ref[r, :].astype(F32) + norm).astype(BF)
        stores.append(store(dx_ref.at[r], dx_hbm.at[r], 8 + c))
        dg1_ref[...] += jnp.sum(gin * unit, axis=0, keepdims=True)

    def rest_of_gate_up():
        gu_start(EARLY, 3)

    mlp_pieces(LATE, 0, GU_PIECES)
    mlp_end(LATE)
    gu_start(EARLY, 1)
    stage2(AR_R2, LATE)
    down_chunk(LATE)
    stage3(AR_R2, LATE)
    stage2(AR_Y, LATE)
    gu_start(EARLY, 2)
    hidden_back(LATE, rest_of_gate_up)
    mlp_pieces(EARLY, 0, 2)
    stage3(AR_Y, LATE)
    gm_copy(LATE, emb).wait_recv()
    lax.fori_loop(0, half_heads // 2, late_mine, 0)
    y_chunk(LATE)
    mlp_pieces(EARLY, 2, GU_PIECES)
    mlp_end(EARLY)
    for i in range(2, half_heads):
        rot_copy(i, mine(i)).start()
    stores.append(store(dgu_ref, dgu_hbm, 3))
    stores.append(store(act_ref, act_hbm, 4))
    stage2(AR_R2, EARLY)
    down_chunk(EARLY)
    gm_copy(LATE, 1 - emb).wait_recv()
    lax.fori_loop(0, 2, late_theirs, 0)
    stage3(AR_R2, EARLY)
    stage2(AR_Y, EARLY)
    hidden_back(EARLY)
    stores.append(store(dh_ref, dh_hbm, 5))
    stores.append(store(dg2_ref, dg2_hbm, 6))
    lax.fori_loop(2, half_heads, late_theirs, 0)
    input_cot(LATE)
    gm_copy(EARLY, 0).wait_recv()
    stage2(AR_R1, LATE)
    early_heads(range(half_heads))
    cot_ref[...] = cot_product(EARLY, 0, half_chans)
    gm_copy(EARLY, 1).wait_recv()
    early_heads(range(half_heads, heads))
    input_cot(EARLY)
    stores.append(store(dqkv_ref, dqkv_hbm, 7))
    stage2(AR_R1, EARLY)
    stage3(AR_R1, LATE)
    stage3(AR_Y, EARLY)
    input_back(LATE)
    y_chunk(EARLY)
    stores.append(store(h_ref, y_hbm, 10))
    stage3(AR_R1, EARLY)
    input_back(EARLY)
    stores.append(store(dg1_ref, dg1_hbm, 11))

    for k in range(3):
        stat_copy(k).wait_send()
    for k in range(2 * CHUNKS):
        dots_all(k).wait_send()
    ga_all.wait_send()
    mix_all(emb).wait_send()
    at = rot_ref.at[step(emb, half_chans)]
    send(at, at, rt_s.at[0], rt_r.at[0], partner).wait_send()
    for c in range(CHUNKS):
        at = (slice(None), pl.ds(c * rows, rows))
        send(gm_send.at[at], gm_recv.at[at], gm_s.at[c], gm_r.at[0], partner).wait_send()
        for i in (AR_R2, AR_Y, AR_R1):
            p2_copy(i, c).wait_send()
    gu_sent(LATE)
    for i in (AR_R2, AR_Y, AR_R1):
        p1_p3_sent(i)
    for copy in stores:
        copy.wait()


def run_layer(x_in, positions, gain_one, gain_two, w_qkv, w_out, w_gu, w_down, grad_out):
    tokens, width = x_in.shape
    ff = w_down.shape[0]
    chans = w_qkv.shape[0]
    mix = w_out.shape[0]
    heads = mix // HEAD
    rows = tokens // CHUNKS
    act = lambda n, dtype=BF: jax.ShapeDtypeStruct((tokens, n), dtype)
    any_spec = pl.BlockSpec(memory_space=pl.ANY)
    vmem_spec = pl.BlockSpec(memory_space=pltpu.VMEM)
    raw_rows = 128 * 32
    scratch = [
        pltpu.VMEM((tokens, width), BF), pltpu.VMEM((tokens, width), BF),
        pltpu.VMEM((chans, width), BF), pltpu.VMEM((mix, width), BF),
        pltpu.VMEM((width, ff), BF), pltpu.VMEM((width, ff), BF), pltpu.VMEM((ff, width), BF),
        pltpu.VMEM((2, raw_rows, 128), BF),
        pltpu.VMEM((1, width), F32), pltpu.VMEM((1, width), F32), pltpu.VMEM((HALF, tokens), F32), pltpu.VMEM((HALF, tokens), F32),
        pltpu.VMEM((tokens, width), BF), pltpu.VMEM((tokens, width), BF), pltpu.VMEM((tokens, width), BF), pltpu.VMEM((tokens, width), BF),
        pltpu.VMEM((tokens, ff), BF), pltpu.VMEM((tokens, 2 * ff), BF),
        pltpu.VMEM((chans, tokens), BF), pltpu.VMEM((heads, tokens, rows), F32), pltpu.VMEM((heads, rows, rows), F32), pltpu.VMEM((mix, tokens), BF), pltpu.VMEM((chans, tokens), BF),
        pltpu.VMEM((tokens, width), BF),
        pltpu.VMEM((2, mix, rows), F32), pltpu.VMEM((rows, width), F32), pltpu.VMEM((2 * CHUNKS, 8, 8, rows), F32), pltpu.VMEM((1, width), F32), pltpu.VMEM((1, width), F32),
        pltpu.VMEM((tokens, 1), F32), pltpu.VMEM((tokens, 1), F32),
        pltpu.VMEM((tokens, ff), BF), pltpu.VMEM((tokens, ff), BF),
        pltpu.VMEM((chans, tokens), BF), pltpu.VMEM((chans, tokens), BF),
        pltpu.VMEM((tokens, 2 * ff), BF), pltpu.VMEM((tokens, 2 * ff), BF),
        pltpu.VMEM((mix, tokens), BF), pltpu.VMEM((mix, tokens), BF),
        pltpu.VMEM((3, 8, tokens), F32), pltpu.VMEM((3, 8, tokens), F32),
        pltpu.VMEM((3, tokens, width), BF), pltpu.VMEM((3, tokens, width // 2), BF), pltpu.VMEM((3, tokens, width // 2), BF),
        pltpu.VMEM((3, tokens, width // 2), BF), pltpu.VMEM((3, tokens, width), BF),
        pltpu.SemaphoreType.DMA((6,)), pltpu.SemaphoreType.DMA((2,)), pltpu.SemaphoreType.DMA((10 + CHUNKS,)),
    ]
    half_heads = heads // 2
    for n in (3, 3, 1, 1, 1, half_heads, CHUNKS, GU_PIECES * CHUNKS, CHUNKS, 2 * CHUNKS, 4, 4 * CHUNKS, 4 * CHUNKS, 4 * CHUNKS, 4, 4 * CHUNKS,
              2 * CHUNKS, 2 * CHUNKS, 1, 1, 1, half_heads):
        scratch += [pltpu.SemaphoreType.DMA((n,))]
    vec = jax.ShapeDtypeStruct((1, width), F32)
    return pl.pallas_call(
        layer_kernel,
        name="layer",
        out_shape=(act(width), act(width), vec, vec, act(width), jax.ShapeDtypeStruct((chans, tokens), BF),
                   jax.ShapeDtypeStruct((mix, tokens), BF), act(width), act(width), act(2 * ff), act(ff)),
        in_specs=[any_spec, any_spec, vmem_spec, vmem_spec, vmem_spec, any_spec, any_spec, any_spec, any_spec],
        out_specs=(any_spec,) * 11,
        scratch_shapes=scratch,
        compiler_params=pltpu.CompilerParams(collective_id=0, has_side_effects=True, vmem_limit_bytes=67000000),
    )(x_in, grad_out, gain_one, gain_two, positions, w_qkv, w_out, w_gu, w_down)


def grads_kernel(act_hbm, dy_hbm, r2_hbm, dgu_hbm, mix_hbm, dh_hbm, dqkv_hbm, r1_hbm, y_in, dx_in, dg1_in, dg2_in,
                 down_out, gu_out, wout_out, qkv_out, y_out, dx_out, dg1_out, dg2_out,
                 act_ref, dy_ref, r2_ref, dgu_ref, mix_ref, dh_ref, dqkv_ref, r1_ref, y_ref, dx_ref, rows_ref, inter_ref,
                 load_sem, rows_sem, inter_sem, end_sem):
    block = rows_ref.shape[1]
    pad = inter_ref.shape[1] // GU_BLOCK
    ff = dgu_ref.shape[1] // 2
    pairs = [(dqkv_hbm, dqkv_ref), (r1_hbm, r1_ref), (r2_hbm, r2_ref), (dgu_hbm, dgu_ref), (mix_hbm, mix_ref), (dh_hbm, dh_ref),
             (act_hbm, act_ref), (dy_hbm, dy_ref), (y_in, y_ref), (dx_in, dx_ref)]
    loads = [pltpu.make_async_copy(src, dst, load_sem.at[n]) for n, (src, dst) in enumerate(pairs)]
    for copy in loads[:2]:
        copy.start()
    dg1_out[...] = dg1_in[...].reshape(dg1_out.shape)
    dg2_out[...] = dg2_in[...].reshape(dg2_out.shape)

    slots, inter_slots = rows_ref.shape[0], inter_ref.shape[0]

    def rows_copy(out, index, slot):
        return pltpu.make_async_copy(rows_ref.at[slot], out.at[step(index, block)], rows_sem.at[slot])

    def product(out, lhs_of, rhs_ref, first):
        def body(i, carry):
            slot = lax.rem(i + first, slots)

            @pl.when(i + first >= slots)
            def _():
                rows_copy(out, 0, slot).wait()
            rows_ref[slot] = lhs_of(i, rhs_ref)
            rows_copy(out, i, slot).start()
            return carry
        count = out.shape[0] // block
        lax.fori_loop(0, count, body, 0)
        return first + count

    def plain_rows(ref):
        return lambda i, rhs_ref: dot_nn(ref[step(i, block), :], rhs_ref[...])

    loads[0].wait()
    loads[1].wait()
    for copy in loads[2:]:
        copy.start()
    sent = product(qkv_out, plain_rows(dqkv_ref), r1_ref, 0)

    loads[2].wait()
    loads[3].wait()

    def inter_copy(index, slot):
        return pltpu.make_async_copy(inter_ref.at[slot].reshape(GU_BLOCK, pad, 128).at[:, 0:32, :],
                                     gu_out.at[step(index, GU_BLOCK)], inter_sem.at[slot])

    gu_steps = gu_out.shape[0] // GU_BLOCK

    def gu_body(i, carry):
        slot = lax.rem(i, inter_slots)

        @pl.when(i >= inter_slots)
        def _():
            inter_copy(0, slot).wait()
        lhs = r2_ref[:, step(i, GU_BLOCK)].T
        for k in range(2):
            for n in range(ff // 512):
                val = dot_nn(lhs, dgu_ref[:, k * ff + n * 512:k * ff + (n + 1) * 512])
                for t in range(4):
                    row = 2 * (4 * n + t) + k
                    inter_ref[slot, pl.ds(row, GU_BLOCK, stride=pad), :] = val[:, t * 128:(t + 1) * 128]
        inter_copy(i, slot).start()
        return carry

    lax.fori_loop(0, gu_steps, gu_body, 0)

    loads[4].wait()
    loads[5].wait()
    sent = product(wout_out, plain_rows(mix_ref), dh_ref, sent)
    loads[6].wait()
    loads[7].wait()
    sent = product(down_out, lambda i, rhs_ref: dot_tn(act_ref[:, step(i, block)], rhs_ref[...]), dy_ref, sent)
    loads[8].wait()
    loads[9].wait()
    ends = [pltpu.make_async_copy(y_ref, y_out, end_sem.at[0]), pltpu.make_async_copy(dx_ref, dx_out, end_sem.at[1])]
    for copy in ends:
        copy.start()
    for slot in range(slots):
        rows_copy(down_out, 0, slot).wait()
    for slot in range(inter_slots):
        inter_copy(0, slot).wait()
    for copy in ends:
        copy.wait()


GU_BLOCK = 128


def weight_grads(act, grad_out, r2, dgu, mix, dh, dqkv, r1, y, dx, dg1, dg2):
    tokens, width = r2.shape
    ff = act.shape[1]
    any_spec = pl.BlockSpec(memory_space=pl.ANY)
    vmem_spec = pl.BlockSpec(memory_space=pltpu.VMEM)
    out = lambda *shape: jax.ShapeDtypeStruct(shape, F32)
    like = lambda a: jax.ShapeDtypeStruct(a.shape, a.dtype)
    arrays = (act, grad_out, r2, dgu, mix, dh, dqkv, r1, y, dx)
    return pl.pallas_call(
        grads_kernel,
        name="weight_grads",
        in_specs=[any_spec] * 10 + [vmem_spec] * 2,
        out_specs=[any_spec] * 6 + [vmem_spec] * 2,
        out_shape=[out(ff, width), out(width, 32, 128), out(mix.shape[0], width), out(dqkv.shape[0], width), like(y), like(dx), out(width), out(width)],
        scratch_shapes=[pltpu.VMEM(a.shape, a.dtype) for a in arrays] + [
            pltpu.VMEM((8, 256, width), F32), pltpu.VMEM((6, GU_BLOCK * 40, 128), F32),
            pltpu.SemaphoreType.DMA((10,)), pltpu.SemaphoreType.DMA((8,)), pltpu.SemaphoreType.DMA((6,)), pltpu.SemaphoreType.DMA((2,))],
        compiler_params=pltpu.CompilerParams(vmem_limit_bytes=56 << 20),
    )(*arrays, dg1, dg2)


def solution(mesh):
    def per_device(x_in, positions, gain_one, gain_two, w_qkv, w_out, w_gu, w_down, grad_out):
        width, groups, chans = w_qkv.shape
        ff = w_down.shape[0]
        qkv_rows = w_qkv.transpose(1, 2, 0).reshape(groups * chans, width)
        gu_rows = w_gu.reshape(width, 2, ff // 128, 128).transpose(0, 2, 1, 3).reshape(width * 2 * (ff // 128), 128)
        y, dx, dg1, dg2, r1, dqkv, mix, dh, r2, dgu, act = run_layer(
            x_in, positions, gain_one, gain_two, qkv_rows, w_out, gu_rows, w_down, grad_out)
        d_down, d_gu, d_out, d_qkv, y, dx, dg1, dg2 = weight_grads(act, grad_out, r2, dgu, mix, dh, dqkv, r1, y, dx, dg1, dg2)
        d_gu = d_gu.reshape(width, ff // 128, 2, 128).transpose(0, 2, 1, 3).reshape(width, 2, ff)
        d_qkv = d_qkv.reshape(groups, chans, width).transpose(2, 0, 1)
        return y, dx, dg1, dg2, d_qkv, d_out, d_gu, d_down

    act_spec = P('dp', 'embed')
    in_specs = (act_spec, P('dp'), P('embed'), P('embed'), P('embed', 'heads', None), P('heads', 'embed'), P('embed', None, 'heads'), P('heads', 'embed'), act_spec)
    out_specs = (act_spec, act_spec, P(('dp', 'embed')), P(('dp', 'embed')), P(('dp', 'embed'), 'heads', None), P(('dp', 'heads'), 'embed'), P(('dp', 'embed'), None, 'heads'), P(('dp', 'heads'), 'embed'))
    return jax.shard_map(per_device, mesh=mesh, in_specs=in_specs, out_specs=out_specs, check_vma=False)
```
